32 devices in a mesh: dp: 2 (over x), row: 4 (over y, core), col: 4 (over z).
Axes of the slice: x: 2, y: 2, z: 4, core: 2. Of those that a mesh axis runs over, the one named last changes fastest.
Arguments:
- tokens: bfloat16 [16384, 1024], P(('dp', 'row'), 'col'), may hold values from -6 to 6
- condition: bfloat16 [16, 1024], P('dp', 'row'), may hold values from -6 to 6
- modulation_weight: bfloat16 [1024, 6, 1024], P('row', None, 'col'), may hold values from -0.1875 to 0.1875
- modulation_bias: bfloat16 [6, 1024], P(None, 'col'), may hold values from -2 to 2
- input_weight: bfloat16 [1024, 3, 1024], P('col', None, 'row'), may hold values from -0.1875 to 0.1875
- input_bias: bfloat16 [2, 1024], P(None, 'row'), may hold values from -2 to 2
- output_weight: bfloat16 [1024, 1024], P('row', 'col'), may hold values from -1.5 to 1.5
- output_bias: bfloat16 [1024], P('col'), may hold values from -3 to 3
- expand_weight: bfloat16 [1024, 4096], P('col', 'row'), may hold values from -0.1875 to 0.1875
- expand_bias: bfloat16 [4096], P('row'), may hold values from -2 to 2
- shrink_weight: bfloat16 [4096, 1024], P('row', 'col'), may hold values from -0.09375 to 0.09375
- shrink_bias: bfloat16 [1024], P('col'), may hold values from -3 to 3
- cotangent: bfloat16 [16384, 1024], P(('dp', 'row'), 'col'), may hold values from -6 to 6
Outputs:
- layer_output: bfloat16 [16384, 1024], P(('dp', 'row'), 'col')
- tokens_gradient: float32 [16384, 1024], P(('dp', 'row'), 'col')
- condition_gradient: float32 [16, 1024], P('dp', 'row')
- modulation_weight_gradient: float32 [1024, 6, 1024], P('row', None, 'col')
- modulation_bias_gradient: float32 [6, 1024], P(None, 'col')
- input_weight_gradient: float32 [1024, 3, 1024], P('col', None, 'row')
- input_bias_gradient: float32 [2, 1024], P(None, 'row')
- output_weight_gradient: float32 [1024, 1024], P('row', 'col')
- output_bias_gradient: float32 [1024], P('col')
- expand_weight_gradient: float32 [1024, 4096], P('col', 'row')
- expand_bias_gradient: float32 [4096], P('row')
- shrink_weight_gradient: float32 [4096, 1024], P('row', 'col')
- shrink_bias_gradient: float32 [1024], P('col')
The draws below stay inside these ranges and needn't reach their ends.
All inputs are finite; a program needn't handle non-finite values.
Results may differ from the reference program's by a relative error of at most 0.01.
The reference program's roundings to bfloat16 on the way count: a program that leaves them out, or rounds other values in their place, can miss the bound.
Values may be sent and summed in bfloat16 or wider, within the bound.
No kernel may reach another device: no remote copies, remote signals or barrier semaphores. Data moves between devices by JAX's collectives and lax.ppermute only.
A program may use at most 192 MiB of HBM per device.

```python
import jax
import jax.numpy as jnp
from jax import lax

D = 1024
HEADS = 16
HEAD_DIM = 64
FF = 4096
LENGTH = 1024
LAT_DEV = 2
LATENTS = 16
TOKENS = 16384
INNER = 1024


def block_scale(rng, shape, cuts, smallest, high):
    loudness = 1.0
    for dim, parts in cuts:
        steps = jax.random.uniform(jax.random.fold_in(jax.random.fold_in(rng, 6), dim), (parts,), jnp.float32, smallest / len(cuts), high / len(cuts))
        loudness = loudness * jnp.repeat(jnp.exp(steps), shape[dim] // parts).reshape((-1,) + (1,) * (len(shape) - 1 - dim))
    return loudness


def centred(rng, extent, scale, limit, cuts=(), dtype=jnp.bfloat16):
    values = jax.random.normal(rng, extent, jnp.float32) * scale
    if len(cuts) > 0:
        values = block_scale(rng, extent, cuts, -0.22, 0.18) * values
    return jnp.clip(values, min=-limit, max=limit).astype(dtype)


def setup_inputs(seed: int = 0) -> dict:
    keys = jax.random.split(jax.random.key(seed), 14)
    return {
        "tokens": centred(keys[0], (TOKENS, D), 1.0, 6.0, ((0, 8), (1, 4))),
        "condition": centred(keys[1], (LATENTS, D), 1.0, 6.0, ((0, 2), (1, 4))),
        "modulation_weight": centred(keys[2], (D, 6, D), D ** -0.5, 0.1875, ((0, 4), (2, 4))),
        "modulation_bias": centred(keys[3], (6, D), 0.3, 2.0, ((1, 4),)),
        "input_weight": centred(keys[4], (D, 3, INNER), D ** -0.5, 0.1875, ((0, 4), (2, 4))),
        "input_bias": centred(keys[5], (2, INNER), 0.3, 2.0, ((1, 4),)),
        "output_weight": centred(keys[6], (INNER, D), (INNER // 64) ** -0.5, 1.5, ((0, 4), (1, 4))),
        "output_bias": centred(keys[7], (D,), 0.5, 3.0, ((0, 4),)),
        "expand_weight": centred(keys[8], (D, FF), D ** -0.5, 0.1875, ((0, 4), (1, 4))),
        "expand_bias": centred(keys[9], (FF,), 0.3, 2.0, ((0, 4),)),
        "shrink_weight": centred(keys[10], (FF, D), FF ** -0.5, 0.09375, ((0, 4), (1, 4))),
        "shrink_bias": centred(keys[11], (D,), 0.5, 3.0, ((0, 4),)),
        "cotangent": centred(keys[12], (TOKENS, D), 1.0, 6.0, ((0, 8), (1, 4))),
    }


EPS = 1e-06

@jax.custom_vjp
def low(v):
    return lax.optimization_barrier(v.astype(jnp.bfloat16)).astype(jnp.float32)

@jax.custom_vjp
def low_back(v):
    return v

def low_keep(v):
    return (low(v), None)

def low_pass(kept, grad):
    return (grad,)

def back_keep(v):
    return (v, None)

def back_low(kept, grad):
    return (low(grad),)
low.defvjp(low_keep, low_pass)
low_back.defvjp(back_keep, back_low)

def gelu_tanh(values):
    return 0.5 * values * (1.0 + jnp.tanh(0.7978845608028654 * (values + 0.044715 * values * values * values)))

def matmul(left, right):
    return jnp.dot(left, right, precision=lax.Precision.HIGHEST)

def normalize(values):
    average = lax.optimization_barrier(jnp.mean(values, axis=-1, keepdims=True))
    spread = lax.optimization_barrier(jnp.mean(values * values, axis=-1, keepdims=True)) - average * average
    return (values - average) * lax.rsqrt(spread + EPS)

def attend(pieces):
    queries, key_rows, values = pieces
    scores = jnp.einsum('qhd,khd->hqk', queries, key_rows, precision=lax.Precision.HIGHEST) * HEAD_DIM ** (-0.5)
    scores = low_back(scores)
    probability = low(jax.nn.softmax(scores, axis=-1))
    return jnp.einsum('hqk,khd->qhd', probability, values, precision=lax.Precision.HIGHEST)

def layer(tokens, condition, modulation_weight, modulation_bias, input_weight, input_bias, output_weight, output_bias, expand_weight, expand_bias, shrink_weight, shrink_bias):
    groups = condition.shape[0]
    features = tokens.shape[1]
    modulation = matmul(low(jax.nn.silu(condition)), modulation_weight.reshape(features, -1)).reshape(groups, 6, features)
    modulation = low_back(modulation + modulation_bias)
    shaped = tokens.reshape(groups, -1, features)

    def modulate(normed, offset):
        return normed * (1.0 + modulation[:, offset + 1][:, None]) + modulation[:, offset][:, None]
    first_in = low(modulate(normalize(shaped), 0)).reshape(-1, features)
    projected = matmul(first_in, input_weight.reshape(features, -1)).reshape(-1, 3, HEADS * HEAD_DIM)
    queries = low(low_back(projected[:, 0] + input_bias[0]))
    key_rows = low(low_back(projected[:, 1]))
    values = low(low_back(projected[:, 2] + input_bias[1]))
    heads_shape = (groups, LENGTH, HEADS, HEAD_DIM)
    attended = lax.map(jax.checkpoint(attend), (queries.reshape(heads_shape), key_rows.reshape(heads_shape), values.reshape(heads_shape)))
    attended = low(low_back(attended.reshape(-1, HEADS * HEAD_DIM)))
    branch_one = low_back(matmul(attended, output_weight) + output_bias)
    middle = shaped + modulation[:, 2][:, None] * branch_one.reshape(groups, -1, features)
    second_in = low(modulate(normalize(middle), 3)).reshape(-1, features)
    expanded = low_back(matmul(second_in, expand_weight) + expand_bias)
    hidden = low(gelu_tanh(expanded))
    branch_two = low_back(matmul(hidden, shrink_weight) + shrink_bias)
    result = middle + modulation[:, 5][:, None] * branch_two.reshape(groups, -1, features)
    return result.reshape(-1, features)

def reference(tokens, condition, modulation_weight, modulation_bias, input_weight, input_bias, output_weight, output_bias, expand_weight, expand_bias, shrink_weight, shrink_bias, cotangent):
    params = (modulation_weight.astype(jnp.float32), modulation_bias.astype(jnp.float32), input_weight.astype(jnp.float32), input_bias.astype(jnp.float32), output_weight.astype(jnp.float32), output_bias.astype(jnp.float32), expand_weight.astype(jnp.float32), expand_bias.astype(jnp.float32), shrink_weight.astype(jnp.float32), shrink_bias.astype(jnp.float32))
    groups = LATENTS // LAT_DEV
    span = LAT_DEV * LENGTH
    token_groups = tokens.astype(jnp.float32).reshape(groups, span, D)
    cond_groups = condition.astype(jnp.float32).reshape(groups, LAT_DEV, D)
    back_groups = cotangent.astype(jnp.float32).reshape(groups, span, D)

    def step(totals, pieces):
        token_block, cond_block, back_block = pieces
        result, pull = jax.vjp(layer, token_block, cond_block, *params)
        pulled = pull(back_block)
        totals = tuple((total + part for total, part in zip(totals, pulled[2:])))
        return (totals, (result, pulled[0], pulled[1]))
    start = tuple((jnp.zeros(param.shape, jnp.float32) for param in params))
    totals, (outputs, token_grads, cond_grads) = lax.scan(step, start, (token_groups, cond_groups, back_groups))
    return (outputs.reshape(TOKENS, D).astype(jnp.bfloat16), token_grads.reshape(TOKENS, D), cond_grads.reshape(LATENTS, D), totals[0], totals[1], totals[2], totals[3], totals[4], totals[5], totals[6], totals[7], totals[8], totals[9])
```

```python
import functools
import math

import jax
import jax.numpy as jnp
from jax import lax
from jax.experimental import pallas as pl
from jax.experimental.pallas import tpu as pltpu
from jax.sharding import Mesh
from jax.sharding import PartitionSpec as P

HEAD_DIM = 64
LENGTH = 1024
EPS = 1e-06
LANES = 128
SCALE = HEAD_DIM ** (-0.5)
SCALE_LOG2 = SCALE * math.log2(math.e)
ROWS = ("y", "core")
COLS = ("lat", "sub")
NT = (((1,), (1,)), ((), ()))
F32 = jnp.float32
BF16 = jnp.bfloat16
VMEM_LIMIT = 56 * 1024 * 1024


def dot(left, right):
    return jnp.dot(left, right, preferred_element_type=F32)


def dot_nt(left, right):
    return lax.dot_general(left, right, NT, preferred_element_type=F32)


def gelu_tanh(values):
    return (
        0.5
        * values
        * (1.0 + jnp.tanh(0.7978845608028654 * (values + 0.044715 * values * values * values)))
    )


def gelu_slope(values):
    inner = jnp.tanh(0.7978845608028654 * (values + 0.044715 * values * values * values))
    rate = 0.7978845608028654 * (1.0 + 3 * 0.044715 * values * values)
    return 0.5 * (1.0 + inner) + 0.5 * values * (1.0 - inner * inner) * rate


def whole(shape):
    return pl.BlockSpec(shape, lambda *_: (0,) * len(shape))


def block(shape, column=0, first=0, step=1):
    return pl.BlockSpec((None, *shape), lambda b: (first + step * b, 0, column))


def call(kernel, grid, in_specs, out_specs, out_shape, scratch=(), flops=0, moved=0, exps=0):
    return pl.pallas_call(
        kernel,
        grid=grid,
        in_specs=in_specs,
        out_specs=out_specs,
        out_shape=out_shape,
        scratch_shapes=list(scratch),
        compiler_params=pltpu.CompilerParams(vmem_limit_bytes=VMEM_LIMIT),
        cost_estimate=pl.CostEstimate(flops=flops, bytes_accessed=moved, transcendentals=exps),
    )


def shaped(shape, dtype):
    return jax.ShapeDtypeStruct(shape, dtype)


def project(left, blocks, bias):
    number, features, _ = blocks.shape
    rows = left.shape[0]

    def kernel(a, g, c, q, kv):
        out = dot(a[...], g[...]) + c[...]
        q[...] = out[:, :LANES].astype(BF16)
        kv[...] = out[:, LANES:].astype(BF16)

    return call(
        kernel,
        (number,),
        [whole(left.shape), block((features, 3 * LANES)), block((1, 3 * LANES))],
        [block((rows, LANES)), block((rows, 2 * LANES))],
        [shaped((number, rows, LANES), BF16), shaped((number, rows, 2 * LANES), BF16)],
        flops=2 * rows * features * number * 3 * LANES,
        moved=2 * number * features * 3 * LANES,
    )(left, blocks, bias)


def expand(left, blocks, bias):
    number, features, _ = blocks.shape
    rows, width = left.shape[0], bias.shape[-1]

    def kernel(a, g, c, e, h):
        out = dot(a[...], g[...]) + c[...]
        e[...] = out
        h[...] = gelu_tanh(out).astype(BF16)

    return call(
        kernel,
        (number,),
        [whole(left.shape), block((features, width)), block((1, width))],
        [block((rows, width)), block((rows, width))],
        [shaped((number, rows, width), F32), shaped((number, rows, width), BF16)],
        flops=2 * rows * features * number * width,
        moved=number * width * (2 * features + 6 * rows),
    )(left, blocks, bias)


def hidden_backward(left, blocks, expanded):
    number, rows, width = expanded.shape
    features = left.shape[1]

    def kernel(a, g, e, back, sums):
        out = (dot(a[...], g[...]) * gelu_slope(e[...])).astype(BF16)
        back[...] = out
        sums[...] = jnp.sum(out.astype(F32), axis=0, keepdims=True)

    return call(
        kernel,
        (number,),
        [whole(left.shape), block((features, width)), block((rows, width))],
        [block((rows, width)), block((1, width))],
        [shaped((number, rows, width), BF16), shaped((number, 1, width), F32)],
        flops=2 * rows * features * number * width,
        moved=number * width * (2 * features + 6 * rows),
    )(left, blocks, expanded)


def attended_backward(left, blocks, column):
    number, features, _ = blocks.shape
    rows = left.shape[0]

    def kernel(a, g, out):
        out[...] = dot(a[...], g[...]).astype(BF16)

    return call(
        kernel,
        (number,),
        [whole(left.shape), block((features, LANES), column)],
        block((rows, LANES)),
        shaped((number, rows, LANES), BF16),
        flops=2 * rows * features * number * LANES,
        moved=number * LANES * (2 * features + 2 * rows),
    )(left, blocks)


def contract(terms, extras, finish, outs):
    number, rows, _ = terms[0][0].shape
    features = terms[0][1].shape[1]
    count, more = len(terms), len(extras)

    def kernel(*refs):
        lefts, rights = refs[:count], refs[count : 2 * count]
        given = refs[2 * count : 2 * count + more]
        results, total = refs[2 * count + more : -1], refs[-1]
        out = dot_nt(lefts[0][...], rights[0][...])
        for left, right in zip(lefts[1:], rights[1:]):
            out = out + dot_nt(left[...], right[...])
        step = pl.program_id(0)

        @pl.when(step == 0)
        def _():
            total[...] = out

        @pl.when(step > 0)
        def _():
            total[...] += out

        @pl.when(step == number - 1)
        def _():
            finish(total, given, results)

    return call(
        kernel,
        (number,),
        [block(left.shape[1:]) for left, _, _ in terms]
        + [block((features, left.shape[2]), column) for left, _, column in terms]
        + [whole(extra.shape) for extra in extras],
        [whole(out.shape) for out in outs],
        outs,
        scratch=[pltpu.VMEM((rows, features), F32)],
        flops=2 * rows * features * number * sum(left.shape[2] for left, _, _ in terms),
        moved=number * sum(2 * left.shape[2] * (features + rows) for left, _, _ in terms),
    )(*[left for left, _, _ in terms], *[right for _, right, _ in terms], *extras)


def by_rows(rows, sums, features, work):
    tile = min(rows, 64)

    def step(i, totals):
        found = work(pl.ds(pl.multiple_of(i * tile, tile), tile))
        return tuple(
            total + jnp.sum(one.reshape(-1, 8, features), axis=0)
            for total, one in zip(totals, found)
        )

    zero = jnp.zeros((8, features), F32)
    totals = lax.fori_loop(0, rows // tile, step, (zero,) * sums)
    return [jnp.sum(total, axis=0, keepdims=True) for total in totals]


def normalize(values):
    average = jnp.mean(values, axis=1, keepdims=True)
    inverse = lax.rsqrt(
        jnp.mean(values * values, axis=1, keepdims=True) - average * average + EPS
    )
    return (values - average) * inverse, inverse


def norm_back(incoming, normed, inverse):
    return inverse * (
        incoming
        - jnp.mean(incoming, axis=1, keepdims=True)
        - normed * jnp.mean(incoming * normed, axis=1, keepdims=True)
    )


def finish_middle(total, given, results):
    tokens, vectors = given
    branch, middle, low = results
    rows, features = total.shape
    shift, scale, gate = vectors[3:4], 1.0 + vectors[4:5], vectors[2:3]
    bias = vectors[6:7]

    def work(here):
        one = total[here, :] + bias
        branch[here, :] = one
        values = tokens[here, :].astype(F32) + gate * one
        middle[here, :] = values
        low[here, :] = (normalize(values)[0] * scale + shift).astype(BF16)
        return ()

    by_rows(rows, 0, features, work)


def finish_output(total, given, results):
    middle, cotangent, vectors = given
    output, sums = results
    rows, features = total.shape
    gate, bias = vectors[5:6], vectors[7:8]

    def work(here):
        two = total[here, :] + bias
        output[here, :] = (middle[here, :] + gate * two).astype(BF16)
        return (two * cotangent[here, :].astype(F32),)

    (gate_back,) = by_rows(rows, 1, features, work)
    sums[...] = gate_back


def finish_middle_back(total, given, results):
    middle, branch, cotangent, vectors = given
    middle_back, low, sums = results
    rows, features = total.shape
    gate, scale = vectors[2:3], 1.0 + vectors[4:5]

    def work(here):
        back = total[here, :]
        normed, inverse = normalize(middle[here, :])
        out = cotangent[here, :].astype(F32) + norm_back(back * scale, normed, inverse)
        middle_back[here, :] = out
        rounded = (gate * out).astype(BF16)
        low[here, :] = rounded
        return back, back * normed, branch[here, :] * out, rounded.astype(F32)

    sums[...] = jnp.concatenate(by_rows(rows, 4, features, work), axis=0)


def finish_tokens_back(total, given, results):
    tokens, middle_back, vectors = given
    tokens_back, sums = results
    rows, features = total.shape
    scale = 1.0 + vectors[1:2]

    def work(here):
        back = total[here, :]
        normed, inverse = normalize(tokens[here, :].astype(F32))
        out = middle_back[here, :] + norm_back(back * scale, normed, inverse)
        tokens_back[here, :] = out.astype(BF16)
        return back, back * normed

    sums[...] = jnp.concatenate(by_rows(rows, 2, features, work), axis=0)


def gradients(pairs, adds=(), first=0, step=1, count=None, halves=False):
    features, rows = pairs[0][0].shape
    parts = [one for _, parts in pairs for one in parts]
    width = sum(one.shape[2] for one in parts)
    count = parts[0].shape[0] if count is None else count
    lefts, rights, extra = len(pairs), len(parts), len(adds)

    def kernel(*refs):
        left_refs = refs[:lefts]
        right_refs = list(refs[lefts : lefts + rights])
        add_refs = refs[lefts + rights : lefts + rights + extra]
        outs = refs[lefts + rights + extra :]
        start = 0
        for left, (_, own) in zip(left_refs, pairs):
            for _ in own:
                right = right_refs.pop(0)
                here = slice(start, start + right.shape[1])
                out = dot(left[...], right[...])
                for add in add_refs:
                    out = out + add[:, here].astype(F32)
                out = out.astype(BF16)
                if halves:
                    outs[0][:, here] = out[: features // 2]
                    outs[1][:, here] = out[features // 2 :]
                else:
                    outs[0][:, here] = out
                start += right.shape[1]

    if halves:
        out_specs = [whole((features // 2, width))] * 2
        outs = [shaped((features // 2, width), BF16)] * 2
    else:
        out_specs = [block((features, width))]
        outs = [shaped((count, features, width), BF16)]
    got = call(
        kernel,
        (count,),
        [whole(left.shape) for left, _ in pairs]
        + [block(one.shape[1:], 0, first, step) for one in parts]
        + [block(add.shape[1:], 0, one, two) for add, one, two in adds],
        out_specs,
        outs,
        flops=2 * rows * features * count * width,
        moved=count * width * features * 2 * (1 + extra),
    )(*[left for left, _ in pairs], *parts, *[add for add, _, _ in adds])
    return got if halves else got[0]


def attend(queries, pieces):
    number, rows, _ = queries.shape
    count = len(pieces)
    keys = sum(piece.shape[1] for piece in pieces)
    tile = min(rows, 256)

    def kernel(*refs):
        query, kv = refs[0], refs[1 : 1 + count]
        out_ref, log_ref = refs[1 + count :]
        head = lax.broadcasted_iota(jnp.int32, (1, LANES), 1) < HEAD_DIM
        for start in range(0, rows, tile):
            here = slice(start, start + tile)
            both = query[here, :]
            outs, logs = [], []
            for keep in (head, ~head):
                one = jnp.where(keep, both, jnp.zeros_like(both))
                scores = [dot_nt(one, piece[:, :LANES]) for piece in kv]
                top = functools.reduce(
                    jnp.maximum, [jnp.max(s, axis=1, keepdims=True) for s in scores]
                )
                weights = [jnp.exp2((s - top) * SCALE_LOG2) for s in scores]
                total = sum(jnp.sum(w, axis=1, keepdims=True) for w in weights)
                inverse = 1.0 / total
                out = sum(
                    dot((w * inverse).astype(BF16), piece[:, LANES:])
                    for w, piece in zip(weights, kv)
                )
                outs.append(out)
                logs.append(top * SCALE_LOG2 + jnp.log(total) * math.log2(math.e))
            out_ref[here, :] = jnp.where(head, outs[0], outs[1]).astype(BF16)
            table = jnp.where(head, logs[0], logs[1]).T
            log_ref[0:1, here] = table[0:1]
            log_ref[1:2, here] = table[HEAD_DIM : HEAD_DIM + 1]

    return call(
        kernel,
        (number,),
        [block((rows, LANES))] + [block((piece.shape[1], 2 * LANES)) for piece in pieces],
        [block((rows, LANES)), block((2, rows))],
        [shaped((number, rows, LANES), BF16), shaped((number, 2, rows), F32)],
        flops=number * 2 * 2 * 2 * rows * keys * 256,
        exps=number * 2 * rows * keys,
        moved=number * 2 * LANES * (2 * rows + 2 * keys),
    )(queries, *pieces)


def attend_back(queries, pieces, logs, incoming, kinds, first=0, number=None):
    number = queries.shape[0] if number is None else number
    rows = queries.shape[1]
    count = len(pieces)
    keys = sum(piece.shape[1] for piece in pieces)
    tile = min(rows, 256)

    def kernel(*refs):
        query, back_ref, log_ref = refs[:3]
        kv = refs[3 : 3 + count]
        query_back = refs[3 + count]
        kv_back = refs[4 + count : 4 + 2 * count]
        sums, scratch = refs[4 + 2 * count], refs[5 + 2 * count :]
        head = lax.broadcasted_iota(jnp.int32, (1, LANES), 1) < HEAD_DIM
        turned = [piece[:, :LANES].T for piece in kv]
        top = lax.broadcasted_iota(jnp.int32, (LANES, 1), 0) < HEAD_DIM
        query_sum = jnp.zeros((1, LANES), F32)
        for start in range(0, rows, tile):
            here = slice(start, start + tile)
            backs = []
            for index, keep in enumerate((head, ~head)):
                zero = jnp.zeros((tile, LANES), BF16)
                one = jnp.where(keep, query[here, :], zero)
                back = jnp.where(keep, back_ref[here, :], zero)
                log = log_ref[index : index + 1, here]
                chances, mixes = [], []
                for piece in kv:
                    scores = dot_nt(piece[:, :LANES], one)
                    chances.append(jnp.exp2(scores * SCALE_LOG2 - log))
                    mixes.append(dot_nt(piece[:, LANES:], back))
                centre = sum(
                    jnp.sum(p * m, axis=0, keepdims=True) for p, m in zip(chances, mixes)
                )
                total = None
                for i in range(count):
                    score_back = (chances[i] * (mixes[i] - centre)).astype(BF16)
                    key_back = dot(score_back, one) * SCALE
                    value_back = dot(chances[i].astype(BF16), back)
                    if start == 0 and index == 0:
                        scratch[i][:, :LANES] = key_back
                        scratch[i][:, LANES:] = value_back
                    else:
                        scratch[i][:, :LANES] += key_back
                        scratch[i][:, LANES:] += value_back
                    term = dot(turned[i], score_back)
                    total = term if total is None else total + term
                backs.append(total)
            both = (jnp.where(top, backs[0], backs[1]).T * SCALE).astype(BF16)
            query_back[here, :] = both
            query_sum = query_sum + jnp.sum(both.astype(F32), axis=0, keepdims=True)
        sums[...] = query_sum
        for out, held in zip(kv_back, scratch):
            out[...] = held[...].astype(out.dtype)

    here = dict(first=first)
    return call(
        kernel,
        (number,),
        [block((rows, LANES), **here), block((rows, LANES), **here), block((2, rows), **here)]
        + [block((piece.shape[1], 2 * LANES), **here) for piece in pieces],
        [block((rows, LANES))]
        + [block((piece.shape[1], 2 * LANES)) for piece in pieces]
        + [block((1, LANES))],
        [shaped((number, rows, LANES), BF16)]
        + [
            shaped((number, piece.shape[1], 2 * LANES), kind)
            for piece, kind in zip(pieces, kinds)
        ]
        + [shaped((number, 1, LANES), F32)],
        scratch=[pltpu.VMEM((piece.shape[1], 2 * LANES), F32) for piece in pieces],
        flops=number * 2 * 5 * 2 * rows * keys * 256,
        exps=number * 2 * rows * keys,
        moved=number * 2 * LANES * (4 * rows + 8 * keys),
    )(queries, incoming, logs, *pieces)


class Plain:
    def __init__(self, sizes):
        self.latents, self.parts, self.width = sizes
        self.row = lax.axis_size("y") * lax.axis_size("core")
        self.col = lax.axis_size("lat") * lax.axis_size("sub")

    def scatter(self, values):
        rows, width = values.shape
        shaped_in = values.reshape(self.latents, 2, LENGTH // 2, width)
        halves = lax.all_to_all(shaped_in, "core", 1, 0, tiled=True)
        pieces = halves.reshape(self.col, -1, width)
        pieces = lax.all_to_all(pieces, COLS, 0, 0, tiled=True)
        return pieces.transpose(1, 0, 2).reshape(-1, self.col * width)

    def collect(self, values):
        rows, features = values.shape
        pieces = values.reshape(rows, self.col, -1).transpose(1, 0, 2)
        pieces = lax.all_to_all(pieces, COLS, 0, 0, tiled=True)
        halves = pieces.reshape(2 * self.latents, 1, LENGTH // 2, -1)
        back = lax.all_to_all(halves, "core", 0, 1, tiled=True)
        return back.reshape(-1, features // self.col)

    def modulation(self, partial, bias, row_bias, col_bias):
        group = 2 * self.latents
        ours = lax.psum(partial, "core").reshape(-1, group, partial.shape[1])
        ours = lax.psum_scatter(ours, "y", scatter_dimension=0, tiled=True)[0] + bias
        sent = jnp.repeat(ours, self.col // group, axis=0)
        got = lax.all_to_all(sent, COLS, 0, 0, tiled=True)
        got = got.reshape(self.col, 6, -1).transpose(1, 0, 2).reshape(6, -1)
        cols = lax.all_gather(col_bias, COLS, axis=1, tiled=True)
        every = lax.all_gather(row_bias, ROWS, axis=0)
        return jnp.concatenate([got, cols], axis=0), [
            every.reshape(self.row * self.parts, 1, -1)
        ]

    def own_parts(self, parts):
        return parts

    def gather(self, parts, order):
        every = lax.all_gather(parts, COLS, axis=1, tiled=True)
        return [lax.all_gather(every, ROWS, axis=0, tiled=True)]

    def share(self, kv):
        return [[lax.all_gather(kv[0], ("core", "sub"), axis=1, tiled=True)]]

    def kinds(self):
        return [F32]

    def give_back(self, backs):
        return [
            lax.psum_scatter(
                backs[0][0], ("core", "sub"), scatter_dimension=1, tiled=True
            ).astype(BF16)
        ]

    def reduce(self, pairs, order):
        grads = gradients(pairs[0]).astype(F32)
        grads = lax.psum_scatter(grads, ROWS, scatter_dimension=0, tiled=True)
        grads = lax.psum_scatter(grads, COLS, scatter_dimension=1, tiled=True)
        return lax.psum(grads, "dp")

    def small(self, vectors, row_sums, col_sums):
        every = ("dp", *ROWS, *COLS)
        group = 2 * self.latents
        total = lax.psum(vectors, ("core", "sub")).astype(BF16)
        mine = lax.all_gather(total[:, None], "lat", axis=1, tiled=True)
        mine = lax.all_gather(mine, "y", axis=1, tiled=True)
        mine = lax.all_gather(mine, "dp", axis=1, tiled=True)
        col = lax.axis_index("lat") * lax.axis_size("sub") + lax.axis_index("sub")
        cut = lax.dynamic_slice_in_dim(mine, col * self.width, self.width, axis=2)
        cut = cut.transpose(1, 0, 2).reshape(mine.shape[1], -1)
        rows = lax.psum(row_sums[0], every).reshape(self.row, self.parts, -1)
        row = lax.axis_index("y") * 2 + lax.axis_index("core")
        rows = lax.dynamic_index_in_dim(rows, row, 0, keepdims=False)
        cols = lax.psum(col_sums, every)
        cols = lax.dynamic_slice_in_dim(cols, col * self.width, self.width, axis=1)
        return cut, rows, cols

    def both_groups(self, values):
        return lax.all_gather(values, "dp", axis=0, tiled=True)


class Cube(Plain):
    def __init__(self, sizes):
        super().__init__(sizes)
        self.x = lax.axis_index("dp")
        self.y = lax.axis_index("y")
        self.c = lax.axis_index("core")
        self.z = lax.axis_index("lat")

    def swap(self, values, axis):
        return lax.ppermute(values, axis, [(0, 1), (1, 0)])

    def along(self, values, bits):
        return lax.ppermute(values, "lat", [(i, i ^ bits) for i in range(4)])

    def scatter(self, values):
        rows, width = values.shape
        halves = values.reshape(self.latents, 2, LENGTH // 2, width)
        keep = lax.dynamic_index_in_dim(halves, self.c, 1, keepdims=False)
        send = lax.dynamic_index_in_dim(halves, 1 - self.c, 1, keepdims=False)
        every = jnp.concatenate([keep, self.swap(send, "core")], axis=0)
        pieces = []
        for bits in range(4):
            latent = self.z ^ bits
            index = ((latent // 2) ^ self.c) * 2 + latent % 2
            piece = lax.dynamic_index_in_dim(every, index, 0, keepdims=False)
            pieces.append(piece if bits == 0 else self.along(piece, bits))
        return jnp.concatenate(pieces, axis=1)

    def collect(self, values):
        rows, features = values.shape
        width = features // 4
        pieces = [values[:, i * width : (i + 1) * width] for i in range(4)]
        pieces = [p if bits == 0 else self.along(p, bits) for bits, p in enumerate(pieces)]
        every = jnp.stack(pieces)

        def latents(core):
            return jnp.stack(
                [
                    lax.dynamic_index_in_dim(every, self.z ^ (2 * core + i), 0, keepdims=False)
                    for i in range(2)
                ]
            )

        keep = latents(self.c)
        got = self.swap(latents(1 - self.c), "core")
        first = jnp.where(self.c == 0, keep, got)
        second = jnp.where(self.c == 0, got, keep)
        return jnp.stack([first, second], axis=1).reshape(-1, width)

    def modulation(self, partial, bias, row_bias, col_bias):
        span = partial.shape[1]
        own = row_bias.reshape(1, -1)
        got = self.swap(jnp.concatenate([partial, own], axis=0), "core")
        ours, other = partial + got[:-1], got[-1:]
        halves = ours.reshape(2, 4, span)
        keep = lax.dynamic_index_in_dim(halves, self.y, 0, keepdims=False)
        send = lax.dynamic_index_in_dim(halves, 1 - self.y, 0, keepdims=False)
        got = self.swap(jnp.concatenate([send, own, other], axis=0), "y")
        ours = keep + got[:4] + bias
        rows = jnp.stack([own, got[4:5], other, got[5:6]]).reshape(2, 2, 2, -1)
        flip = jnp.stack([rows[:, :, 1], rows[:, :, 0]], axis=2)
        rows = jnp.where(self.x == 0, rows, flip).transpose(0, 2, 1, 3).reshape(2, 4, 1, -1)
        pieces = []
        for bits in range(4):
            piece = lax.dynamic_index_in_dim(ours, self.z ^ bits, 0, keepdims=False)
            piece = jnp.concatenate([piece.reshape(6, -1), col_bias], axis=0)
            pieces.append(piece if bits == 0 else self.along(piece, bits))
        return jnp.concatenate(pieces, axis=1), [rows[0], rows[1]]

    def own_parts(self, parts):
        return lax.dynamic_index_in_dim(parts, self.x, 0, keepdims=False)

    def gather(self, part, order):
        part = jnp.concatenate([part, self.along(part, 1)], axis=0)
        part = jnp.concatenate([part, self.along(part, 2)], axis=0)
        first, second = ("y", "dp") if order == "yx" else ("dp", "y")
        pair = jnp.stack([part, self.swap(part, first)])
        other = self.swap(pair, second)
        four = jnp.stack([pair, other], axis=0 if order == "yx" else 1)
        four = four.reshape(4, *part.shape)
        return [four, self.swap(four, "core")]

    def share(self, kv):
        return [[kv[0], self.swap(kv[1], "core")], [kv[1], self.swap(kv[0], "core")]]

    def kinds(self):
        return [F32, BF16]

    def give_back(self, backs):
        got = [self.swap(backs[1][1], "core"), self.swap(backs[0][1], "core")]
        return [(own[0] + one.astype(F32)).astype(BF16) for own, one in zip(backs, got)]

    def reduce(self, pairs, order):
        near = self.swap(gradients(pairs[1]), "core")
        if order == "xy":
            axes, first, step, last = ("dp", "y"), 2, 1, 1
        else:
            axes, first, step, last = ("y", "dp"), 1, 2, 2
        sent = gradients(pairs[0], [(near, first, step)], first, step, 2)
        second = self.swap(sent, axes[0])
        sent = gradients(pairs[0], [(near, last, 1), (second, 1, 1)], last, 1, 1)
        third = self.swap(sent, axes[1])
        low, high = gradients(
            pairs[0], [(near, 0, 1), (second, 0, 1), (third, 0, 1)], 0, 1, 1, halves=True
        )
        low = low.astype(F32) + self.along(high, 2).astype(F32)
        rows = low.shape[0] // 2
        own = (low[:rows] + self.along(low[rows:].astype(BF16), 1).astype(F32)).astype(BF16)
        other = self.swap(own, "dp")
        return jnp.stack(
            [jnp.where(self.x == 0, own, other), jnp.where(self.x == 0, other, own)]
        ).astype(F32)

    def small(self, vectors, row_sums, col_sums):
        span = row_sums[0].shape[-1]
        features = vectors.shape[1]

        def flat(*parts):
            return jnp.concatenate([part.reshape(-1, LANES) for part in parts], axis=0)

        def cut(message, *shapes):
            parts, start = [], 0
            for shape in shapes:
                size = math.prod(shape) // LANES
                parts.append(message[start : start + size].reshape(shape))
                start += size
            return parts

        rows0, rows1 = (one.reshape(2, 2, span) for one in row_sums)
        got = self.swap(flat(rows1, col_sums, vectors), "core")
        got = cut(got, rows1.shape, col_sums.shape, vectors.shape)
        rows, cols = rows0 + got[0], col_sums + got[1]
        mine = (vectors + got[2]).astype(BF16).astype(F32)
        got = self.swap(flat(rows[:, 1], cols, mine), "y")
        got = cut(got, (2, span), cols.shape, mine.shape)
        rows, cols = rows[:, 0] + got[0], cols + got[1]
        pair = jnp.stack([mine, got[2]])
        got = self.swap(flat(rows, cols, pair), "dp")
        got = cut(got, rows.shape, cols.shape, pair.shape)
        rows = rows + jnp.stack([got[0][1], got[0][0]])
        rows = jnp.where(self.x == 0, rows, jnp.stack([rows[1], rows[0]]))
        cols = cols + got[1]
        four = jnp.stack([pair, got[2]]).reshape(4, 6, features)
        width = self.width
        found = []
        for bits in range(4):
            here = slice(bits * width, (bits + 1) * width)
            piece = [four[:, :, here], cols[:, here], rows]
            if bits:
                got = self.along(flat(*piece), bits)
                piece = cut(got, *[part.shape for part in piece])
            found.append(piece)
        tree = [(found[0][i] + found[1][i]) + (found[2][i] + found[3][i]) for i in (1, 2)]
        every = jnp.stack([one[0] for one in found])
        every = every.reshape(16, -1)
        place = lax.broadcasted_iota(jnp.int32, (16, 16), 0)
        held = lax.broadcasted_iota(jnp.int32, (16, 16), 1)
        latent = (
            (((held // 2) % 2) ^ self.x) * 8 + ((held % 2) ^ self.y) * 4 + ((held // 4) ^ self.z)
        )
        chosen = (latent == place).astype(F32)
        every = jnp.dot(chosen, every, precision=lax.Precision.HIGHEST).astype(BF16)
        return every, tree[1], tree[0]

    def both_groups(self, values):
        got = self.swap(values, "dp")
        return jnp.where(
            self.x == 0,
            jnp.concatenate([values, got], axis=0),
            jnp.concatenate([got, values], axis=0),
        )


def body(
    fast,
    tokens,
    condition,
    modulation_weight,
    modulation_bias,
    input_weight,
    input_bias,
    output_weight,
    output_bias,
    expand_weight,
    expand_bias,
    shrink_weight,
    shrink_bias,
    cotangent,
):
    width = tokens.shape[1]
    inner = input_weight.shape[2]
    parts = inner // LANES
    units = expand_weight.shape[1] // parts
    sizes = (tokens.shape[0] // LENGTH, parts, width)
    net = (Cube if fast else Plain)(sizes)

    own_in = net.own_parts(
        input_weight.reshape(width, 3, parts, LANES)
        .transpose(2, 0, 1, 3)
        .reshape(parts, width, 3 * LANES)
    )
    own_out = net.own_parts(output_weight.reshape(parts, LANES, width).transpose(0, 2, 1))
    own_expand = net.own_parts(expand_weight.reshape(width, parts, units).transpose(1, 0, 2))
    own_shrink = net.own_parts(shrink_weight.reshape(parts, units, width).transpose(0, 2, 1))
    out_column = units // LANES

    condition_float = condition.astype(F32)
    silu_low = jax.nn.silu(condition_float).astype(BF16)
    modulator = modulation_weight.reshape(modulation_weight.shape[0], -1)
    row_bias = jnp.concatenate(
        [
            input_bias.reshape(2, parts, LANES).transpose(1, 0, 2).reshape(parts, -1),
            expand_bias.reshape(parts, units),
        ],
        axis=1,
    ).astype(F32)
    vectors, row_biases = net.modulation(
        dot(silu_low, modulator),
        modulation_bias.astype(F32).reshape(1, -1),
        row_bias,
        jnp.stack([output_bias, shrink_bias]).astype(F32),
    )
    mine = net.scatter(tokens)
    in_bufs = net.gather(own_in, "yx")
    out_bufs = net.gather(jnp.concatenate([own_expand, own_out], axis=-1), "xy")
    shrink_bufs = net.gather(own_shrink, "yx")
    back = net.scatter(cotangent)
    rows = mine.shape[0]
    features = mine.shape[1]
    in_biases = [
        jnp.concatenate(
            [one[..., :LANES], jnp.zeros_like(one[..., :LANES]), one[..., LANES : 2 * LANES]],
            axis=-1,
        )
        for one in row_biases
    ]
    expand_biases = [one[..., 2 * LANES :] for one in row_biases]

    normed, _ = normalize(mine.astype(F32))
    low_one = (normed * (1.0 + vectors[1:2]) + vectors[0:1]).astype(BF16)
    queries, own_kv = [], []
    for buf, bias in zip(in_bufs, in_biases):
        one, two = project(low_one, buf, bias)
        queries.append(one)
        own_kv.append(two)
    kv = net.share(own_kv)
    attended, logs = [], []
    for one, pieces in zip(queries, kv):
        out, log = attend(one, pieces)
        attended.append(out)
        logs.append(log)
    branch_one, middle, low_two = contract(
        [(one, buf, out_column) for one, buf in zip(attended, out_bufs)],
        [mine, vectors],
        finish_middle,
        [
            shaped((rows, features), F32),
            shaped((rows, features), F32),
            shaped((rows, features), BF16),
        ],
    )
    expanded, hidden = [], []
    for buf, bias in zip(out_bufs, expand_biases):
        one, two = expand(low_two, buf, bias)
        expanded.append(one)
        hidden.append(two)
    output, gate_two_back = contract(
        [(one, buf, 0) for one, buf in zip(hidden, shrink_bufs)],
        [middle, back, vectors],
        finish_output,
        [shaped((rows, features), BF16), shaped((1, features), F32)],
    )

    branch_two_back = (vectors[5:6] * back.astype(F32)).astype(BF16)
    shrink_sum = jnp.sum(branch_two_back.astype(F32), axis=0, keepdims=True)
    turned_two_back = branch_two_back.T
    shrink_parts = net.reduce([[(turned_two_back, [one])] for one in hidden], "xy")
    expanded_back, expand_sums = [], []
    for buf, one in zip(shrink_bufs, expanded):
        two, sums = hidden_backward(branch_two_back, buf, one)
        expanded_back.append(two)
        expand_sums.append(sums)
    middle_back, branch_one_back, sums_two = contract(
        [(one, buf, 0) for one, buf in zip(expanded_back, out_bufs)],
        [middle, branch_one, back, vectors],
        finish_middle_back,
        [
            shaped((rows, features), F32),
            shaped((rows, features), BF16),
            shaped((4, features), F32),
        ],
    )
    turned_two, turned_one_back = low_two.T, branch_one_back.T
    out_parts = net.reduce(
        [
            [(turned_two, [one]), (turned_one_back, [two])]
            for one, two in zip(expanded_back, attended)
        ],
        "yx",
    )
    incoming = [attended_backward(branch_one_back, buf, out_column) for buf in out_bufs]
    query_back, backs, query_sums = [], [], []
    for one, pieces, log, two in zip(queries, kv, logs, incoming):
        got = attend_back(one, pieces, log, two, net.kinds())
        query_back.append(got[0])
        backs.append(got[1:-1])
        query_sums.append(got[-1])
    kv_back = net.give_back(backs)
    value_sums = [
        jnp.sum(one[:, :, LANES:].astype(F32), axis=1, keepdims=True) for one in kv_back
    ]
    turned_one = low_one.T
    in_parts = net.reduce(
        [[(turned_one, [one, two])] for one, two in zip(query_back, kv_back)], "xy"
    )
    tokens_back, sums_one = contract(
        [(one, buf, 0) for one, buf in zip(query_back, in_bufs)]
        + [(one[:, :, :LANES], buf, 1) for one, buf in zip(kv_back, in_bufs)]
        + [(one[:, :, LANES:], buf, 2) for one, buf in zip(kv_back, in_bufs)],
        [mine, middle_back, vectors],
        finish_tokens_back,
        [shaped((rows, features), BF16), shaped((2, features), F32)],
    )

    summed = jnp.concatenate([sums_one, sums_two[2:3], sums_two[0:2], gate_two_back], axis=0)
    row_sums = [
        jnp.concatenate([one, two, three], axis=-1)
        for one, two, three in zip(query_sums, value_sums, expand_sums)
    ]
    col_sums = jnp.concatenate([sums_two[3:4], shrink_sum], axis=0)
    every, row_found, col_found = net.small(summed, row_sums, col_sums)
    silu_all = net.both_groups(silu_low)
    modulation_weight_gradient = lax.dot_general(
        silu_all, every, (((0,), (0,)), ((), ())), preferred_element_type=F32
    ).reshape(modulation_weight.shape)
    modulation_bias_gradient = jnp.sum(every.astype(F32), axis=0).reshape(6, width)
    groups = condition.shape[0]
    ours = lax.dynamic_slice_in_dim(every, lax.axis_index("dp") * groups, groups, axis=0)
    silu_back = lax.psum(dot_nt(ours, modulator), COLS)
    silu_pull = jax.vjp(jax.nn.silu, condition_float)[1]
    condition_gradient = silu_pull(silu_back)[0]

    return (
        net.collect(output),
        net.collect(tokens_back).astype(F32),
        condition_gradient,
        modulation_weight_gradient,
        modulation_bias_gradient,
        in_parts.reshape(parts, width, 3, LANES)
        .transpose(1, 2, 0, 3)
        .reshape(input_weight.shape),
        row_found[:, : 2 * LANES]
        .reshape(parts, 2, LANES)
        .transpose(1, 0, 2)
        .reshape(input_bias.shape),
        out_parts[:, :, units:].transpose(0, 2, 1).reshape(output_weight.shape),
        col_found[0],
        out_parts[:, :, :units].transpose(1, 0, 2).reshape(expand_weight.shape),
        row_found[:, 2 * LANES :].reshape(expand_bias.shape),
        shrink_parts.transpose(0, 2, 1).reshape(shrink_weight.shape),
        col_found[1],
    )


def solution(mesh):
    dp, row, col = (mesh.shape[name] for name in ("dp", "row", "col"))

    def run(*arrays):
        latents = arrays[0].shape[0] // (dp * row * LENGTH)
        group = 2 * latents
        refined = Mesh(
            mesh.devices.reshape(dp, row // 2, 2, group, col // group),
            ("dp", "y", "core", "lat", "sub"),
        )
        fast = (dp, row, col, latents) == (2, 4, 4, 2)
        token = P(("dp", *ROWS), COLS)
        weights = (
            P(ROWS, None, COLS),
            P(None, COLS),
            P(COLS, None, ROWS),
            P(None, ROWS),
            P(ROWS, COLS),
            P(COLS),
            P(COLS, ROWS),
            P(ROWS),
            P(ROWS, COLS),
            P(COLS),
        )
        given = P("dp", ROWS)
        return jax.shard_map(
            functools.partial(body, fast),
            mesh=refined,
            in_specs=(token, given, *weights, token),
            out_specs=(token, token, given, *weights),
            check_vma=False,
        )(*arrays)

    return run
```

```python
import functools
import math

import jax
import jax.numpy as jnp
from jax import lax
from jax.experimental import pallas as pl
from jax.experimental.layout import Layout, with_layout_constraint
from jax.experimental.pallas import tpu as pltpu
from jax.sharding import Mesh
from jax.sharding import PartitionSpec as P

HEAD_DIM = 64
LENGTH = 1024
EPS = 1e-06
LANES = 128
SCALE = HEAD_DIM ** (-0.5)
SCALE_LOG2 = SCALE * math.log2(math.e)
ROWS = ("y", "core")
COLS = ("lat", "sub")
NT = (((1,), (1,)), ((), ()))
F32 = jnp.float32
BF16 = jnp.bfloat16
VMEM_LIMIT = 56 * 1024 * 1024
LAST = []


def dot(left, right):
    return jnp.dot(left, right, preferred_element_type=F32)


def dot_nt(left, right):
    return lax.dot_general(left, right, NT, preferred_element_type=F32)


def gelu_tanh(values):
    return (
        0.5
        * values
        * (1.0 + jnp.tanh(0.7978845608028654 * (values + 0.044715 * values * values * values)))
    )


def gelu_slope(values):
    inner = jnp.tanh(0.7978845608028654 * (values + 0.044715 * values * values * values))
    rate = 0.7978845608028654 * (1.0 + 3 * 0.044715 * values * values)
    return 0.5 * (1.0 + inner) + 0.5 * values * (1.0 - inner * inner) * rate


def whole(shape):
    return pl.BlockSpec(shape, lambda *_: (0,) * len(shape))


def fixed(shape):
    return pl.BlockSpec(
        shape, lambda *_: (0,) * len(shape), pipeline_mode=pl.Buffered(1)
    )


def block(shape, column=0, first=0, step=1):
    return pl.BlockSpec((None, *shape), lambda b, *_: (first + step * b, 0, column))


def tabled(shape, place, start=0):
    row, column = place

    def index(b, table):
        return table[row, b], 0, start if column is None else start + table[column, b]

    return pl.BlockSpec((None, *shape), index)


def call(name, kernel, grid, in_specs, out_specs, out_shape, scratch=(), table=None):
    run = pl.pallas_call(
        kernel,
        grid_spec=pltpu.PrefetchScalarGridSpec(
            num_scalar_prefetch=0 if table is None else 1,
            grid=grid,
            in_specs=in_specs,
            out_specs=out_specs,
            scratch_shapes=list(scratch),
        ),
        out_shape=out_shape,
        compiler_params=pltpu.CompilerParams(vmem_limit_bytes=VMEM_LIMIT),
        cost_estimate=pl.CostEstimate(flops=0, bytes_accessed=0, transcendentals=0),
        name=name,
    )

    def ordered(first, *others):
        first = after(first, *LAST)
        found = run(first, *others) if table is None else run(table, first, *others)
        LAST[:] = jax.tree.leaves(found)[:1]
        return found

    return ordered


def after(value, *others):
    return lax.optimization_barrier((value, *others))[0]


def shaped(shape, dtype):
    return jax.ShapeDtypeStruct(shape, dtype)


def project(left, query_blocks, kv_blocks, bias):
    number, features, _ = query_blocks.shape
    rows = left.shape[0]

    def kernel(a, g, h, c, query, kv):
        query[...] = (dot(a[...], g[...]) + c[:, :LANES]).astype(BF16)
        kv[:, :LANES] = dot(a[...], h[:, :LANES]).astype(BF16)
        kv[:, LANES:] = (dot(a[...], h[:, LANES:]) + c[:, LANES : 2 * LANES]).astype(BF16)

    return call(
        "project",
        kernel,
        (number,),
        [
            fixed(left.shape),
            block((features, LANES)),
            block((features, 2 * LANES)),
            block((1, bias.shape[-1])),
        ],
        [block((rows, LANES)), block((rows, 2 * LANES))],
        [shaped((number, rows, LANES), BF16), shaped((number, rows, 2 * LANES), BF16)],
    )(left, query_blocks, kv_blocks, bias)


def feed_forward(left, late, bias, parts, extras):
    number, _, width = bias.shape
    rows, features = left.shape

    def late_block(start):
        return pl.BlockSpec(
            (None, features, width), lambda b: (b // parts, 0, start + b % parts)
        )

    def kernel(a, g, h, c, middle, cotangent, vectors, expanded, hidden, output, sums, total):
        out = dot(a[...], g[...]) + c[...]
        expanded[...] = out
        low = gelu_tanh(out).astype(BF16)
        hidden[...] = low
        out = dot_nt(low, h[...])

        @pl.when(pl.program_id(0) == 0)
        def _():
            total[...] = out

        @pl.when(pl.program_id(0) > 0)
        def _():
            total[...] += out

        @pl.when(pl.program_id(0) == number - 1)
        def _():
            finish_output(total, (middle, cotangent, vectors), (output, sums))

    return call(
        "feed_forward",
        kernel,
        (number,),
        [fixed(left.shape), late_block(0), late_block(parts), block((1, width))]
        + [fixed(extra.shape) for extra in extras],
        [
            block((rows, width)),
            block((rows, width)),
            whole((rows, features)),
            whole((1, features)),
        ],
        [
            shaped((number, rows, width), F32),
            shaped((number, rows, width), BF16),
            shaped((rows, features), BF16),
            shaped((1, features), F32),
        ],
        scratch=[pltpu.VMEM((rows, features), F32)],
    )(left, late, late, bias, *extras)


def feed_back(name, low, turned, late, expanded, hidden, table, parts, extras, before, apart):
    _, rows, width = expanded.shape
    features = low.shape[1]
    number = table.shape[1]
    count = number // 2 if apart else 1
    more = [] if before is None else [before]

    def kernel(table_ref, *refs):
        low, turned_low, turned_in, shrink, grow, before_act, after_act = refs[:7]
        refs = list(refs[7:])
        start = [refs.pop(0) for _ in more]
        given = [refs.pop(0) for _ in extras]
        shrink_outs = [refs.pop(0) for _ in range(count)]
        expand_outs = [refs.pop(0) for _ in range(count)]
        sums = refs.pop(0)
        results, total = (refs[:-1], refs[-1]) if extras else (None, refs[0])
        step = pl.program_id(0)
        back = dot(low[...], shrink[...]) * gelu_slope(before_act[...])
        back = back.astype(BF16)
        sums[...] = jnp.sum(back.astype(F32), axis=0, keepdims=True)
        found = dot(turned_low[...], after_act[...]).astype(BF16)
        grown = dot(turned_in[...], back).astype(BF16)
        if apart:
            for index in range(count):

                @pl.when(step // 2 == index)
                def _():
                    shrink_outs[index][...] = found
                    expand_outs[index][...] = grown

        else:
            shrink_outs[0][...] = found
            expand_outs[0][...] = grown
        out = dot_nt(back, grow[...])

        @pl.when(step == 0)
        def _():
            total[...] = out + start[0][...] if start else out

        @pl.when(step > 0)
        def _():
            total[...] += out

        if extras:

            @pl.when(step == number - 1)
            def _():
                finish_middle_back(total, given, results)

    weight = (features, width)
    ends = [shaped((number, 1, width), F32)]
    end_specs = [block((1, width))]
    if extras:
        ends += [
            shaped((rows, features), F32),
            shaped((rows, features), BF16),
            shaped((features, rows), BF16),
            shaped((4, features), F32),
        ]
    else:
        ends += [shaped((rows, features), F32)]
    end_specs += [whole(one.shape) for one in ends[1:]]
    if apart:
        outs = [shaped((2, *weight), BF16)] * number
        out_specs = [
            pl.BlockSpec(
                (None, *weight), lambda b, _, at=at: (jnp.clip(b - 2 * at, 0, 1), 0, 0)
            )
            for at in range(count)
        ] * 2
    else:
        outs, out_specs = [shaped((number, *weight), BF16)] * 2, [block(weight)] * 2
    got = call(
        name,
        kernel,
        (number,),
        [
            fixed(low.shape),
            *[fixed(one.shape) for one in turned],
            tabled(weight, (1, 2), parts),
            tabled(weight, (1, 2), 0),
            tabled((rows, width), (0, None)),
            tabled((rows, width), (0, None)),
        ]
        + [fixed(one.shape) for one in (*more, *extras)],
        out_specs + end_specs,
        outs + ends,
        scratch=[pltpu.VMEM((rows, features), F32)] if extras else (),
        table=table,
    )(low, *turned, late, late, expanded, hidden, *more, *extras)
    return got[:count], got[count : 2 * count], got[2 * count :]


def add_up(name, blocks, upper=None):
    _, features, width = blocks[0][0][0].shape
    tile = min(features if upper is None else features // 2, 512)
    terms = [one for block_terms in blocks for one in block_terms]
    count = len(blocks)

    def kernel(*refs):
        if upper is not None:
            refs = refs[1:]
        given = list(refs[: len(terms)]) if upper is None else list(refs[: 2 * len(terms)])
        outs = refs[len(given) :]

        def total(number):
            return sum(given.pop(0)[...].astype(F32) for _ in range(number)).astype(BF16)

        if upper is None:
            for index, one in enumerate(blocks):
                outs[0][index] = total(len(one))
        else:
            for out in outs:
                out[...] = total(len(terms))

    def spec(index, side=None):
        if side is None:
            return pl.BlockSpec((None, tile, width), lambda i: (index, i, 0))
        half = features // 2 // tile
        if side == 0:
            return pl.BlockSpec((None, tile, width), lambda i, t: (index, t[0] * half + i, 0))
        return pl.BlockSpec((None, tile, width), lambda i, t: (index, (1 - t[0]) * half + i, 0))

    arrays = [array for array, _ in terms]
    if upper is None:
        return call(
            name,
            kernel,
            (features // tile,),
            [spec(index) for _, index in terms],
            pl.BlockSpec((count, tile, width), lambda i: (0, i, 0)),
            shaped((count, features, width), BF16),
        )(*arrays)
    return call(
        name,
        kernel,
        (features // 2 // tile,),
        [spec(index, 0) for _, index in terms] + [spec(index, 1) for _, index in terms],
        [pl.BlockSpec((tile, width), lambda i, _: (i, 0))] * 2,
        [shaped((features // 2, width), BF16)] * 2,
        table=jnp.full((1,), upper, jnp.int32),
    )(*arrays, *arrays)


def attended_backward(left, late, table, start):
    number = table.shape[1]
    rows, features = left.shape

    def kernel(_, a, g, out):
        out[...] = dot(a[...], g[...]).astype(BF16)

    return call(
        "attended_back",
        kernel,
        (number,),
        [fixed(left.shape), tabled((features, LANES), (0, 1), start)],
        block((rows, LANES)),
        shaped((number, rows, LANES), BF16),
        table=table,
    )(left, late)


def contract(name, terms, extras, finish, outs, table=None):
    number, rows, _ = terms[0][0].shape
    features = terms[0][1].shape[1]
    count, more = len(terms), len(extras)

    def kernel(*refs):
        refs = refs if table is None else refs[1:]
        lefts, rights = refs[:count], refs[count : 2 * count]
        given = refs[2 * count : 2 * count + more]
        results, total = refs[2 * count + more : -1], refs[-1]
        out = dot_nt(lefts[0][...], rights[0][...])
        for left, right in zip(lefts[1:], rights[1:]):
            out = out + dot_nt(left[...], right[...])
        step = pl.program_id(0)

        @pl.when(step == 0)
        def _():
            total[...] = out

        @pl.when(step > 0)
        def _():
            total[...] += out

        @pl.when(step == number - 1)
        def _():
            finish(total, given, results)

    return call(
        name,
        kernel,
        (number,),
        [block(left.shape[1:]) for left, _, _ in terms]
        + [where(features, left.shape[2]) for left, _, where in terms]
        + [fixed(extra.shape) for extra in extras],
        [whole(out.shape) for out in outs],
        outs,
        scratch=[pltpu.VMEM((rows, features), F32)],
        table=table,
    )(*[left for left, _, _ in terms], *[right for _, right, _ in terms], *extras)


def by_rows(rows, sums, features, work, tile=64):
    tile = min(rows, tile)

    def step(i, totals):
        found = work(pl.ds(pl.multiple_of(i * tile, tile), tile))
        return tuple(
            total + jnp.sum(one.reshape(-1, 8, features), axis=0)
            for total, one in zip(totals, found)
        )

    zero = jnp.zeros((8, features), F32)
    totals = lax.fori_loop(0, rows // tile, step, (zero,) * sums)
    return [jnp.sum(total, axis=0, keepdims=True) for total in totals]


def normalize(values):
    average = jnp.mean(values, axis=1, keepdims=True)
    inverse = lax.rsqrt(
        jnp.mean(values * values, axis=1, keepdims=True) - average * average + EPS
    )
    return (values - average) * inverse, inverse


def norm_back(incoming, normed, inverse):
    return inverse * (
        incoming
        - jnp.mean(incoming, axis=1, keepdims=True)
        - normed * jnp.mean(incoming * normed, axis=1, keepdims=True)
    )


def enter(tokens, vectors):
    rows, features = tokens.shape

    def kernel(tokens, vectors, low, turned):
        shift, scale = vectors[0:1], 1.0 + vectors[1:2]

        def work(here):
            values = normalize(tokens[here, :].astype(F32))[0] * scale + shift
            values = values.astype(BF16)
            low[here, :] = values
            turned[:, here] = values.T
            return ()

        by_rows(rows, 0, features, work, LANES)

    return call(
        "enter",
        kernel,
        (1,),
        [whole(tokens.shape), whole(vectors.shape)],
        [whole((rows, features)), whole((features, rows))],
        [shaped((rows, features), BF16), shaped((features, rows), BF16)],
    )(tokens, vectors)


def enter_back(cotangent, vectors):
    rows, features = cotangent.shape

    def kernel(cotangent, vectors, low, turned, sums):
        gate = vectors[5:6]

        def work(here):
            values = (gate * cotangent[here, :].astype(F32)).astype(BF16)
            low[here, :] = values
            turned[:, here] = values.T
            return (values.astype(F32),)

        (sums[...],) = by_rows(rows, 1, features, work, LANES)

    return call(
        "enter_back",
        kernel,
        (1,),
        [whole(cotangent.shape), whole(vectors.shape)],
        [whole((rows, features)), whole((features, rows)), whole((1, features))],
        [
            shaped((rows, features), BF16),
            shaped((features, rows), BF16),
            shaped((1, features), F32),
        ],
    )(cotangent, vectors)


def finish_middle(total, given, results):
    tokens, vectors = given
    branch, middle, low, turned = results
    rows, features = total.shape
    shift, scale, gate = vectors[3:4], 1.0 + vectors[4:5], vectors[2:3]
    bias = vectors[6:7]

    def work(here):
        one = total[here, :] + bias
        branch[here, :] = one
        values = tokens[here, :].astype(F32) + gate * one
        middle[here, :] = values
        values = (normalize(values)[0] * scale + shift).astype(BF16)
        low[here, :] = values
        turned[:, here] = values.T
        return ()

    by_rows(rows, 0, features, work, LANES)


def finish_output(total, given, results):
    middle, cotangent, vectors = given
    output, sums = results
    rows, features = total.shape
    gate, bias = vectors[5:6], vectors[7:8]

    def work(here):
        two = total[here, :] + bias
        output[here, :] = (middle[here, :] + gate * two).astype(BF16)
        return (two * cotangent[here, :].astype(F32),)

    (gate_back,) = by_rows(rows, 1, features, work)
    sums[...] = gate_back


def finish_middle_back(total, given, results):
    middle, branch, cotangent, vectors = given
    middle_back, low, turned, sums = results
    rows, features = total.shape
    gate, scale = vectors[2:3], 1.0 + vectors[4:5]

    def work(here):
        back = total[here, :]
        normed, inverse = normalize(middle[here, :])
        out = cotangent[here, :].astype(F32) + norm_back(back * scale, normed, inverse)
        middle_back[here, :] = out
        rounded = (gate * out).astype(BF16)
        low[here, :] = rounded
        turned[:, here] = rounded.T
        return back, back * normed, branch[here, :] * out, rounded.astype(F32)

    sums[...] = jnp.concatenate(by_rows(rows, 4, features, work, LANES), axis=0)


def finish_tokens_back(total, given, results):
    tokens, middle_back, vectors = given
    tokens_back, sums = results
    rows, features = total.shape
    scale = 1.0 + vectors[1:2]

    def work(here):
        back = total[here, :]
        normed, inverse = normalize(tokens[here, :].astype(F32))
        out = middle_back[here, :] + norm_back(back * scale, normed, inverse)
        tokens_back[here, :] = out.astype(BF16)
        return back, back * normed

    sums[...] = jnp.concatenate(by_rows(rows, 2, features, work), axis=0)


def chosen(parts):
    found = parts[0][...]
    for index, part in enumerate(parts[1:], 1):
        found = jnp.where(pl.program_id(0) == index, part[...], found)
    return found


def gradients(name, pairs, count, first=0, table=None, adds=(), form="one"):
    features, rows = pairs[0][0].shape
    parts = [one for _, parts in pairs for one in parts]
    width = sum(one.shape[2] for one in parts)
    lefts, rights = len(pairs), len(parts)
    given = [one for add in adds for one in add]

    def kernel(*refs):
        if table is not None:
            table_ref, *refs = refs
        left_refs = refs[:lefts]
        right_refs = list(refs[lefts : lefts + rights])
        add_refs = list(refs[lefts + rights : lefts + rights + len(given)])
        outs = refs[lefts + rights + len(given) :]
        found = []
        for left, (_, own) in zip(left_refs, pairs):
            for _ in own:
                found.append(dot(left[...], right_refs.pop(0)[...]))
        out = found[0] if len(found) == 1 else jnp.concatenate(found, axis=1)
        for add in adds:
            out = out + chosen([add_refs.pop(0) for _ in add]).astype(F32)
        out = out.astype(BF16)
        if form == "one":
            outs[0][...] = out
        elif form == "apart":
            for index, one in enumerate(outs):

                @pl.when(pl.program_id(0) == index)
                def _():
                    one[...] = out

        else:
            half = features // 2
            for index in range(2):

                @pl.when(table_ref[1, 0] == index)
                def _():
                    outs[index][...] = out[:half]
                    outs[1 - index][...] = out[half:]

    def right_spec(one):
        if table is None or form == "halves" and first is not None:
            return block(one.shape[1:], 0, first)
        return tabled(one.shape[1:], (0, None))

    def addend(one):
        array, index = one
        return pl.BlockSpec((None, *array.shape[1:]), lambda *_: (index, 0, 0))

    if form == "one":
        out_specs, shape = [block((features, width))], (count, features, width)
    else:
        shape = (features // (2 if form == "halves" else 1), width)
        out_specs = [whole(shape)] * (2 if form == "halves" else count)
    got = call(
        name,
        kernel,
        (count,),
        [fixed(left.shape) for left, _ in pairs]
        + [right_spec(one) for one in parts]
        + [addend(one) for one in given],
        out_specs,
        [shaped(shape, BF16)] * len(out_specs),
        table=table,
    )(*[left for left, _ in pairs], *parts, *[array for array, _ in given])
    return got[0] if form == "one" else got


def attend(queries, pieces):
    number, rows, _ = queries.shape
    count = len(pieces)
    keys = sum(piece.shape[1] for piece in pieces)
    tile = min(rows, 256)

    def kernel(*refs):
        query, kv = refs[0], refs[1 : 1 + count]
        out_ref, log_ref = refs[1 + count :]
        head = lax.broadcasted_iota(jnp.int32, (1, LANES), 1) < HEAD_DIM
        for start in range(0, rows, tile):
            here = slice(start, start + tile)
            both = query[here, :]
            outs, logs = [], []
            for keep in (head, ~head):
                one = jnp.where(keep, both, jnp.zeros_like(both))
                scores = [dot_nt(one, piece[:, :LANES]) for piece in kv]
                top = functools.reduce(
                    jnp.maximum, [jnp.max(s, axis=1, keepdims=True) for s in scores]
                )
                weights = [jnp.exp2((s - top) * SCALE_LOG2) for s in scores]
                total = sum(jnp.sum(w, axis=1, keepdims=True) for w in weights)
                inverse = 1.0 / total
                out = sum(
                    dot((w * inverse).astype(BF16), piece[:, LANES:])
                    for w, piece in zip(weights, kv)
                )
                outs.append(out)
                logs.append(top * SCALE_LOG2 + jnp.log(total) * math.log2(math.e))
            out_ref[here, :] = jnp.where(head, outs[0], outs[1]).astype(BF16)
            table = jnp.where(head, logs[0], logs[1]).T
            log_ref[0:1, here] = table[0:1]
            log_ref[1:2, here] = table[HEAD_DIM : HEAD_DIM + 1]

    return call(
        "attend",
        kernel,
        (number,),
        [block((rows, LANES))] + [block((piece.shape[1], 2 * LANES)) for piece in pieces],
        [block((rows, LANES)), block((2, rows))],
        [shaped((number, rows, LANES), BF16), shaped((number, 2, rows), F32)],
    )(queries, *pieces)


def attend_back(queries, pieces, logs, incoming, first, kinds):
    number, rows, _ = queries.shape
    count = len(pieces)
    keys = sum(piece.shape[1] for piece in pieces)
    tile = min(rows, 256)

    def kernel(*refs):
        query, back_ref, log_ref = refs[:3]
        kv = refs[3 : 3 + count]
        query_back = refs[3 + count]
        kv_back = refs[4 + count : 4 + 2 * count]
        sums, scratch = refs[4 + 2 * count], refs[5 + 2 * count :]
        head = lax.broadcasted_iota(jnp.int32, (1, LANES), 1) < HEAD_DIM
        turned = [piece[:, :LANES].T for piece in kv]
        top = lax.broadcasted_iota(jnp.int32, (LANES, 1), 0) < HEAD_DIM
        query_sum = jnp.zeros((1, LANES), F32)
        for start in range(0, rows, tile):
            here = slice(start, start + tile)
            backs = []
            for index, keep in enumerate((head, ~head)):
                zero = jnp.zeros((tile, LANES), BF16)
                one = jnp.where(keep, query[here, :], zero)
                back = jnp.where(keep, back_ref[here, :], zero)
                log = log_ref[index : index + 1, here]
                chances, mixes = [], []
                for piece in kv:
                    scores = dot_nt(piece[:, :LANES], one)
                    chances.append(jnp.exp2(scores * SCALE_LOG2 - log))
                    mixes.append(dot_nt(piece[:, LANES:], back))
                centre = sum(
                    jnp.sum(p * m, axis=0, keepdims=True) for p, m in zip(chances, mixes)
                )
                total = None
                for i in range(count):
                    score_back = (chances[i] * (mixes[i] - centre)).astype(BF16)
                    key_back = dot(score_back, one) * SCALE
                    value_back = dot(chances[i].astype(BF16), back)
                    if start == 0 and index == 0:
                        scratch[i][:, :LANES] = key_back
                        scratch[i][:, LANES:] = value_back
                    else:
                        scratch[i][:, :LANES] += key_back
                        scratch[i][:, LANES:] += value_back
                    term = dot(turned[i], score_back)
                    total = term if total is None else total + term
                backs.append(total)
            both = (jnp.where(top, backs[0], backs[1]).T * SCALE).astype(BF16)
            query_back[here, :] = both
            query_sum = query_sum + jnp.sum(both.astype(F32), axis=0, keepdims=True)
        sums[...] = query_sum
        for out, held in zip(kv_back, scratch):
            out[...] = held[...].astype(out.dtype)

    return call(
        "attend_back",
        kernel,
        (number,),
        [block((rows, LANES)), block((rows, LANES), first=first), block((2, rows))]
        + [block((piece.shape[1], 2 * LANES)) for piece in pieces],
        [block((rows, LANES))]
        + [block((piece.shape[1], 2 * LANES)) for piece in pieces]
        + [block((1, LANES))],
        [shaped((number, rows, LANES), BF16)]
        + [
            shaped((number, piece.shape[1], 2 * LANES), kind)
            for piece, kind in zip(pieces, kinds)
        ]
        + [shaped((number, 1, LANES), F32)],
        scratch=[pltpu.VMEM((piece.shape[1], 2 * LANES), F32) for piece in pieces],
    )(queries, incoming, logs, *pieces)


def block_at(features, width):
    return block((features, width))


class Steps:
    def __init__(self, steps):
        self.steps, self.result = steps, None
        self.got = next(steps)

    def step(self):
        if self.result is None:
            try:
                self.got = self.steps.send(self.got)
            except StopIteration as end:
                self.got = self.result = end.value

    def hold(self):
        LAST.extend(jax.tree.leaves(self.got))

    def behind(self, *values):
        (*values, self.got) = lax.optimization_barrier((*values, self.got))
        return values

    def finish(self):
        while self.result is None:
            self.step()
        return self.result


class Plain:
    def __init__(self, sizes):
        self.latents, self.parts, self.width = sizes
        self.row = lax.axis_size("y") * lax.axis_size("core")
        self.col = lax.axis_size("lat") * lax.axis_size("sub")

    def scatter(self, values, held=None):
        rows, width = values.shape
        shaped_in = values.reshape(self.latents, 2, LENGTH // 2, width)
        halves = lax.all_to_all(shaped_in, "core", 1, 0, tiled=True)
        pieces = halves.reshape(self.col, -1, width)
        pieces = lax.all_to_all(pieces, COLS, 0, 0, tiled=True)
        return pieces.transpose(1, 0, 2).reshape(-1, self.col * width), held

    def collect_start(self, values):
        rows = values.shape[0]
        pieces = values.reshape(rows, self.col, -1).transpose(1, 0, 2)
        return [lax.all_to_all(pieces, COLS, 0, 0, tiled=True)]

    def collect(self, pieces):
        (pieces,) = pieces
        halves = pieces.reshape(2 * self.latents, 1, LENGTH // 2, -1)
        back = lax.all_to_all(halves, "core", 0, 1, tiled=True)
        return back.reshape(-1, self.width)

    def modulation(self, partial, bias, row_bias, col_bias):
        group = 2 * self.latents
        ours = lax.psum(partial, "core").reshape(-1, group, partial.shape[1])
        ours = lax.psum_scatter(ours, "y", scatter_dimension=0, tiled=True)[0] + bias
        sent = jnp.repeat(ours, self.col // group, axis=0)
        got = lax.all_to_all(sent, COLS, 0, 0, tiled=True)
        got = got.reshape(self.col, 6, -1).transpose(1, 0, 2).reshape(6, -1)
        cols = lax.all_gather(col_bias, COLS, axis=1, tiled=True)
        every = lax.all_gather(row_bias, ROWS, axis=0)
        return jnp.concatenate([got, cols], axis=0), [
            every.reshape(self.row * self.parts, 1, -1)
        ]

    def gather(self, parts, held):
        del held
        every = lax.all_gather(parts, COLS, axis=1, tiled=True)
        every = lax.all_gather(every, ROWS, axis=0, tiled=True)
        return [every[:, :, :LANES]], [every[:, :, LANES:]]

    def gather_start(self, parts):
        return parts

    def gather_late(self, part):
        every = lax.all_gather(part, (*ROWS, *COLS), axis=0, tiled=True)
        return every.reshape(self.row, -1, part.shape[1])

    def expand_bias(self, row_bias, biases):
        every = lax.all_gather(row_bias, ROWS, axis=0)
        return every.reshape(self.row * self.parts, 1, -1)

    def with_units(self, row_sums, unit_sums):
        return [jnp.concatenate([row_sums[0], unit_sums[0]], axis=-1)]

    def tables(self):
        blocks = jnp.arange(self.row * self.parts, dtype=jnp.int32)
        return [jnp.stack([blocks // self.parts, blocks % self.parts])]


    def share(self, kv):
        return [[lax.all_gather(kv[0], ("core", "sub"), axis=1, tiled=True)]]

    def kinds(self):
        return [F32]

    PLACES = ((0, 0),)

    def give_back(self, backs, x):
        return [
            lax.psum_scatter(
                backs[0][0], ("core", "sub"), scatter_dimension=1, tiled=True
            ).astype(BF16)
        ]

    def sum_up(self, *args):
        return Steps(self.reduce(*args))

    def feed_back(self, low, turned, late, expanded, hidden, extras):
        blocks = jnp.arange(self.row * self.parts, dtype=jnp.int32)
        table = jnp.stack([blocks, blocks // self.parts, blocks % self.parts])
        shrink, grow, (sums, *ends) = feed_back(
            "feed_back",
            low,
            turned,
            late,
            expanded,
            hidden,
            table,
            self.parts,
            extras,
            None,
            False,
        )
        steps = [Steps(self.reduce_ready(one[0])) for one in (shrink, grow)]
        return steps, ends, [sums]

    def reduce(self, name, pairs):
        pairs = pairs[0]()
        grads = gradients(name, pairs, pairs[0][1][0].shape[0])
        return (yield from self.reduce_ready(grads))

    def reduce_ready(self, grads):
        grads = grads.astype(F32)
        grads = yield grads
        grads = lax.psum_scatter(grads, ROWS, scatter_dimension=0, tiled=True)
        grads = lax.psum_scatter(grads, COLS, scatter_dimension=1, tiled=True)
        return lax.psum(grads, "dp")

    def small(self, vectors, row_sums, col_sums):
        every = ("dp", *ROWS, *COLS)
        group = 2 * self.latents
        total = yield lax.psum(vectors, ("core", "sub"))
        total = total.astype(BF16)
        mine = lax.all_gather(total[:, None], "lat", axis=1, tiled=True)
        mine = lax.all_gather(mine, "y", axis=1, tiled=True)
        mine = lax.all_gather(mine, "dp", axis=1, tiled=True)
        col = lax.axis_index("lat") * lax.axis_size("sub") + lax.axis_index("sub")
        cut = lax.dynamic_slice_in_dim(mine, col * self.width, self.width, axis=2)
        cut = cut.transpose(1, 0, 2).reshape(mine.shape[1], -1)
        rows = lax.psum(row_sums[0], every).reshape(self.row, self.parts, -1)
        row = lax.axis_index("y") * 2 + lax.axis_index("core")
        rows = lax.dynamic_index_in_dim(rows, row, 0, keepdims=False)
        cols = lax.psum(col_sums, every)
        cols = lax.dynamic_slice_in_dim(cols, col * self.width, self.width, axis=1)
        return cut, rows, cols

    def col_sum(self, values):
        return lax.psum(values, COLS)

    def both_groups(self, values):
        return lax.all_gather(values, "dp", axis=0, tiled=True)


class Cube(Plain):
    PLACES = ((0, 0), (0, 1), (1, 0), (1, 1))

    def __init__(self, sizes):
        super().__init__(sizes)
        self.x = lax.axis_index("dp")
        self.y = lax.axis_index("y")
        self.c = lax.axis_index("core")
        self.z = lax.axis_index("lat")

    def swap(self, values, axis):
        return lax.ppermute(values, axis, [(0, 1), (1, 0)])

    def along(self, values, bits):
        return lax.ppermute(values, "lat", [(i, i ^ bits) for i in range(4)])

    def scatter(self, values, held=None):
        rows, width = values.shape
        halves = values.reshape(self.latents, 2, LENGTH // 2, width)
        keep = lax.dynamic_index_in_dim(halves, self.c, 1, keepdims=False)
        send = lax.dynamic_index_in_dim(halves, 1 - self.c, 1, keepdims=False)
        every = jnp.concatenate([keep, self.swap(send, "core")], axis=0)
        if held is not None:
            every, held = lax.optimization_barrier((every, held))
        pieces = []
        for bits in range(4):
            latent = self.z ^ bits
            index = ((latent // 2) ^ self.c) * 2 + latent % 2
            piece = lax.dynamic_index_in_dim(every, index, 0, keepdims=False)
            pieces.append(piece if bits == 0 else self.along(piece, bits))
        return jnp.concatenate(self.placed(pieces), axis=1), held

    def placed(self, pieces):
        odd, high = self.z % 2 == 1, self.z >= 2
        one, two, three, four = pieces
        one, two = jnp.where(odd, two, one), jnp.where(odd, one, two)
        three, four = jnp.where(odd, four, three), jnp.where(odd, three, four)
        return [
            jnp.where(high, three, one),
            jnp.where(high, four, two),
            jnp.where(high, one, three),
            jnp.where(high, two, four),
        ]

    def collect_start(self, values):
        width = self.width
        pieces = self.placed([values[:, i * width : (i + 1) * width] for i in range(4)])
        return [p if bits == 0 else self.along(p, bits) for bits, p in enumerate(pieces)]

    def collect(self, pieces):
        width = self.width
        every = jnp.stack(pieces)

        def latents(core):
            return jnp.stack(
                [
                    lax.dynamic_index_in_dim(every, self.z ^ (2 * core + i), 0, keepdims=False)
                    for i in range(2)
                ]
            )

        keep = latents(self.c)
        got = self.swap(latents(1 - self.c), "core")
        first = jnp.where(self.c == 0, keep, got)
        second = jnp.where(self.c == 0, got, keep)
        return jnp.stack([first, second], axis=1).reshape(-1, width)

    def modulation(self, partial, bias, row_bias, col_bias):
        span = partial.shape[1]
        own = row_bias.reshape(1, -1)
        got = self.swap(jnp.concatenate([partial, own], axis=0), "core")
        ours, other = partial + got[:-1], got[-1:]
        halves = ours.reshape(2, 4, span)
        keep = lax.dynamic_index_in_dim(halves, self.y, 0, keepdims=False)
        send = lax.dynamic_index_in_dim(halves, 1 - self.y, 0, keepdims=False)
        got = self.swap(jnp.concatenate([send, own, other], axis=0), "y")
        ours = keep + got[:4] + bias
        rows = jnp.stack([own, got[4:5], other, got[5:6]]).reshape(2, 2, 2, -1)
        flip = jnp.stack([rows[:, :, 1], rows[:, :, 0]], axis=2)
        rows = jnp.where(self.x == 0, rows, flip).transpose(2, 0, 1, 3)[:, :, :, None]
        pieces = []
        for bits in range(4):
            piece = lax.dynamic_index_in_dim(ours, self.z ^ bits, 0, keepdims=False)
            piece = jnp.concatenate([piece.reshape(6, -1), col_bias], axis=0)
            pieces.append(piece if bits == 0 else self.along(piece, bits))
        vectors = jnp.concatenate(self.placed(pieces), axis=1)
        return vectors, [rows[x, core] for x, core in self.PLACES]

    def gather_start(self, parts):
        part = lax.dynamic_index_in_dim(parts, self.x, 0, keepdims=False)
        odd, high = self.z % 2 == 1, self.z >= 2
        got = self.along(part, 1)
        part = jnp.concatenate([jnp.where(odd, got, part), jnp.where(odd, part, got)], axis=0)
        got = self.along(part, 2)
        part = jnp.concatenate(
            [jnp.where(high, got, part), jnp.where(high, part, got)], axis=0
        )

        return part

    def gather(self, part, held):
        one, two = part[:, :LANES], part[:, LANES:]
        one_pair = jnp.stack([one, self.swap(one, "dp")])
        near = jnp.stack([two, self.swap(two, "y")])
        near = after(near, one_pair, *held)
        far = self.swap(near, "dp")
        kv = [near, self.swap(near, "core"), far, self.swap(far, "core")]
        got = self.swap(one_pair, "y")
        near = jnp.stack([one_pair[0], got[0]])
        far = jnp.stack([one_pair[1], got[1]])
        queries = [near, self.swap(near, "core"), far, self.swap(far, "core")]
        return queries, kv

    def expand_bias(self, row_bias, biases):
        number = self.row * self.parts
        table = jnp.concatenate(self.tables(), axis=1)
        place = table[0] * self.parts + table[1]
        chosen = place[None, :] == lax.broadcasted_iota(jnp.int32, (number, number), 0)
        every = jnp.concatenate(biases, axis=0)[:, 0]
        found = jnp.dot(chosen.astype(F32), every, precision=lax.Precision.HIGHEST)
        return found[:, None]

    def with_units(self, row_sums, unit_sums):
        found = []
        for one, (x, core) in zip(row_sums, self.PLACES):
            units = unit_sums[1 - core][2 * x : 2 * x + 2]
            found.append(jnp.concatenate([one, units], axis=-1))
        return found

    def tables(self):
        side = jnp.arange(2, dtype=jnp.int32)
        return [
            jnp.stack(
                [(side ^ self.y) * 2 + (self.c ^ core), jnp.full((2,), self.x ^ x)]
            ).astype(jnp.int32)
            for x, core in self.PLACES
        ]

    def share(self, kv):
        return [
            [kv[2 * x + core], self.swap(kv[2 * x + 1 - core], "core")]
            for x, core in self.PLACES
        ]

    def kinds(self):
        return [F32, BF16]

    def give_back(self, backs, x):
        pair = backs[2 * x : 2 * x + 2]
        got = [self.swap(pair[1 - core][1], "core") for core in (0, 1)]
        return [(own[0] + one.astype(F32)).astype(BF16) for own, one in zip(pair, got)]

    def feed_back(self, low, turned, late, expanded, hidden, extras):
        tables = self.tables()
        found, sums, before = [], [], None
        for core in (1, 0):
            rows, parts = jnp.concatenate([tables[core], tables[2 + core]], axis=1)
            shrink, grow, (one, *ends) = feed_back(
                "feed_back",
                low,
                turned,
                late,
                expanded,
                hidden,
                jnp.stack([rows * self.parts + parts, rows, parts]),
                self.parts,
                [] if core else extras,
                before,
                core == 1,
            )
            if core:
                (before,) = ends
                found = [[self.swap(one, "core") for one in part] for part in (shrink, grow)]
            else:
                LAST.extend([one for part in found for one in part])
                steps = [
                    Steps(self.reduce_ready(name, near[0], far, order))
                    for name, near, far, order in (
                        ("d_shrink", shrink, found[0], "xy"),
                        ("d_expand", grow, found[1], "yx"),
                    )
                ]
            sums.append(one)
        return steps, ends, sums

    def reduce_ready(self, name, near, far, order):
        axes, one, two = (("dp", "y"), 2, 1) if order == "xy" else (("y", "dp"), 1, 2)
        far = [(far[x], y) for x in (0, 1) for y in (0, 1)]
        sent = add_up(name, [[(near, one), far[one]], [(near, 3), far[3]]])
        second = self.swap(sent, axes[0])
        second = yield second
        sent = add_up(name, [[(near, two), far[two], (second, 1)]])
        third = self.swap(sent, axes[1])
        third = yield third
        keep, send = add_up(
            name, [[(near, 0), far[0], (second, 0), (third, 0)]], upper=self.z // 2
        )
        return (yield from self.reduce_end(name, keep, send))

    def reduce_end(self, name, keep, other):
        got = lax.ppermute(other, "lat", [(0, 1), (3, 2)])
        got = yield got
        other = add_up(name + "_out", [[(other[None], 0), (got[None], 0)]])[0]
        got = lax.ppermute(other, "lat", [(1, 2), (2, 1)])
        got = yield got
        own, send = add_up(
            name + "_in", [[(keep[None], 0), (got[None], 0)]], upper=self.z % 2
        )
        got = self.along(send, 1)
        got = yield got
        own = (own.astype(F32) + got.astype(F32)).astype(BF16)
        got = self.swap(own, "dp")
        return jnp.stack(
            [jnp.where(self.x == 0, own, got), jnp.where(self.x == 0, got, own)]
        ).astype(F32)

    def reduce(self, name, pairs):
        def grads(places, adds=(), form="one"):
            x, y, core = places[0]
            table = None
            if form == "halves":
                table = jnp.full((2, 1), self.z // 2, jnp.int32)
            return gradients(name, pairs[2 * x + core](), len(places), y, table, adds, form)

        near = [None, None]
        for x in (1, 0):
            sent = grads([(x, 0, 1), (x, 1, 1)], form="apart")
            sent = yield [self.swap(one, "core") for one in sent]
            near[x] = [(one[None], 0) for one in sent]
            if x == 1:
                second = self.swap(grads([(1, 0, 0), (1, 1, 0)], [near[1]]), "dp")
                second = yield second
                second = [(second, 0), (second, 1)]
        third = self.swap(grads([(0, 1, 0)], [[near[0][1]], [second[1]]]), "y")
        third = yield third
        keep, send = grads(
            [(0, 0, 0)], [[near[0][0]], [second[0]], [(third, 0)]], form="halves"
        )
        return (yield from self.reduce_end(name, keep, send))

    def small(self, vectors, row_sums, col_sums):
        span = row_sums[0].shape[-1]
        features = vectors.shape[1]

        def flat(*parts):
            return jnp.concatenate([part.reshape(-1, LANES) for part in parts], axis=0)

        def cut(message, *shapes):
            parts, start = [], 0
            for shape in shapes:
                size = math.prod(shape) // LANES
                parts.append(message[start : start + size].reshape(shape))
                start += size
            return parts

        every = jnp.stack(row_sums).reshape(2, 2, 2, span)
        rows0, rows1 = every[:, 0], every[:, 1]
        got = yield self.swap(flat(rows1, col_sums, vectors), "core")
        got = cut(got, rows1.shape, col_sums.shape, vectors.shape)
        rows, cols = rows0 + got[0], col_sums + got[1]
        mine = (vectors + got[2]).astype(BF16).astype(F32)
        got = yield self.swap(flat(rows[:, 1], cols, mine), "y")
        got = cut(got, (2, span), cols.shape, mine.shape)
        rows, cols = rows[:, 0] + got[0], cols + got[1]
        pair = jnp.stack([mine, got[2]])
        got = yield self.swap(flat(rows, cols, pair), "dp")
        got = cut(got, rows.shape, cols.shape, pair.shape)
        rows = rows + jnp.stack([got[0][1], got[0][0]])
        rows = jnp.where(self.x == 0, rows, jnp.stack([rows[1], rows[0]]))
        cols = cols + got[1]
        four = jnp.stack([pair, got[2]]).reshape(4, 6, features)
        width = self.width

        def cuts(values):
            return self.placed(
                [values[..., i * width : (i + 1) * width] for i in range(4)]
            )

        found = []
        for bits, piece in enumerate(zip(cuts(four), cuts(cols))):
            piece = [*piece, rows]
            if bits:
                got = self.along(flat(*piece), bits)
                piece = cut(got, *[part.shape for part in piece])
            found.append(piece)
        tree = [(found[0][i] + found[1][i]) + (found[2][i] + found[3][i]) for i in (1, 2)]
        every = jnp.stack([one[0] for one in found])
        every = every.reshape(16, -1)
        place = lax.broadcasted_iota(jnp.int32, (16, 16), 0)
        held = lax.broadcasted_iota(jnp.int32, (16, 16), 1)
        latent = (
            (((held // 2) % 2) ^ self.x) * 8 + ((held % 2) ^ self.y) * 4 + ((held // 4) ^ self.z)
        )
        chosen = (latent == place).astype(F32)
        every = jnp.dot(chosen, every, precision=lax.Precision.HIGHEST).astype(BF16)
        return every, tree[1], tree[0]

    def col_sum(self, values):
        got = [values] + [self.along(values, bits) for bits in (1, 2, 3)]
        return (got[0] + got[1]) + (got[2] + got[3])

    def both_groups(self, values):
        got = self.swap(values, "dp")
        return jnp.where(
            self.x == 0,
            jnp.concatenate([values, got], axis=0),
            jnp.concatenate([got, values], axis=0),
        )


def body(
    fast,
    tokens,
    condition,
    modulation_weight,
    modulation_bias,
    input_weight,
    input_bias,
    output_weight,
    output_bias,
    expand_weight,
    expand_bias,
    shrink_weight,
    shrink_bias,
    cotangent,
):
    LAST.clear()
    width = tokens.shape[1]
    inner = input_weight.shape[2]
    parts = inner // LANES
    units = expand_weight.shape[1] // parts
    sizes = (tokens.shape[0] // LENGTH, parts, width)
    net = (Cube if fast else Plain)(sizes)

    own_in = (
        input_weight.reshape(width, 3, parts, LANES)
        .transpose(2, 0, 1, 3)
        .reshape(parts, width, 3 * LANES)
    )
    own_late = with_layout_constraint(
        jnp.concatenate([expand_weight, shrink_weight.T, output_weight.T], axis=1),
        Layout((0, 1)),
    )
    out_start = 2 * parts * units // LANES

    condition_float = condition.astype(F32)
    silu_low = jax.nn.silu(condition_float).astype(BF16)
    modulator = modulation_weight.reshape(modulation_weight.shape[0], -1)
    row_bias = jnp.concatenate(
        [
            input_bias.reshape(2, parts, LANES).transpose(1, 0, 2).reshape(parts, -1),
            expand_bias.reshape(parts, units),
        ],
        axis=1,
    ).astype(F32)
    late = net.gather_late(own_late)
    vectors, row_biases = net.modulation(
        dot(silu_low, modulator),
        modulation_bias.astype(F32).reshape(1, -1),
        row_bias,
        jnp.stack([output_bias, shrink_bias]).astype(F32),
    )
    own_in = net.gather_start(own_in)
    mine, own_in = net.scatter(tokens, own_in)
    query_bufs, kv_bufs = net.gather(own_in, [mine, vectors])
    rows = mine.shape[0]
    features = mine.shape[1]
    expand_biases = net.expand_bias(
        row_bias[:, 2 * LANES :], [one[..., 2 * LANES :] for one in row_biases]
    )
    tables = net.tables()

    low_one, turned_one = enter(mine, vectors)
    queries, own_kv = [], []
    for one, two, bias in zip(query_bufs, kv_bufs, row_biases):
        one, two = project(low_one, one, two, bias)
        queries.append(one)
        own_kv.append(two)
    kv = net.share(own_kv)
    back, _ = net.scatter(after(cotangent, own_kv[0]))
    attended, logs = [], []
    for one, pieces in zip(queries, kv):
        out, log = attend(one, pieces)
        attended.append(out)
        logs.append(log)

    branch_two_back, turned_two_back, shrink_sum = enter_back(back, vectors)

    def out_place(number):
        def place(features, width):
            return tabled((features, width), (2 * number, 2 * number + 1), out_start)

        return place

    branch_one, middle, low_two, turned_two = contract(
        "out",
        [(one, late, out_place(i)) for i, one in enumerate(attended)],
        [mine, vectors],
        finish_middle,
        [
            shaped((rows, features), F32),
            shaped((rows, features), F32),
            shaped((rows, features), BF16),
            shaped((features, rows), BF16),
        ],
        table=jnp.concatenate(tables, axis=0),
    )
    expanded, hidden, output, gate_two_back = feed_forward(
        low_two, late, expand_biases, parts, [middle, back, vectors]
    )
    output = net.collect_start(output)

    steps, ends, expand_sums = net.feed_back(
        branch_two_back,
        (turned_two_back, turned_two),
        late,
        expanded,
        hidden,
        [middle, branch_one, back, vectors],
    )
    middle_back, branch_one_back, turned_one_back, sums_two = ends
    shrink_steps, expand_steps = steps
    incoming = attended_backward(
        branch_one_back, late, jnp.concatenate(tables, axis=1), out_start
    )
    number = len(kv)
    query_back, backs, query_sums = [None] * number, [None] * number, [None] * number
    kv_back = [None] * number

    def attention_back(i):
        got = attend_back(
            queries[i], kv[i], logs[i], incoming, i * queries[i].shape[0], net.kinds()
        )
        query_back[i], backs[i], query_sums[i] = got[0], got[1:-1], got[-1]

    def kv_final(i):
        pair = net.give_back(backs, i // 2)
        kv_back[i : i + len(pair)] = pair

    def pair(i):
        return lambda: [
            (turned_one, [query_back[i], kv_back[i]]),
            (turned_one_back, [attended[i]]),
        ]

    half = number // 2
    for i in reversed(range(half, number)):
        attention_back(i)
    kv_final(half)
    in_steps = net.sum_up("d_in", [pair(j) for j in range(number)])
    shrink_steps.step()
    expand_steps.step()
    crossing = []
    if half:
        in_steps.step()
        crossing = [in_steps.got]
        for i in reversed(range(half)):
            if i == 0:
                shrink_steps.hold()
                expand_steps.hold()
            attention_back(i)
        shrink_steps.step()
        expand_steps.step()
        kv_final(0)
        in_steps.step()
        shrink_steps.step()
        in_steps.step()
        expand_steps.step()
    value_sums = [
        jnp.sum(one[:, :, LANES:].astype(F32), axis=1, keepdims=True) for one in kv_back
    ]
    LAST.extend(crossing)
    tokens_back, sums_one = contract(
        "tokens_back",
        [(one, buf, block_at) for one, buf in zip(query_back, query_bufs)]
        + [(one, buf, block_at) for one, buf in zip(kv_back, kv_bufs)],
        [mine, middle_back, vectors],
        finish_tokens_back,
        [shaped((rows, features), BF16), shaped((2, features), F32)],
    )
    summed = jnp.concatenate([sums_one, sums_two[2:3], sums_two[0:2], gate_two_back], axis=0)
    tokens_back = net.collect_start(tokens_back)
    shrink_steps.step()
    expand_steps.step()
    row_sums = [
        jnp.concatenate([one, two], axis=-1) for one, two in zip(query_sums, value_sums)
    ]
    row_sums = net.with_units(row_sums, expand_sums)
    col_sums = jnp.concatenate([sums_two[3:4], shrink_sum], axis=0)
    (summed,) = in_steps.behind(summed)
    small_steps = Steps(net.small(summed, row_sums, col_sums))
    in_steps.step()
    small_steps.step()
    LAST.extend(tokens_back[1:])
    small_steps.hold()
    in_steps.step()
    small_steps.step()
    small_steps.hold()
    in_steps.step()
    shrink_parts = shrink_steps.finish()
    expand_parts = expand_steps.finish()
    in_parts = in_steps.finish()

    every, row_found, col_found = small_steps.finish()
    silu_all = net.both_groups(silu_low)
    modulation_weight_gradient = lax.dot_general(
        silu_all, every, (((0,), (0,)), ((), ())), preferred_element_type=F32
    ).reshape(modulation_weight.shape)
    modulation_bias_gradient = jnp.sum(every.astype(F32), axis=0).reshape(6, width)
    groups = condition.shape[0]
    ours = lax.dynamic_slice_in_dim(every, lax.axis_index("dp") * groups, groups, axis=0)
    silu_back = net.col_sum(dot_nt(ours, modulator))
    silu_pull = jax.vjp(jax.nn.silu, condition_float)[1]
    condition_gradient = silu_pull(silu_back)[0]

    return (
        net.collect(output),
        net.collect(tokens_back).astype(F32),
        condition_gradient,
        modulation_weight_gradient,
        modulation_bias_gradient,
        in_parts[:, :, : 3 * LANES]
        .reshape(parts, width, 3, LANES)
        .transpose(1, 2, 0, 3)
        .reshape(input_weight.shape),
        row_found[:, : 2 * LANES]
        .reshape(parts, 2, LANES)
        .transpose(1, 0, 2)
        .reshape(input_bias.shape),
        in_parts[:, :, 3 * LANES :].transpose(0, 2, 1).reshape(output_weight.shape),
        col_found[0],
        expand_parts.transpose(1, 0, 2).reshape(expand_weight.shape),
        row_found[:, 2 * LANES :].reshape(expand_bias.shape),
        shrink_parts.transpose(0, 2, 1).reshape(shrink_weight.shape),
        col_found[1],
    )


def solution(mesh):
    dp, row, col = (mesh.shape[name] for name in ("dp", "row", "col"))

    def run(*arrays):
        latents = arrays[0].shape[0] // (dp * row * LENGTH)
        group = 2 * latents
        refined = Mesh(
            mesh.devices.reshape(dp, row // 2, 2, group, col // group),
            ("dp", "y", "core", "lat", "sub"),
        )
        fast = (dp, row, col, latents) == (2, 4, 4, 2)
        token = P(("dp", *ROWS), COLS)
        weights = (
            P(ROWS, None, COLS),
            P(None, COLS),
            P(COLS, None, ROWS),
            P(None, ROWS),
            P(ROWS, COLS),
            P(COLS),
            P(COLS, ROWS),
            P(ROWS),
            P(ROWS, COLS),
            P(COLS),
        )
        given = P("dp", ROWS)
        return jax.shard_map(
            functools.partial(body, fast),
            mesh=refined,
            in_specs=(token, given, *weights, token),
            out_specs=(token, token, given, *weights),
            check_vma=False,
        )(*arrays)

    return run
```

```python
import functools
import math

import jax
import jax.numpy as jnp
from jax import lax
from jax.experimental import pallas as pl
from jax.experimental.layout import Layout, with_layout_constraint
from jax.experimental.pallas import tpu as pltpu
from jax.sharding import Mesh
from jax.sharding import PartitionSpec as P

HEAD_DIM = 64
LENGTH = 1024
EPS = 1e-06
LANES = 128
SCALE = HEAD_DIM ** (-0.5)
SCALE_LOG2 = SCALE * math.log2(math.e)
ROWS = ("y", "core")
COLS = ("lat", "sub")
NT = (((1,), (1,)), ((), ()))
F32 = jnp.float32
BF16 = jnp.bfloat16
VMEM_LIMIT = 56 * 1024 * 1024
LAST = []


def dot(left, right):
    return jnp.dot(left, right, preferred_element_type=F32)


def dot_nt(left, right):
    return lax.dot_general(left, right, NT, preferred_element_type=F32)


def gelu_tanh(values):
    return (
        0.5
        * values
        * (1.0 + jnp.tanh(0.7978845608028654 * (values + 0.044715 * values * values * values)))
    )


def gelu_slope(values):
    inner = jnp.tanh(0.7978845608028654 * (values + 0.044715 * values * values * values))
    rate = 0.7978845608028654 * (1.0 + 3 * 0.044715 * values * values)
    return 0.5 * (1.0 + inner) + 0.5 * values * (1.0 - inner * inner) * rate


def whole(shape):
    return pl.BlockSpec(shape, lambda *_: (0,) * len(shape))


def fixed(shape):
    return pl.BlockSpec(
        shape, lambda *_: (0,) * len(shape), pipeline_mode=pl.Buffered(1)
    )


def block(shape, column=0, first=0, step=1):
    return pl.BlockSpec((None, *shape), lambda b, *_: (first + step * b, 0, column))


def tabled(shape, place, start=0):
    row, column = place

    def index(b, table):
        return table[row, b], 0, start if column is None else start + table[column, b]

    return pl.BlockSpec((None, *shape), index)


def call(name, kernel, grid, in_specs, out_specs, out_shape, scratch=(), table=None):
    run = pl.pallas_call(
        kernel,
        grid_spec=pltpu.PrefetchScalarGridSpec(
            num_scalar_prefetch=0 if table is None else 1,
            grid=grid,
            in_specs=in_specs,
            out_specs=out_specs,
            scratch_shapes=list(scratch),
        ),
        out_shape=out_shape,
        compiler_params=pltpu.CompilerParams(vmem_limit_bytes=VMEM_LIMIT),
        cost_estimate=pl.CostEstimate(flops=0, bytes_accessed=0, transcendentals=0),
        name=name,
    )

    def ordered(first, *others):
        first = after(first, *LAST)
        found = run(first, *others) if table is None else run(table, first, *others)
        LAST[:] = jax.tree.leaves(found)[:1]
        return found

    return ordered


def after(value, *others):
    return lax.optimization_barrier((value, *others))[0]


def shaped(shape, dtype):
    return jax.ShapeDtypeStruct(shape, dtype)


def gate(values):
    def kernel(given, out):
        out[...] = given[...]

    return call(
        "gate", kernel, (1,), [whole(values.shape)], whole(values.shape), shaped(values.shape, values.dtype)
    )(values)


def project(left, query_blocks, kv_blocks, bias):
    number, features, _ = query_blocks.shape
    rows = left.shape[0]

    def kernel(a, g, h, c, query, kv):
        query[...] = (dot(a[...], g[...]) + c[:, :LANES]).astype(BF16)
        kv[:, :LANES] = dot(a[...], h[:, :LANES]).astype(BF16)
        kv[:, LANES:] = (dot(a[...], h[:, LANES:]) + c[:, LANES : 2 * LANES]).astype(BF16)

    return call(
        "project",
        kernel,
        (number,),
        [
            fixed(left.shape),
            block((features, LANES)),
            block((features, 2 * LANES)),
            block((1, bias.shape[-1])),
        ],
        [block((rows, LANES)), block((rows, 2 * LANES))],
        [shaped((number, rows, LANES), BF16), shaped((number, rows, 2 * LANES), BF16)],
    )(left, query_blocks, kv_blocks, bias)


def feed_forward(left, late, bias, parts, extras):
    number, _, width = bias.shape
    rows, features = left.shape

    def late_block(start):
        return pl.BlockSpec(
            (None, features, width), lambda b: (b // parts, 0, start + b % parts)
        )

    def kernel(a, g, h, c, middle, cotangent, vectors, expanded, hidden, output, sums, total):
        out = dot(a[...], g[...]) + c[...]
        expanded[...] = out
        low = gelu_tanh(out).astype(BF16)
        hidden[...] = low
        out = dot_nt(low, h[...])

        @pl.when(pl.program_id(0) == 0)
        def _():
            total[...] = out

        @pl.when(pl.program_id(0) > 0)
        def _():
            total[...] += out

        @pl.when(pl.program_id(0) == number - 1)
        def _():
            finish_output(total, (middle, cotangent, vectors), (output, sums))

    return call(
        "feed_forward",
        kernel,
        (number,),
        [fixed(left.shape), late_block(0), late_block(parts), block((1, width))]
        + [fixed(extra.shape) for extra in extras],
        [
            block((rows, width)),
            block((rows, width)),
            whole((rows, features)),
            whole((1, features)),
        ],
        [
            shaped((number, rows, width), F32),
            shaped((number, rows, width), BF16),
            shaped((rows, features), BF16),
            shaped((1, features), F32),
        ],
        scratch=[pltpu.VMEM((rows, features), F32)],
    )(left, late, late, bias, *extras)


def feed_back(name, low, turned, late, expanded, hidden, table, parts, extras, before, apart):
    _, rows, width = expanded.shape
    features = low.shape[1]
    number = table.shape[1]
    count = number // 2 if apart else 1
    more = [] if before is None else [before]

    def kernel(table_ref, *refs):
        low, turned_low, turned_in, shrink, grow, before_act, after_act = refs[:7]
        refs = list(refs[7:])
        start = [refs.pop(0) for _ in more]
        given = [refs.pop(0) for _ in extras]
        shrink_outs = [refs.pop(0) for _ in range(count)]
        expand_outs = [refs.pop(0) for _ in range(count)]
        sums = refs.pop(0)
        results, total = (refs[:-1], refs[-1]) if extras else (None, refs[0])
        step = pl.program_id(0)
        back = dot(low[...], shrink[...]) * gelu_slope(before_act[...])
        back = back.astype(BF16)
        sums[...] = jnp.sum(back.astype(F32), axis=0, keepdims=True)
        found = dot(turned_low[...], after_act[...]).astype(BF16)
        grown = dot(turned_in[...], back).astype(BF16)
        if apart:
            for index in range(count):

                @pl.when(step // 2 == index)
                def _():
                    shrink_outs[index][...] = found
                    expand_outs[index][...] = grown

        else:
            shrink_outs[0][...] = found
            expand_outs[0][...] = grown
        out = dot_nt(back, grow[...])

        @pl.when(step == 0)
        def _():
            total[...] = out + start[0][...] if start else out

        @pl.when(step > 0)
        def _():
            total[...] += out

        if extras:

            @pl.when(step == number - 1)
            def _():
                finish_middle_back(total, given, results)

    weight = (features, width)
    ends = [shaped((number, 1, width), F32)]
    end_specs = [block((1, width))]
    if extras:
        ends += [
            shaped((rows, features), F32),
            shaped((rows, features), BF16),
            shaped((features, rows), BF16),
            shaped((4, features), F32),
        ]
    else:
        ends += [shaped((rows, features), F32)]
    end_specs += [whole(one.shape) for one in ends[1:]]
    if apart:
        outs = [shaped((2, *weight), BF16)] * number
        out_specs = [
            pl.BlockSpec(
                (None, *weight), lambda b, _, at=at: (jnp.clip(b - 2 * at, 0, 1), 0, 0)
            )
            for at in range(count)
        ] * 2
    else:
        outs, out_specs = [shaped((number, *weight), BF16)] * 2, [block(weight)] * 2
    got = call(
        name,
        kernel,
        (number,),
        [
            fixed(low.shape),
            *[fixed(one.shape) for one in turned],
            tabled(weight, (1, 2), parts),
            tabled(weight, (1, 2), 0),
            tabled((rows, width), (0, None)),
            tabled((rows, width), (0, None)),
        ]
        + [fixed(one.shape) for one in (*more, *extras)],
        out_specs + end_specs,
        outs + ends,
        scratch=[pltpu.VMEM((rows, features), F32)] if extras else (),
        table=table,
    )(low, *turned, late, late, expanded, hidden, *more, *extras)
    return got[:count], got[count : 2 * count], got[2 * count :]


def add_up(name, blocks, upper=None):
    _, features, width = blocks[0][0][0].shape
    tile = min(features if upper is None else features // 2, 512)
    terms = [one for block_terms in blocks for one in block_terms]
    count = len(blocks)

    def kernel(*refs):
        if upper is not None:
            refs = refs[1:]
        given = list(refs[: len(terms)]) if upper is None else list(refs[: 2 * len(terms)])
        outs = refs[len(given) :]

        def total(number):
            return sum(given.pop(0)[...].astype(F32) for _ in range(number)).astype(BF16)

        if upper is None:
            for index, one in enumerate(blocks):
                outs[0][index] = total(len(one))
        else:
            for out in outs:
                out[...] = total(len(terms))

    def spec(index, side=None):
        if side is None:
            return pl.BlockSpec((None, tile, width), lambda i: (index, i, 0))
        half = features // 2 // tile
        if side == 0:
            return pl.BlockSpec((None, tile, width), lambda i, t: (index, t[0] * half + i, 0))
        return pl.BlockSpec((None, tile, width), lambda i, t: (index, (1 - t[0]) * half + i, 0))

    arrays = [array for array, _ in terms]
    if upper is None:
        return call(
            name,
            kernel,
            (features // tile,),
            [spec(index) for _, index in terms],
            pl.BlockSpec((count, tile, width), lambda i: (0, i, 0)),
            shaped((count, features, width), BF16),
        )(*arrays)
    return call(
        name,
        kernel,
        (features // 2 // tile,),
        [spec(index, 0) for _, index in terms] + [spec(index, 1) for _, index in terms],
        [pl.BlockSpec((tile, width), lambda i, _: (i, 0))] * 2,
        [shaped((features // 2, width), BF16)] * 2,
        table=jnp.full((1,), upper, jnp.int32),
    )(*arrays, *arrays)


def attended_backward(left, late, table, start):
    number = table.shape[1]
    rows, features = left.shape

    def kernel(_, a, g, out):
        out[...] = dot(a[...], g[...]).astype(BF16)

    return call(
        "attended_back",
        kernel,
        (number,),
        [fixed(left.shape), tabled((features, LANES), (0, 1), start)],
        block((rows, LANES)),
        shaped((number, rows, LANES), BF16),
        table=table,
    )(left, late)


def contract(name, terms, extras, finish, outs, table=None):
    terms = [(left if isinstance(left, list) else [left], *more) for left, *more in terms]
    number = max(len(left) * left[0].shape[0] for left, _, _ in terms)
    rows = terms[0][0][0].shape[1]
    features = terms[0][1].shape[1]
    count, more = len(terms), len(extras)
    given_lefts = [one for left, _, _ in terms for one in left]

    def kernel(*refs):
        refs = list(refs if table is None else refs[1:])
        lefts = [chosen([refs.pop(0) for _ in left]) for left, _, _ in terms]
        rights = refs[:count]
        given = refs[count : count + more]
        results, total = refs[count + more : -1], refs[-1]
        out = dot_nt(lefts[0], rights[0][...])
        for left, right in zip(lefts[1:], rights[1:]):
            out = out + dot_nt(left, right[...])
        step = pl.program_id(0)

        @pl.when(step == 0)
        def _():
            total[...] = out

        @pl.when(step > 0)
        def _():
            total[...] += out

        @pl.when(step == number - 1)
        def _():
            finish(total, given, results)

    return call(
        name,
        kernel,
        (number,),
        [
            block(one.shape[1:], step=0 if len(left) > 1 else 1)
            for left, _, _ in terms
            for one in left
        ]
        + [where(features, left[0].shape[2]) for left, _, where in terms]
        + [fixed(extra.shape) for extra in extras],
        [whole(out.shape) for out in outs],
        outs,
        scratch=[pltpu.VMEM((rows, features), F32)],
        table=table,
    )(*given_lefts, *[right for _, right, _ in terms], *extras)


def by_rows(rows, sums, features, work, tile=64):
    tile = min(rows, tile)

    def step(i, totals):
        found = work(pl.ds(pl.multiple_of(i * tile, tile), tile))
        return tuple(
            total + jnp.sum(one.reshape(-1, 8, features), axis=0)
            for total, one in zip(totals, found)
        )

    zero = jnp.zeros((8, features), F32)
    totals = lax.fori_loop(0, rows // tile, step, (zero,) * sums)
    return [jnp.sum(total, axis=0, keepdims=True) for total in totals]


def normalize(values):
    average = jnp.mean(values, axis=1, keepdims=True)
    inverse = lax.rsqrt(
        jnp.mean(values * values, axis=1, keepdims=True) - average * average + EPS
    )
    return (values - average) * inverse, inverse


def norm_back(incoming, normed, inverse):
    return inverse * (
        incoming
        - jnp.mean(incoming, axis=1, keepdims=True)
        - normed * jnp.mean(incoming * normed, axis=1, keepdims=True)
    )


def enter(tokens, vectors):
    rows, features = tokens.shape

    def kernel(tokens, vectors, low, turned):
        shift, scale = vectors[0:1], 1.0 + vectors[1:2]

        def work(here):
            values = normalize(tokens[here, :].astype(F32))[0] * scale + shift
            values = values.astype(BF16)
            low[here, :] = values
            turned[:, here] = values.T
            return ()

        by_rows(rows, 0, features, work, LANES)

    return call(
        "enter",
        kernel,
        (1,),
        [whole(tokens.shape), whole(vectors.shape)],
        [whole((rows, features)), whole((features, rows))],
        [shaped((rows, features), BF16), shaped((features, rows), BF16)],
    )(tokens, vectors)


def enter_back(cotangent, vectors):
    rows, features = cotangent.shape

    def kernel(cotangent, vectors, low, turned, sums):
        gate = vectors[5:6]

        def work(here):
            values = (gate * cotangent[here, :].astype(F32)).astype(BF16)
            low[here, :] = values
            turned[:, here] = values.T
            return (values.astype(F32),)

        (sums[...],) = by_rows(rows, 1, features, work, LANES)

    return call(
        "enter_back",
        kernel,
        (1,),
        [whole(cotangent.shape), whole(vectors.shape)],
        [whole((rows, features)), whole((features, rows)), whole((1, features))],
        [
            shaped((rows, features), BF16),
            shaped((features, rows), BF16),
            shaped((1, features), F32),
        ],
    )(cotangent, vectors)


def finish_middle(total, given, results):
    tokens, vectors = given
    branch, middle, low, turned = results
    rows, features = total.shape
    shift, scale, gate = vectors[3:4], 1.0 + vectors[4:5], vectors[2:3]
    bias = vectors[6:7]

    def work(here):
        one = total[here, :] + bias
        branch[here, :] = one
        values = tokens[here, :].astype(F32) + gate * one
        middle[here, :] = values
        values = (normalize(values)[0] * scale + shift).astype(BF16)
        low[here, :] = values
        turned[:, here] = values.T
        return ()

    by_rows(rows, 0, features, work, LANES)


def finish_output(total, given, results):
    middle, cotangent, vectors = given
    output, sums = results
    rows, features = total.shape
    gate, bias = vectors[5:6], vectors[7:8]

    def work(here):
        two = total[here, :] + bias
        output[here, :] = (middle[here, :] + gate * two).astype(BF16)
        return (two * cotangent[here, :].astype(F32),)

    (gate_back,) = by_rows(rows, 1, features, work)
    sums[...] = gate_back


def finish_middle_back(total, given, results):
    middle, branch, cotangent, vectors = given
    middle_back, low, turned, sums = results
    rows, features = total.shape
    gate, scale = vectors[2:3], 1.0 + vectors[4:5]

    def work(here):
        back = total[here, :]
        normed, inverse = normalize(middle[here, :])
        out = cotangent[here, :].astype(F32) + norm_back(back * scale, normed, inverse)
        middle_back[here, :] = out
        rounded = (gate * out).astype(BF16)
        low[here, :] = rounded
        turned[:, here] = rounded.T
        return back, back * normed, branch[here, :] * out, rounded.astype(F32)

    sums[...] = jnp.concatenate(by_rows(rows, 4, features, work, LANES), axis=0)


def finish_tokens_back(total, given, results):
    tokens, middle_back, vectors = given
    tokens_back, sums = results
    rows, features = total.shape
    scale = 1.0 + vectors[1:2]

    def work(here):
        back = total[here, :]
        normed, inverse = normalize(tokens[here, :].astype(F32))
        out = middle_back[here, :] + norm_back(back * scale, normed, inverse)
        tokens_back[here, :] = out.astype(BF16)
        return back, back * normed

    sums[...] = jnp.concatenate(by_rows(rows, 2, features, work), axis=0)


def chosen(parts):
    found = parts[0][...]
    for index, part in enumerate(parts[1:], 1):
        found = jnp.where(pl.program_id(0) == index, part[...], found)
    return found


def gradients(name, pairs, count, adds=(), form="one"):
    features, rows = pairs[0][0].shape
    parts = [one for _, parts in pairs for one in parts]
    width = sum(one.shape[2] for one, _ in parts)
    lefts, rights = len(pairs), len(parts)
    half = features // 2
    split = [isinstance(add[0], list) for add in adds]
    given = []
    for add, two in zip(adds, split):
        given += [(one[side][None], 0) for side in (0, 1) for one in add] if two else add

    def kernel(*refs):
        left_refs = refs[:lefts]
        right_refs = list(refs[lefts : lefts + rights])
        add_refs = list(refs[lefts + rights : lefts + rights + len(given)])
        outs = refs[lefts + rights + len(given) :]
        found = []
        for left, (_, own) in zip(left_refs, pairs):
            for _ in own:
                found.append(dot(left[...], right_refs.pop(0)[...]))
        out = found[0] if len(found) == 1 else jnp.concatenate(found, axis=1)
        for add, two in zip(adds, split):
            sides = [
                chosen([add_refs.pop(0) for _ in add]).astype(F32)
                for _ in range(2 if two else 1)
            ]
            out = out + (jnp.concatenate(sides, axis=0) if two else sides[0])
        out = out.astype(BF16)
        if form == "one":
            outs[0][...] = out
        else:
            for index in range(count):

                @pl.when(pl.program_id(0) == index)
                def _():
                    outs[2 * index][...] = out[:half]
                    outs[2 * index + 1][...] = out[half:]

    def addend(one):
        array, index = one
        return pl.BlockSpec((None, *array.shape[1:]), lambda *_: (index, 0, 0))

    if form == "one":
        out_specs, shape = [block((features, width))], (count, features, width)
    else:
        shape = (half, width)
        out_specs = [whole(shape)] * (2 * count)
    got = call(
        name,
        kernel,
        (count,),
        [fixed(left.shape) for left, _ in pairs]
        + [block(one.shape[1:], 0, first) for one, first in parts]
        + [addend(one) for one in given],
        out_specs,
        [shaped(shape, BF16)] * len(out_specs),
    )(
        *[left for left, _ in pairs],
        *[one for one, _ in parts],
        *[array for array, _ in given],
    )
    return got[0] if form == "one" else got


def attend(queries, pieces):
    number, rows, _ = queries.shape
    count = len(pieces)
    keys = sum(piece.shape[1] for piece in pieces)
    tile = min(rows, 256)

    def kernel(*refs):
        query, kv = refs[0], refs[1 : 1 + count]
        out_ref, log_ref = refs[1 + count :]
        head = lax.broadcasted_iota(jnp.int32, (1, LANES), 1) < HEAD_DIM
        for start in range(0, rows, tile):
            here = slice(start, start + tile)
            both = query[here, :]
            outs, logs = [], []
            for keep in (head, ~head):
                one = jnp.where(keep, both, jnp.zeros_like(both))
                scores = [dot_nt(one, piece[:, :LANES]) for piece in kv]
                top = functools.reduce(
                    jnp.maximum, [jnp.max(s, axis=1, keepdims=True) for s in scores]
                )
                weights = [jnp.exp2((s - top) * SCALE_LOG2) for s in scores]
                total = sum(jnp.sum(w, axis=1, keepdims=True) for w in weights)
                inverse = 1.0 / total
                out = sum(
                    dot((w * inverse).astype(BF16), piece[:, LANES:])
                    for w, piece in zip(weights, kv)
                )
                outs.append(out)
                logs.append(top * SCALE_LOG2 + jnp.log(total) * math.log2(math.e))
            out_ref[here, :] = jnp.where(head, outs[0], outs[1]).astype(BF16)
            table = jnp.where(head, logs[0], logs[1]).T
            log_ref[0:1, here] = table[0:1]
            log_ref[1:2, here] = table[HEAD_DIM : HEAD_DIM + 1]

    return call(
        "attend",
        kernel,
        (number,),
        [block((rows, LANES))] + [block((piece.shape[1], 2 * LANES)) for piece in pieces],
        [block((rows, LANES)), block((2, rows))],
        [shaped((number, rows, LANES), BF16), shaped((number, 2, rows), F32)],
    )(queries, *pieces)


def attend_back(queries, pieces, logs, incoming, first, kinds, begin, number):
    rows = queries.shape[1]
    count = len(pieces)
    keys = sum(piece.shape[1] for piece in pieces)
    tile = min(rows, 256)

    def kernel(*refs):
        query, back_ref, log_ref = refs[:3]
        kv = refs[3 : 3 + count]
        query_back = refs[3 + count]
        kv_back = refs[4 + count : 4 + 2 * count]
        sums, scratch = refs[4 + 2 * count], refs[5 + 2 * count :]
        head = lax.broadcasted_iota(jnp.int32, (1, LANES), 1) < HEAD_DIM
        turned = [piece[:, :LANES].T for piece in kv]
        top = lax.broadcasted_iota(jnp.int32, (LANES, 1), 0) < HEAD_DIM
        query_sum = jnp.zeros((1, LANES), F32)
        for start in range(0, rows, tile):
            here = slice(start, start + tile)
            backs = []
            for index, keep in enumerate((head, ~head)):
                zero = jnp.zeros((tile, LANES), BF16)
                one = jnp.where(keep, query[here, :], zero)
                back = jnp.where(keep, back_ref[here, :], zero)
                log = log_ref[index : index + 1, here]
                chances, mixes = [], []
                for piece in kv:
                    scores = dot_nt(piece[:, :LANES], one)
                    chances.append(jnp.exp2(scores * SCALE_LOG2 - log))
                    mixes.append(dot_nt(piece[:, LANES:], back))
                centre = sum(
                    jnp.sum(p * m, axis=0, keepdims=True) for p, m in zip(chances, mixes)
                )
                total = None
                for i in range(count):
                    score_back = (chances[i] * (mixes[i] - centre)).astype(BF16)
                    key_back = dot(score_back, one) * SCALE
                    value_back = dot(chances[i].astype(BF16), back)
                    if start == 0 and index == 0:
                        scratch[i][:, :LANES] = key_back
                        scratch[i][:, LANES:] = value_back
                    else:
                        scratch[i][:, :LANES] += key_back
                        scratch[i][:, LANES:] += value_back
                    term = dot(turned[i], score_back)
                    total = term if total is None else total + term
                backs.append(total)
            both = (jnp.where(top, backs[0], backs[1]).T * SCALE).astype(BF16)
            query_back[here, :] = both
            query_sum = query_sum + jnp.sum(both.astype(F32), axis=0, keepdims=True)
        sums[...] = query_sum
        for out, held in zip(kv_back, scratch):
            out[...] = held[...].astype(out.dtype)

    return call(
        "attend_back",
        kernel,
        (number,),
        [
            block((rows, LANES), first=begin),
            block((rows, LANES), first=first + begin),
            block((2, rows), first=begin),
        ]
        + [block((piece.shape[1], 2 * LANES), first=begin) for piece in pieces],
        [block((rows, LANES))]
        + [block((piece.shape[1], 2 * LANES)) for piece in pieces]
        + [block((1, LANES))],
        [shaped((number, rows, LANES), BF16)]
        + [
            shaped((number, piece.shape[1], 2 * LANES), kind)
            for piece, kind in zip(pieces, kinds)
        ]
        + [shaped((number, 1, LANES), F32)],
        scratch=[pltpu.VMEM((piece.shape[1], 2 * LANES), F32) for piece in pieces],
    )(queries, incoming, logs, *pieces)


def block_at(features, width):
    return block((features, width))


class Steps:
    def __init__(self, steps):
        self.steps, self.result = steps, None
        self.got = next(steps)

    def step(self):
        if self.result is None:
            try:
                self.got = self.steps.send(self.got)
            except StopIteration as end:
                self.got = self.result = end.value

    def hold(self):
        LAST.extend(jax.tree.leaves(self.got))

    def behind(self, *values):
        (*values, self.got) = lax.optimization_barrier((*values, self.got))
        return values

    def finish(self):
        while self.result is None:
            self.step()
        return self.result


class Plain:
    def __init__(self, sizes):
        self.latents, self.parts, self.width = sizes
        self.row = lax.axis_size("y") * lax.axis_size("core")
        self.col = lax.axis_size("lat") * lax.axis_size("sub")

    def scatter(self, values, held=None):
        rows, width = values.shape
        shaped_in = values.reshape(self.latents, 2, LENGTH // 2, width)
        halves = lax.all_to_all(shaped_in, "core", 1, 0, tiled=True)
        pieces = halves.reshape(self.col, -1, width)
        pieces = lax.all_to_all(pieces, COLS, 0, 0, tiled=True)
        return pieces.transpose(1, 0, 2).reshape(-1, self.col * width), held

    def collect_start(self, values):
        rows = values.shape[0]
        pieces = values.reshape(rows, self.col, -1).transpose(1, 0, 2)
        return [lax.all_to_all(pieces, COLS, 0, 0, tiled=True)]

    def collect(self, pieces):
        (pieces,) = pieces
        halves = pieces.reshape(2 * self.latents, 1, LENGTH // 2, -1)
        back = lax.all_to_all(halves, "core", 0, 1, tiled=True)
        return back.reshape(-1, self.width)

    def modulation(self, partial, bias, row_bias, col_bias):
        group = 2 * self.latents
        ours = lax.psum(partial, "core").reshape(-1, group, partial.shape[1])
        ours = lax.psum_scatter(ours, "y", scatter_dimension=0, tiled=True)[0] + bias
        sent = jnp.repeat(ours, self.col // group, axis=0)
        got = lax.all_to_all(sent, COLS, 0, 0, tiled=True)
        got = got.reshape(self.col, 6, -1).transpose(1, 0, 2).reshape(6, -1)
        cols = lax.all_gather(col_bias, COLS, axis=1, tiled=True)
        every = lax.all_gather(row_bias, ROWS, axis=0)
        return jnp.concatenate([got, cols], axis=0), [
            every.reshape(self.row * self.parts, 1, -1)
        ]

    def gather(self, parts, held):
        del held
        every = lax.all_gather(parts, COLS, axis=1, tiled=True)
        every = lax.all_gather(every, ROWS, axis=0, tiled=True)
        return [every[:, :, :LANES]], [every[:, :, LANES:]]

    def gather_start(self, parts):
        return parts

    def gather_late(self, part):
        every = lax.all_gather(part, (*ROWS, *COLS), axis=0, tiled=True)
        return every.reshape(self.row, -1, part.shape[1])

    def expand_bias(self, row_bias, biases):
        every = lax.all_gather(row_bias, ROWS, axis=0)
        return every.reshape(self.row * self.parts, 1, -1)

    def with_units(self, row_sums, unit_sums):
        return [jnp.concatenate([row_sums[0], unit_sums[0]], axis=-1)]

    def tables(self):
        blocks = jnp.arange(self.row * self.parts, dtype=jnp.int32)
        return [jnp.stack([blocks // self.parts, blocks % self.parts])]


    def share(self, kv):
        return [[lax.all_gather(kv[0], ("core", "sub"), axis=1, tiled=True)]]

    def kinds(self):
        return [F32]

    PLACES = ((0, 0),)

    def give_back(self, backs):
        return [
            lax.psum_scatter(
                backs[0][0], ("core", "sub"), scatter_dimension=1, tiled=True
            ).astype(BF16)
        ]

    def sum_up(self, *args):
        return Steps(self.reduce(*args))

    def feed_back(self, low, turned, late, expanded, hidden, extras):
        blocks = jnp.arange(self.row * self.parts, dtype=jnp.int32)
        table = jnp.stack([blocks, blocks // self.parts, blocks % self.parts])
        shrink, grow, (sums, *ends) = feed_back(
            "feed_back",
            low,
            turned,
            late,
            expanded,
            hidden,
            table,
            self.parts,
            extras,
            None,
            False,
        )
        steps = [Steps(self.reduce_ready(one[0])) for one in (shrink, grow)]
        return steps, ends, [sums]

    def reduce(self, name, pairs):
        grads = gradients(name, pairs(0, 0, 0), self.row * self.parts)
        return (yield from self.reduce_ready(grads))

    def reduce_ready(self, grads):
        grads = grads.astype(F32)
        grads = yield grads
        grads = lax.psum_scatter(grads, ROWS, scatter_dimension=0, tiled=True)
        grads = lax.psum_scatter(grads, COLS, scatter_dimension=1, tiled=True)
        return lax.psum(grads, "dp")

    def small(self, vectors, row_sums, col_sums):
        every = ("dp", *ROWS, *COLS)
        group = 2 * self.latents
        total = yield lax.psum(vectors, ("core", "sub"))
        total = total.astype(BF16)
        mine = lax.all_gather(total[:, None], "lat", axis=1, tiled=True)
        mine = lax.all_gather(mine, "y", axis=1, tiled=True)
        mine = lax.all_gather(mine, "dp", axis=1, tiled=True)
        col = lax.axis_index("lat") * lax.axis_size("sub") + lax.axis_index("sub")
        cut = lax.dynamic_slice_in_dim(mine, col * self.width, self.width, axis=2)
        cut = cut.transpose(1, 0, 2).reshape(mine.shape[1], -1)
        rows = lax.psum(row_sums[0], every).reshape(self.row, self.parts, -1)
        row = lax.axis_index("y") * 2 + lax.axis_index("core")
        rows = lax.dynamic_index_in_dim(rows, row, 0, keepdims=False)
        cols = lax.psum(col_sums, every)
        cols = lax.dynamic_slice_in_dim(cols, col * self.width, self.width, axis=1)
        return cut, rows, cols

    def col_sum(self, values):
        return lax.psum(values, COLS)

    def both_groups(self, values):
        return lax.all_gather(values, "dp", axis=0, tiled=True)


class Cube(Plain):
    PLACES = ((0, 0), (0, 1), (1, 0), (1, 1))

    def __init__(self, sizes):
        super().__init__(sizes)
        self.x = lax.axis_index("dp")
        self.y = lax.axis_index("y")
        self.c = lax.axis_index("core")
        self.z = lax.axis_index("lat")

    def swap(self, values, axis):
        return lax.ppermute(values, axis, [(0, 1), (1, 0)])

    def along(self, values, bits):
        return lax.ppermute(values, "lat", [(i, i ^ bits) for i in range(4)])

    def scatter(self, values, held=None):
        rows, width = values.shape
        halves = values.reshape(self.latents, 2, LENGTH // 2, width)
        keep = lax.dynamic_index_in_dim(halves, self.c, 1, keepdims=False)
        send = lax.dynamic_index_in_dim(halves, 1 - self.c, 1, keepdims=False)
        every = jnp.concatenate([keep, self.swap(send, "core")], axis=0)
        if held is not None:
            every, held = lax.optimization_barrier((every, held))
        pieces = []
        for latent in range(4):
            index = ((latent // 2) ^ self.c) * 2 + latent % 2
            pieces.append(lax.dynamic_index_in_dim(every, index, 0, keepdims=False))
        pieces = lax.all_to_all(jnp.stack(pieces), "lat", 0, 0, tiled=True)
        return pieces.transpose(1, 0, 2).reshape(-1, 4 * width), held

    def placed(self, pieces):
        odd, high = self.z % 2 == 1, self.z >= 2
        one, two, three, four = pieces
        one, two = jnp.where(odd, two, one), jnp.where(odd, one, two)
        three, four = jnp.where(odd, four, three), jnp.where(odd, three, four)
        return [
            jnp.where(high, three, one),
            jnp.where(high, four, two),
            jnp.where(high, one, three),
            jnp.where(high, two, four),
        ]

    def collect_start(self, values):
        pieces = values.reshape(-1, 4, self.width).transpose(1, 0, 2)
        return [lax.all_to_all(pieces, "lat", 0, 0, tiled=True)]

    def collect(self, pieces):
        width = self.width
        every = pieces[0].reshape(2, 2, -1, width)

        def latents(core):
            return lax.dynamic_index_in_dim(every, core, 0, keepdims=False)

        keep = latents(self.c)
        got = self.swap(latents(1 - self.c), "core")
        first = jnp.where(self.c == 0, keep, got)
        second = jnp.where(self.c == 0, got, keep)
        return jnp.stack([first, second], axis=1).reshape(-1, width)

    def modulation(self, partial, bias, row_bias, col_bias):
        span = partial.shape[1]
        own = row_bias.reshape(1, -1)
        got = self.swap(jnp.concatenate([partial, own], axis=0), "core")
        ours, other = partial + got[:-1], got[-1:]
        halves = ours.reshape(2, 4, span)
        keep = lax.dynamic_index_in_dim(halves, self.y, 0, keepdims=False)
        send = lax.dynamic_index_in_dim(halves, 1 - self.y, 0, keepdims=False)
        got = self.swap(jnp.concatenate([send, own, other], axis=0), "y")
        ours = keep + got[:4] + bias
        rows = jnp.stack([own, got[4:5], other, got[5:6]]).reshape(2, 2, 2, -1)
        flip = jnp.stack([rows[:, :, 1], rows[:, :, 0]], axis=2)
        rows = jnp.where(self.x == 0, rows, flip).transpose(2, 0, 1, 3)[:, :, :, None]
        pieces = []
        for bits in range(4):
            piece = lax.dynamic_index_in_dim(ours, self.z ^ bits, 0, keepdims=False)
            piece = jnp.concatenate([piece.reshape(6, -1), col_bias], axis=0)
            pieces.append(piece if bits == 0 else self.along(piece, bits))
        vectors = jnp.concatenate(self.placed(pieces), axis=1)
        return vectors, [rows[x, core] for x, core in self.PLACES]

    def gather_start(self, parts):
        part = lax.dynamic_index_in_dim(parts, self.x, 0, keepdims=False)
        odd, high = self.z % 2 == 1, self.z >= 2
        got = self.along(part, 1)
        part = jnp.concatenate([jnp.where(odd, got, part), jnp.where(odd, part, got)], axis=0)
        got = self.along(part, 2)
        part = jnp.concatenate(
            [jnp.where(high, got, part), jnp.where(high, part, got)], axis=0
        )

        return part

    def gather(self, part, held):
        one, two = part[:, :LANES], part[:, LANES:]
        one_pair = jnp.stack([one, self.swap(one, "dp")])
        near = jnp.stack([two, self.swap(two, "y")])
        near = after(near, one_pair, *held)
        far = self.swap(near, "dp")
        kv = [near, self.swap(near, "core"), far, self.swap(far, "core")]
        got = self.swap(one_pair, "y")
        near = jnp.stack([one_pair[0], got[0]])
        far = jnp.stack([one_pair[1], got[1]])
        queries = [near, self.swap(near, "core"), far, self.swap(far, "core")]
        return queries, kv

    def expand_bias(self, row_bias, biases):
        number = self.row * self.parts
        table = jnp.concatenate(self.tables(), axis=1)
        place = table[0] * self.parts + table[1]
        chosen = place[None, :] == lax.broadcasted_iota(jnp.int32, (number, number), 0)
        every = jnp.concatenate(biases, axis=0)[:, 0]
        found = jnp.dot(chosen.astype(F32), every, precision=lax.Precision.HIGHEST)
        return found[:, None]

    def with_units(self, row_sums, unit_sums):
        found = []
        for one, (x, core) in zip(row_sums, self.PLACES):
            units = unit_sums[1 - core][2 * x : 2 * x + 2]
            found.append(jnp.concatenate([one, units], axis=-1))
        return found

    def tables(self):
        side = jnp.arange(2, dtype=jnp.int32)
        return [
            jnp.stack(
                [(side ^ self.y) * 2 + (self.c ^ core), jnp.full((2,), self.x ^ x)]
            ).astype(jnp.int32)
            for x, core in self.PLACES
        ]

    def share(self, kv):
        return [
            [kv[2 * x + core], self.swap(kv[2 * x + 1 - core], "core")]
            for x, core in self.PLACES
        ]

    def kinds(self):
        return [F32, BF16]

    def give_back(self, backs):
        got = [self.swap(backs[1 - core][1], "core") for core in (0, 1)]
        return [(own[0] + one.astype(F32)).astype(BF16) for own, one in zip(backs, got)]

    def feed_back(self, low, turned, late, expanded, hidden, extras):
        tables = self.tables()
        found, sums, before = [], [], None
        for core in (1, 0):
            rows, parts = jnp.concatenate([tables[core], tables[2 + core]], axis=1)
            shrink, grow, (one, *ends) = feed_back(
                "feed_back",
                low,
                turned,
                late,
                expanded,
                hidden,
                jnp.stack([rows * self.parts + parts, rows, parts]),
                self.parts,
                [] if core else extras,
                before,
                core == 1,
            )
            if core:
                (before,) = ends
                found = [[self.swap(one, "core") for one in part] for part in (shrink, grow)]
            else:
                LAST.extend([one for part in found for one in part])
                steps = [
                    Steps(self.reduce_ready(name, near[0], far, order))
                    for name, near, far, order in (
                        ("d_shrink", shrink, found[0], "yx"),
                        ("d_expand", grow, found[1], "xy"),
                    )
                ]
            sums.append(one)
        return steps, ends, sums

    def reduce_ready(self, name, near, far, order):
        axes, one, two = (("dp", "y"), 2, 1) if order == "xy" else (("y", "dp"), 1, 2)
        far = [(far[x], y) for x in (0, 1) for y in (0, 1)]
        sent = add_up(name, [[(near, one), far[one]], [(near, 3), far[3]]])
        second = yield self.swap(sent, axes[0])
        sent = add_up(name, [[(near, two), far[two], (second, 1)]])
        third = yield self.swap(sent, axes[1])
        terms = [(near, 0), far[0], (second, 0), (third, 0)]
        return (yield from self.reduce_col(add_up(name, [terms])))

    def reduce_col(self, blocks):
        own = yield lax.psum_scatter(blocks[0], COLS, scatter_dimension=0, tiled=True)
        got = yield self.swap(gate(own), "dp")
        return jnp.stack(
            [jnp.where(self.x == 0, own, got), jnp.where(self.x == 0, got, own)]
        ).astype(F32)

    def reduce(self, name, pairs):
        def grads(place, count, adds=(), form="one"):
            return gradients(name, pairs(*place), count, adds, form)

        def far(place, count):
            sent = grads(place, count, form="apart")
            return [self.swap(one, "core") for one in sent]

        near = yield far((1, 0, 1), 2)
        second = yield self.swap(grads((1, 0, 0), 2, [[near[:2], near[2:]]]), "dp")
        near = yield far((0, 1, 1), 1)
        last = yield far((0, 0, 1), 1)
        third = yield self.swap(grads((0, 1, 0), 1, [[near], [(second, 1)]]), "y")
        adds = [[last], [(second, 0)], [(third, 0)]]
        return (yield from self.reduce_col(grads((0, 0, 0), 1, adds)))

    def small(self, vectors, row_sums, col_sums):
        span = row_sums[0].shape[-1]
        features = vectors.shape[1]

        def flat(*parts):
            return jnp.concatenate([part.reshape(-1, LANES) for part in parts], axis=0)

        def cut(message, *shapes):
            parts, start = [], 0
            for shape in shapes:
                size = math.prod(shape) // LANES
                parts.append(message[start : start + size].reshape(shape))
                start += size
            return parts

        every = jnp.stack(row_sums).reshape(2, 2, 2, span)
        rows0, rows1 = every[:, 0], every[:, 1]
        got = yield self.swap(gate(flat(rows1, col_sums, vectors)), "core")
        got = cut(got, rows1.shape, col_sums.shape, vectors.shape)
        rows, cols = rows0 + got[0], col_sums + got[1]
        mine = (vectors + got[2]).astype(BF16).astype(F32)
        got = yield self.swap(gate(flat(rows[:, 1], cols, mine)), "y")
        got = cut(got, (2, span), cols.shape, mine.shape)
        rows, cols = rows[:, 0] + got[0], cols + got[1]
        pair = jnp.stack([mine, got[2]])
        got = yield self.swap(gate(flat(rows, cols, pair)), "dp")
        got = cut(got, rows.shape, cols.shape, pair.shape)
        rows = rows + jnp.stack([got[0][1], got[0][0]])
        rows = jnp.where(self.x == 0, rows, jnp.stack([rows[1], rows[0]]))
        cols = cols + got[1]
        four = jnp.stack([pair, got[2]]).reshape(4, 6, features)
        width = self.width

        def cuts(values):
            return self.placed(
                [values[..., i * width : (i + 1) * width] for i in range(4)]
            )

        found = []
        for bits, piece in enumerate(zip(cuts(four), cuts(cols))):
            piece = [*piece, rows]
            if bits:
                got = self.along(flat(*piece), bits)
                piece = cut(got, *[part.shape for part in piece])
            found.append(piece)
        tree = [(found[0][i] + found[1][i]) + (found[2][i] + found[3][i]) for i in (1, 2)]
        every = jnp.stack([one[0] for one in found])
        every = every.reshape(16, -1)
        place = lax.broadcasted_iota(jnp.int32, (16, 16), 0)
        held = lax.broadcasted_iota(jnp.int32, (16, 16), 1)
        latent = (
            (((held // 2) % 2) ^ self.x) * 8 + ((held % 2) ^ self.y) * 4 + ((held // 4) ^ self.z)
        )
        chosen = (latent == place).astype(F32)
        every = jnp.dot(chosen, every, precision=lax.Precision.HIGHEST).astype(BF16)
        return every, tree[1], tree[0]

    def col_sum(self, values):
        got = [values] + [self.along(values, bits) for bits in (1, 2, 3)]
        return (got[0] + got[1]) + (got[2] + got[3])

    def both_groups(self, values):
        got = self.swap(values, "dp")
        return jnp.where(
            self.x == 0,
            jnp.concatenate([values, got], axis=0),
            jnp.concatenate([got, values], axis=0),
        )


def body(
    fast,
    tokens,
    condition,
    modulation_weight,
    modulation_bias,
    input_weight,
    input_bias,
    output_weight,
    output_bias,
    expand_weight,
    expand_bias,
    shrink_weight,
    shrink_bias,
    cotangent,
):
    LAST.clear()
    width = tokens.shape[1]
    inner = input_weight.shape[2]
    parts = inner // LANES
    units = expand_weight.shape[1] // parts
    sizes = (tokens.shape[0] // LENGTH, parts, width)
    net = (Cube if fast else Plain)(sizes)

    own_in = (
        input_weight.reshape(width, 3, parts, LANES)
        .transpose(2, 0, 1, 3)
        .reshape(parts, width, 3 * LANES)
    )
    own_late = with_layout_constraint(
        jnp.concatenate([expand_weight, shrink_weight.T, output_weight.T], axis=1),
        Layout((0, 1)),
    )
    out_start = 2 * parts * units // LANES

    condition_float = condition.astype(F32)
    silu_low = jax.nn.silu(condition_float).astype(BF16)
    modulator = modulation_weight.reshape(modulation_weight.shape[0], -1)
    row_bias = jnp.concatenate(
        [
            input_bias.reshape(2, parts, LANES).transpose(1, 0, 2).reshape(parts, -1),
            expand_bias.reshape(parts, units),
        ],
        axis=1,
    ).astype(F32)
    late = net.gather_late(own_late)
    vectors, row_biases = net.modulation(
        dot(silu_low, modulator),
        modulation_bias.astype(F32).reshape(1, -1),
        row_bias,
        jnp.stack([output_bias, shrink_bias]).astype(F32),
    )
    own_in = net.gather_start(own_in)
    mine, own_in = net.scatter(tokens, own_in)
    query_bufs, kv_bufs = net.gather(own_in, [mine, vectors])
    rows = mine.shape[0]
    features = mine.shape[1]
    expand_biases = net.expand_bias(
        row_bias[:, 2 * LANES :], [one[..., 2 * LANES :] for one in row_biases]
    )
    tables = net.tables()

    silu_all = net.both_groups(silu_low)
    LAST.append(silu_all)

    low_one, turned_one = enter(mine, vectors)
    queries, own_kv = [], []
    for one, two, bias in zip(query_bufs, kv_bufs, row_biases):
        one, two = project(low_one, one, two, bias)
        queries.append(one)
        own_kv.append(two)
    kv = net.share(own_kv)
    back, _ = net.scatter(after(cotangent, own_kv[0]))
    attended, logs = [], []
    for one, pieces in zip(queries, kv):
        out, log = attend(one, pieces)
        attended.append(out)
        logs.append(log)

    branch_two_back, turned_two_back, shrink_sum = enter_back(back, vectors)

    def out_place(number):
        def place(features, width):
            return tabled((features, width), (2 * number, 2 * number + 1), out_start)

        return place

    branch_one, middle, low_two, turned_two = contract(
        "out",
        [(one, late, out_place(i)) for i, one in enumerate(attended)],
        [mine, vectors],
        finish_middle,
        [
            shaped((rows, features), F32),
            shaped((rows, features), F32),
            shaped((rows, features), BF16),
            shaped((features, rows), BF16),
        ],
        table=jnp.concatenate(tables, axis=0),
    )
    expanded, hidden, output, gate_two_back = feed_forward(
        low_two, late, expand_biases, parts, [middle, back, vectors]
    )

    steps, ends, expand_sums = net.feed_back(
        branch_two_back,
        (turned_two_back, turned_two),
        late,
        expanded,
        hidden,
        [middle, branch_one, back, vectors],
    )
    middle_back, branch_one_back, turned_one_back, sums_two = ends
    shrink_steps, expand_steps = steps
    incoming = attended_backward(
        branch_one_back, late, jnp.concatenate(tables, axis=1), out_start
    )
    output = net.collect_start(gate(output))
    number = len(kv)
    blocks = queries[0].shape[0]
    found = {}

    def attention_back(i, begin, count):
        got = attend_back(
            queries[i], kv[i], logs[i], incoming, i * blocks, net.kinds(), begin, count
        )
        found[i, begin] = [got[0], got[1:-1], got[-1]]

    def kv_final(keys):
        for key, one in zip(keys, net.give_back([found[key][1] for key in keys])):
            found[key][1] = one

    def pairs(x, y, core):
        i = 2 * x + core
        key, begin = ((i, 0), y) if (i, 1) not in found else ((i, y), 0)
        heads = [(found[key][0], begin), (found[key][1], begin)]
        return [(turned_one, heads), (turned_one_back, [(attended[i], y)])]

    def every_block(i, which):
        ones = [found[key][which] for key in sorted(found) if key[0] == i]
        return ones if len(ones) > 1 else ones[0]

    if number > 1:
        attention_back(3, 0, 2)
        attention_back(2, 0, 2)
        LAST.extend(output)
        shrink_steps.hold()
        expand_steps.hold()
        shrink_steps.step()
        expand_steps.step()
        kv_final([(2, 0), (3, 0)])
        in_steps = net.sum_up("d_in", pairs)
        attention_back(1, 1, 1)
        in_steps.step()
        attention_back(0, 1, 1)
        shrink_steps.step()
        kv_final([(0, 1), (1, 1)])
        in_steps.step()
        attention_back(1, 0, 1)
        attention_back(0, 0, 1)
        expand_steps.step()
        kv_final([(0, 0), (1, 0)])
        in_steps.step()
        in_steps.step()
    else:
        attention_back(0, 0, blocks)
        kv_final([(0, 0)])
        in_steps = net.sum_up("d_in", pairs)
    shrink_steps.hold()
    tokens_back, sums_one = contract(
        "tokens_back",
        [(every_block(i, 0), buf, block_at) for i, buf in enumerate(query_bufs)]
        + [(every_block(i, 1), buf, block_at) for i, buf in enumerate(kv_bufs)],
        [mine, middle_back, vectors],
        finish_tokens_back,
        [shaped((rows, features), BF16), shaped((2, features), F32)],
    )
    summed = jnp.concatenate([sums_one, sums_two[2:3], sums_two[0:2], gate_two_back], axis=0)

    def value_sum(one):
        return jnp.sum(one[:, :, LANES:].astype(F32), axis=1, keepdims=True)

    row_sums = []
    for i in range(number):
        ones = [found[key] for key in sorted(found) if key[0] == i]
        row_sums.append(
            jnp.concatenate(
                [
                    jnp.concatenate([one[2], value_sum(one[1])], axis=-1)
                    for one in ones
                ]
            )
        )
    row_sums = net.with_units(row_sums, expand_sums)
    col_sums = jnp.concatenate([sums_two[3:4], shrink_sum], axis=0)
    tokens_back = net.collect_start(gate(tokens_back))
    small_steps = Steps(net.small(summed, row_sums, col_sums))
    in_steps.step()
    small_steps.step()
    LAST.extend(tokens_back)
    small_steps.step()
    shrink_steps.step()
    expand_steps.step()
    in_steps.step()
    shrink_parts = shrink_steps.finish()
    expand_parts = expand_steps.finish()
    in_parts = in_steps.finish()

    every, row_found, col_found = small_steps.finish()
    modulation_weight_gradient = lax.dot_general(
        silu_all, every, (((0,), (0,)), ((), ())), preferred_element_type=F32
    ).reshape(modulation_weight.shape)
    modulation_bias_gradient = jnp.sum(every.astype(F32), axis=0).reshape(6, width)
    groups = condition.shape[0]
    ours = lax.dynamic_slice_in_dim(every, lax.axis_index("dp") * groups, groups, axis=0)
    silu_back = net.col_sum(dot_nt(ours, modulator))
    silu_pull = jax.vjp(jax.nn.silu, condition_float)[1]
    condition_gradient = silu_pull(silu_back)[0]

    return (
        net.collect(output),
        net.collect(tokens_back).astype(F32),
        condition_gradient,
        modulation_weight_gradient,
        modulation_bias_gradient,
        in_parts[:, :, : 3 * LANES]
        .reshape(parts, width, 3, LANES)
        .transpose(1, 2, 0, 3)
        .reshape(input_weight.shape),
        row_found[:, : 2 * LANES]
        .reshape(parts, 2, LANES)
        .transpose(1, 0, 2)
        .reshape(input_bias.shape),
        in_parts[:, :, 3 * LANES :].transpose(0, 2, 1).reshape(output_weight.shape),
        col_found[0],
        expand_parts.transpose(1, 0, 2).reshape(expand_weight.shape),
        row_found[:, 2 * LANES :].reshape(expand_bias.shape),
        shrink_parts.transpose(0, 2, 1).reshape(shrink_weight.shape),
        col_found[1],
    )


def solution(mesh):
    dp, row, col = (mesh.shape[name] for name in ("dp", "row", "col"))

    def run(*arrays):
        latents = arrays[0].shape[0] // (dp * row * LENGTH)
        group = 2 * latents
        refined = Mesh(
            mesh.devices.reshape(dp, row // 2, 2, group, col // group),
            ("dp", "y", "core", "lat", "sub"),
        )
        fast = (dp, row, col, latents) == (2, 4, 4, 2)
        token = P(("dp", *ROWS), COLS)
        weights = (
            P(ROWS, None, COLS),
            P(None, COLS),
            P(COLS, None, ROWS),
            P(None, ROWS),
            P(ROWS, COLS),
            P(COLS),
            P(COLS, ROWS),
            P(ROWS),
            P(ROWS, COLS),
            P(COLS),
        )
        given = P("dp", ROWS)
        return jax.shard_map(
            functools.partial(body, fast),
            mesh=refined,
            in_specs=(token, given, *weights, token),
            out_specs=(token, token, given, *weights),
            check_vma=False,
        )(*arrays)

    return run
```

```python
import functools
import math

import jax
import jax.numpy as jnp
from jax import lax
from jax.experimental import pallas as pl
from jax.experimental.layout import Layout, with_layout_constraint
from jax.experimental.pallas import tpu as pltpu
from jax.sharding import Mesh
from jax.sharding import PartitionSpec as P

HEAD_DIM = 64
LENGTH = 1024
EPS = 1e-06
LANES = 128
SCALE = HEAD_DIM ** (-0.5)
SCALE_LOG2 = SCALE * math.log2(math.e)
ROWS = ("y", "core")
COLS = ("lat", "sub")
NT = (((1,), (1,)), ((), ()))
F32 = jnp.float32
BF16 = jnp.bfloat16
VMEM_LIMIT = 56 * 1024 * 1024
LAST = []


def dot(left, right):
    return jnp.dot(left, right, preferred_element_type=F32)


def dot_nt(left, right):
    return lax.dot_general(left, right, NT, preferred_element_type=F32)


def gelu_and_slope(values):
    square = values * values
    half = 0.5 + 0.5 * jnp.tanh(0.7978845608028654 * values * (1.0 + 0.044715 * square))
    rate = (2 * 0.7978845608028654) * (1.0 + 3 * 0.044715 * square)
    return values * half, half + values * (half - half * half) * rate


def whole(shape):
    return pl.BlockSpec(shape, lambda *_: (0,) * len(shape))


def fixed(shape):
    return pl.BlockSpec(
        shape, lambda *_: (0,) * len(shape), pipeline_mode=pl.Buffered(1)
    )


def block(shape, column=0, first=0, step=1):
    return pl.BlockSpec((None, *shape), lambda b, *_: (first + step * b, 0, column))


def tabled(shape, place, start=0):
    row, column = place

    def index(b, table):
        return table[row, b], 0, start if column is None else start + table[column, b]

    return pl.BlockSpec((None, *shape), index)


def call(name, kernel, grid, in_specs, out_specs, out_shape, scratch=(), table=None):
    run = pl.pallas_call(
        kernel,
        grid_spec=pltpu.PrefetchScalarGridSpec(
            num_scalar_prefetch=0 if table is None else 1,
            grid=grid,
            in_specs=in_specs,
            out_specs=out_specs,
            scratch_shapes=list(scratch),
        ),
        out_shape=out_shape,
        compiler_params=pltpu.CompilerParams(vmem_limit_bytes=VMEM_LIMIT),
        cost_estimate=pl.CostEstimate(flops=0, bytes_accessed=0, transcendentals=0),
        name=name,
    )

    def ordered(first, *others):
        first = after(first, *LAST)
        found = run(first, *others) if table is None else run(table, first, *others)
        LAST[:] = jax.tree.leaves(found)[:1]
        return found

    return ordered


def after(value, *others):
    return lax.optimization_barrier((value, *others))[0]


def shaped(shape, dtype):
    return jax.ShapeDtypeStruct(shape, dtype)


def gate(values):
    def kernel(given, out):
        out[...] = given[...]

    return call(
        "gate", kernel, (1,), [whole(values.shape)], whole(values.shape), shaped(values.shape, values.dtype)
    )(values)


def project(left, query_blocks, kv_blocks, bias):
    number, features, _ = query_blocks.shape
    rows = left.shape[0]

    def kernel(a, g, h, c, query, kv):
        query[...] = (dot(a[...], g[...]) + c[:, :LANES]).astype(BF16)
        kv[:, :LANES] = dot(a[...], h[:, :LANES]).astype(BF16)
        kv[:, LANES:] = (dot(a[...], h[:, LANES:]) + c[:, LANES : 2 * LANES]).astype(BF16)

    return call(
        "project",
        kernel,
        (number,),
        [
            fixed(left.shape),
            block((features, LANES)),
            block((features, 2 * LANES)),
            block((1, bias.shape[-1])),
        ],
        [block((rows, LANES)), block((rows, 2 * LANES))],
        [shaped((number, rows, LANES), BF16), shaped((number, rows, 2 * LANES), BF16)],
    )(left, query_blocks, kv_blocks, bias)


def feed_forward(left, late, bias, extras):
    number, _, width = bias.shape
    rows, features = left.shape

    def kernel(a, g, h, c, middle, vectors, slopes, hidden, branch, output, total):
        low, slope = gelu_and_slope(dot(a[...], g[...]) + c[...])
        slopes[...] = slope
        low = low.astype(BF16)
        hidden[...] = low
        out = dot_nt(low, h[...])

        @pl.when(pl.program_id(0) == 0)
        def _():
            total[...] = out

        @pl.when(pl.program_id(0) > 0)
        def _():
            total[...] += out

        @pl.when(pl.program_id(0) == number - 1)
        def _():
            finish_output(total, (middle, vectors), (branch, output))

    return call(
        "feed_forward",
        kernel,
        (number,),
        [
            fixed(left.shape),
            block((features, width)),
            block((features, width), 1),
            block((1, width)),
        ]
        + [fixed(extra.shape) for extra in extras],
        [
            block((rows, width)),
            block((rows, width)),
            whole((rows, features)),
            whole((rows, features)),
        ],
        [
            shaped((number, rows, width), F32),
            shaped((number, rows, width), BF16),
            shaped((rows, features), F32),
            shaped((rows, features), BF16),
        ],
        scratch=[pltpu.VMEM((rows, features), F32)],
    )(left, late, late, bias, *extras)


def feed_back(name, low, turned, late, slopes, hidden, table, parts, extras, before):
    _, rows, width = slopes.shape
    features = low.shape[1]
    number = table.shape[1]
    part = width // parts
    more = [] if before is None else [before]

    def kernel(table_ref, *refs):
        low, turned_low, turned_in, shrink, grow, slope, after_act = refs[:7]
        refs = list(refs[7:])
        start = [refs.pop(0) for _ in more]
        given = [refs.pop(0) for _ in extras]
        shrink_outs = [refs.pop(0) for _ in range(parts)]
        expand_outs = [refs.pop(0) for _ in range(parts)]
        sums = refs.pop(0)
        results, total = (refs[:-1], refs[-1]) if extras else (None, refs[0])
        step = pl.program_id(0)
        back = (dot(low[...], shrink[...]) * slope[...]).astype(BF16)
        sums[...] = jnp.sum(back.astype(F32), axis=0, keepdims=True)
        side = table_ref[1, 0]
        for place in range(parts):
            here = slice(place * part, (place + 1) * part)
            found = dot(turned_low[...], after_act[:, here]).astype(BF16)
            grown = dot(turned_in[...], back[:, here]).astype(BF16)
            for index in range(parts):

                @pl.when(side == (place ^ index))
                def _():
                    shrink_outs[index][...] = found
                    expand_outs[index][...] = grown

        out = dot_nt(back, grow[...])

        @pl.when(step == 0)
        def _():
            total[...] = out + start[0][...] if start else out

        @pl.when(step > 0)
        def _():
            total[...] += out

        if extras:

            @pl.when(step == number - 1)
            def _():
                finish_middle_back(total, given, results)

    ends = [shaped((number, 1, width), F32)]
    if extras:
        ends += [
            shaped((rows, features), F32),
            shaped((rows, features), BF16),
            shaped((features, rows), BF16),
            shaped((4, features), F32),
        ]
    else:
        ends += [shaped((rows, features), F32)]
    outs = [shaped((number, features, part), BF16)] * (2 * parts)
    got = call(
        name,
        kernel,
        (number,),
        [
            fixed(low.shape),
            *[fixed(one.shape) for one in turned],
            tabled((features, width), (0, None), 1),
            tabled((features, width), (0, None), 0),
            tabled((rows, width), (0, None)),
            tabled((rows, width), (0, None)),
        ]
        + [fixed(one.shape) for one in (*more, *extras)],
        [block((features, part))] * (2 * parts)
        + [block((1, width))]
        + [whole(one.shape) for one in ends[1:]],
        outs + ends,
        scratch=[pltpu.VMEM((rows, features), F32)] if extras else (),
        table=table,
    )(low, *turned, late, late, slopes, hidden, *more, *extras)
    return got[:parts], got[parts : 2 * parts], got[2 * parts :]


def add_up(name, blocks, upper=None):
    _, features, width = blocks[0][0][0].shape
    tile = min(features if upper is None else features // 2, 512)
    terms = [one for block_terms in blocks for one in block_terms]
    count = len(blocks)

    def kernel(*refs):
        if upper is not None:
            refs = refs[1:]
        given = list(refs[: len(terms)]) if upper is None else list(refs[: 2 * len(terms)])
        outs = refs[len(given) :]

        def total(number):
            return sum(given.pop(0)[...].astype(F32) for _ in range(number)).astype(BF16)

        if upper is None:
            for index, one in enumerate(blocks):
                outs[0][index] = total(len(one))
        else:
            for out in outs:
                out[...] = total(len(terms))

    def spec(index, side=None):
        if side is None:
            return pl.BlockSpec((None, tile, width), lambda i: (index, i, 0))
        half = features // 2 // tile
        if side == 0:
            return pl.BlockSpec((None, tile, width), lambda i, t: (index, t[0] * half + i, 0))
        return pl.BlockSpec((None, tile, width), lambda i, t: (index, (1 - t[0]) * half + i, 0))

    arrays = [array for array, _ in terms]
    if upper is None:
        return call(
            name,
            kernel,
            (features // tile,),
            [spec(index) for _, index in terms],
            pl.BlockSpec((count, tile, width), lambda i: (0, i, 0)),
            shaped((count, features, width), BF16),
        )(*arrays)
    return call(
        name,
        kernel,
        (features // 2 // tile,),
        [spec(index, 0) for _, index in terms] + [spec(index, 1) for _, index in terms],
        [pl.BlockSpec((tile, width), lambda i, _: (i, 0))] * 2,
        [shaped((features // 2, width), BF16)] * 2,
        table=jnp.full((1,), upper, jnp.int32),
    )(*arrays, *arrays)


def attended_backward(left, late, table, start):
    number = table.shape[1]
    rows, features = left.shape

    def kernel(_, a, g, out):
        out[...] = dot(a[...], g[...]).astype(BF16)

    return call(
        "attended_back",
        kernel,
        (number,),
        [fixed(left.shape), tabled((features, LANES), (0, 1), start)],
        block((rows, LANES)),
        shaped((number, rows, LANES), BF16),
        table=table,
    )(left, late)


def contract(name, terms, extras, finish, outs, table=None):
    terms = [(left if isinstance(left, list) else [left], *more) for left, *more in terms]
    number = max(len(left) * left[0].shape[0] for left, _, _ in terms)
    rows = terms[0][0][0].shape[1]
    features = terms[0][1].shape[1]
    count, more = len(terms), len(extras)
    given_lefts = [one for left, _, _ in terms for one in left]

    def kernel(*refs):
        refs = list(refs if table is None else refs[1:])
        lefts = [chosen([refs.pop(0) for _ in left]) for left, _, _ in terms]
        rights = refs[:count]
        given = refs[count : count + more]
        results, total = refs[count + more : -1], refs[-1]
        out = dot_nt(lefts[0], rights[0][...])
        for left, right in zip(lefts[1:], rights[1:]):
            out = out + dot_nt(left, right[...])
        step = pl.program_id(0)

        @pl.when(step == 0)
        def _():
            total[...] = out

        @pl.when(step > 0)
        def _():
            total[...] += out

        @pl.when(step == number - 1)
        def _():
            finish(total, given, results)

    return call(
        name,
        kernel,
        (number,),
        [
            block(one.shape[1:], step=0 if len(left) > 1 else 1)
            for left, _, _ in terms
            for one in left
        ]
        + [where(features, left[0].shape[2]) for left, _, where in terms]
        + [fixed(extra.shape) for extra in extras],
        [whole(out.shape) for out in outs],
        outs,
        scratch=[pltpu.VMEM((rows, features), F32)],
        table=table,
    )(*given_lefts, *[right for _, right, _ in terms], *extras)


def by_rows(rows, sums, features, work, tile=64):
    tile = min(rows, tile)

    def step(i, totals):
        found = work(pl.ds(pl.multiple_of(i * tile, tile), tile))
        return tuple(
            total + jnp.sum(one.reshape(-1, 8, features), axis=0)
            for total, one in zip(totals, found)
        )

    zero = jnp.zeros((8, features), F32)
    totals = lax.fori_loop(0, rows // tile, step, (zero,) * sums)
    return [jnp.sum(total, axis=0, keepdims=True) for total in totals]


def normalize(values):
    average = jnp.mean(values, axis=1, keepdims=True)
    inverse = lax.rsqrt(
        jnp.mean(values * values, axis=1, keepdims=True) - average * average + EPS
    )
    return (values - average) * inverse, inverse


def norm_back(incoming, normed, inverse):
    return inverse * (
        incoming
        - jnp.mean(incoming, axis=1, keepdims=True)
        - normed * jnp.mean(incoming * normed, axis=1, keepdims=True)
    )


def enter(tokens, vectors):
    rows, features = tokens.shape

    def kernel(tokens, vectors, low, turned):
        shift, scale = vectors[0:1], 1.0 + vectors[1:2]

        def work(here):
            values = normalize(tokens[here, :].astype(F32))[0] * scale + shift
            values = values.astype(BF16)
            low[here, :] = values
            turned[:, here] = values.T
            return ()

        by_rows(rows, 0, features, work, LANES)

    return call(
        "enter",
        kernel,
        (1,),
        [whole(tokens.shape), whole(vectors.shape)],
        [whole((rows, features)), whole((features, rows))],
        [shaped((rows, features), BF16), shaped((features, rows), BF16)],
    )(tokens, vectors)


def enter_back(cotangent, branch, vectors):
    rows, features = cotangent.shape

    def kernel(cotangent, branch, vectors, low, turned, sums):
        gate = vectors[5:6]

        def work(here):
            upstream = cotangent[here, :].astype(F32)
            values = (gate * upstream).astype(BF16)
            low[here, :] = values
            turned[:, here] = values.T
            return values.astype(F32), branch[here, :] * upstream

        sums[...] = jnp.concatenate(by_rows(rows, 2, features, work, LANES), axis=0)

    return call(
        "enter_back",
        kernel,
        (1,),
        [whole(cotangent.shape), whole(branch.shape), whole(vectors.shape)],
        [whole((rows, features)), whole((features, rows)), whole((2, features))],
        [
            shaped((rows, features), BF16),
            shaped((features, rows), BF16),
            shaped((2, features), F32),
        ],
    )(cotangent, branch, vectors)


def finish_middle(total, given, results):
    tokens, vectors = given
    branch, middle, low, turned = results
    rows, features = total.shape
    shift, scale, gate = vectors[3:4], 1.0 + vectors[4:5], vectors[2:3]
    bias = vectors[6:7]

    def work(here):
        one = total[here, :] + bias
        branch[here, :] = one
        values = tokens[here, :].astype(F32) + gate * one
        middle[here, :] = values
        values = (normalize(values)[0] * scale + shift).astype(BF16)
        low[here, :] = values
        turned[:, here] = values.T
        return ()

    by_rows(rows, 0, features, work, LANES)


def finish_output(total, given, results):
    middle, vectors = given
    branch, output = results
    rows, features = total.shape
    gate, bias = vectors[5:6], vectors[7:8]

    def work(here):
        two = total[here, :] + bias
        branch[here, :] = two
        output[here, :] = (middle[here, :] + gate * two).astype(BF16)
        return ()

    by_rows(rows, 0, features, work)


def finish_middle_back(total, given, results):
    middle, branch, cotangent, vectors = given
    middle_back, low, turned, sums = results
    rows, features = total.shape
    gate, scale = vectors[2:3], 1.0 + vectors[4:5]

    def work(here):
        back = total[here, :]
        normed, inverse = normalize(middle[here, :])
        out = cotangent[here, :].astype(F32) + norm_back(back * scale, normed, inverse)
        middle_back[here, :] = out
        rounded = (gate * out).astype(BF16)
        low[here, :] = rounded
        turned[:, here] = rounded.T
        return back, back * normed, branch[here, :] * out, rounded.astype(F32)

    sums[...] = jnp.concatenate(by_rows(rows, 4, features, work, LANES), axis=0)


def finish_tokens_back(total, given, results):
    tokens, middle_back, vectors = given
    tokens_back, sums = results
    rows, features = total.shape
    scale = 1.0 + vectors[1:2]

    def work(here):
        back = total[here, :]
        normed, inverse = normalize(tokens[here, :].astype(F32))
        out = middle_back[here, :] + norm_back(back * scale, normed, inverse)
        tokens_back[here, :] = out.astype(BF16)
        return back, back * normed

    sums[...] = jnp.concatenate(by_rows(rows, 2, features, work), axis=0)


def chosen(parts):
    found = parts[0][...]
    for index, part in enumerate(parts[1:], 1):
        found = jnp.where(pl.program_id(0) == index, part[...], found)
    return found


def gradients(name, pairs, count, adds=(), form="one"):
    features, rows = pairs[0][0].shape
    parts = [one for _, parts in pairs for one in parts]
    width = sum(one.shape[2] for one, _ in parts)
    lefts, rights = len(pairs), len(parts)
    half = features // 2
    split = [isinstance(add[0], list) for add in adds]
    given = []
    for add, two in zip(adds, split):
        given += [(one[side][None], 0) for side in (0, 1) for one in add] if two else add

    def kernel(*refs):
        left_refs = refs[:lefts]
        right_refs = list(refs[lefts : lefts + rights])
        add_refs = list(refs[lefts + rights : lefts + rights + len(given)])
        outs = refs[lefts + rights + len(given) :]
        found = []
        for left, (_, own) in zip(left_refs, pairs):
            for _ in own:
                found.append(dot(left[...], right_refs.pop(0)[...]))
        out = found[0] if len(found) == 1 else jnp.concatenate(found, axis=1)
        for add, two in zip(adds, split):
            sides = [
                chosen([add_refs.pop(0) for _ in add]).astype(F32)
                for _ in range(2 if two else 1)
            ]
            out = out + (jnp.concatenate(sides, axis=0) if two else sides[0])
        out = out.astype(BF16)
        if form == "one":
            outs[0][...] = out
        else:
            for index in range(count):

                @pl.when(pl.program_id(0) == index)
                def _():
                    outs[2 * index][...] = out[:half]
                    outs[2 * index + 1][...] = out[half:]

    def addend(one):
        array, index = one
        return pl.BlockSpec((None, *array.shape[1:]), lambda *_: (index, 0, 0))

    if form == "one":
        out_specs, shape = [block((features, width))], (count, features, width)
    else:
        shape = (half, width)
        out_specs = [whole(shape)] * (2 * count)
    got = call(
        name,
        kernel,
        (count,),
        [fixed(left.shape) for left, _ in pairs]
        + [block(one.shape[1:], 0, first) for one, first in parts]
        + [addend(one) for one in given],
        out_specs,
        [shaped(shape, BF16)] * len(out_specs),
    )(
        *[left for left, _ in pairs],
        *[one for one, _ in parts],
        *[array for array, _ in given],
    )
    return got[0] if form == "one" else got


def attend(queries, pieces):
    number, rows, _ = queries.shape
    count = len(pieces)
    keys = sum(piece.shape[1] for piece in pieces)
    tile = min(rows, 256)

    def kernel(*refs):
        query, kv = refs[0], refs[1 : 1 + count]
        out_ref, log_ref = refs[1 + count :]
        head = lax.broadcasted_iota(jnp.int32, (1, LANES), 1) < HEAD_DIM

        def step(i, _):
            here = pl.ds(pl.multiple_of(i * tile, tile), tile)
            both = query[here, :]
            outs, logs = [], []
            for keep in (head, ~head):
                one = jnp.where(keep, both, jnp.zeros_like(both))
                scores = [dot_nt(one, piece[:, :LANES]) for piece in kv]
                top = functools.reduce(
                    jnp.maximum, [jnp.max(s, axis=1, keepdims=True) for s in scores]
                )
                weights = [jnp.exp2((s - top) * SCALE_LOG2) for s in scores]
                total = sum(jnp.sum(w, axis=1, keepdims=True) for w in weights)
                inverse = 1.0 / total
                out = sum(
                    dot((w * inverse).astype(BF16), piece[:, LANES:])
                    for w, piece in zip(weights, kv)
                )
                outs.append(out)
                logs.append(top * SCALE_LOG2 + jnp.log(total) * math.log2(math.e))
            out_ref[here, :] = jnp.where(head, outs[0], outs[1]).astype(BF16)
            table = jnp.where(head, logs[0], logs[1]).T
            log_ref[0:1, here] = table[0:1]
            log_ref[1:2, here] = table[HEAD_DIM : HEAD_DIM + 1]
            return 0

        lax.fori_loop(0, rows // tile, step, 0)

    return call(
        "attend",
        kernel,
        (number,),
        [block((rows, LANES))] + [block((piece.shape[1], 2 * LANES)) for piece in pieces],
        [block((rows, LANES)), block((2, rows))],
        [shaped((number, rows, LANES), BF16), shaped((number, 2, rows), F32)],
    )(queries, *pieces)


def attend_back(queries, pieces, logs, incoming, first, kinds, begin, number):
    rows = queries.shape[1]
    count = len(pieces)
    keys = sum(piece.shape[1] for piece in pieces)
    tile = min(rows, 256)

    def kernel(*refs):
        query, back_ref, log_ref = refs[:3]
        kv = refs[3 : 3 + count]
        query_back = refs[3 + count]
        kv_back = refs[4 + count : 4 + 2 * count]
        sums, scratch = refs[4 + 2 * count], refs[5 + 2 * count :]
        head = lax.broadcasted_iota(jnp.int32, (1, LANES), 1) < HEAD_DIM
        turned = [piece[:, :LANES].T for piece in kv]
        top = lax.broadcasted_iota(jnp.int32, (LANES, 1), 0) < HEAD_DIM
        for held in scratch:
            held[...] = jnp.zeros_like(held)

        def step(j, query_sum):
            here = pl.ds(pl.multiple_of(j * tile, tile), tile)
            backs = []
            for index, keep in enumerate((head, ~head)):
                zero = jnp.zeros((tile, LANES), BF16)
                one = jnp.where(keep, query[here, :], zero)
                back = jnp.where(keep, back_ref[here, :], zero)
                log = log_ref[index : index + 1, here]
                chances, mixes = [], []
                for piece in kv:
                    scores = dot_nt(piece[:, :LANES], one)
                    chances.append(jnp.exp2(scores * SCALE_LOG2 - log))
                    mixes.append(dot_nt(piece[:, LANES:], back))
                centre = sum(
                    jnp.sum(p * m, axis=0, keepdims=True) for p, m in zip(chances, mixes)
                )
                total = None
                for i in range(count):
                    score_back = (chances[i] * (mixes[i] - centre)).astype(BF16)
                    scratch[i][:, :LANES] += dot(score_back, one) * SCALE
                    scratch[i][:, LANES:] += dot(chances[i].astype(BF16), back)
                    term = dot(turned[i], score_back)
                    total = term if total is None else total + term
                backs.append(total)
            both = (jnp.where(top, backs[0], backs[1]).T * SCALE).astype(BF16)
            query_back[here, :] = both
            return query_sum + jnp.sum(both.astype(F32), axis=0, keepdims=True)

        sums[...] = lax.fori_loop(0, rows // tile, step, jnp.zeros((1, LANES), F32))
        for out, held in zip(kv_back, scratch):
            out[...] = held[...].astype(out.dtype)

    return call(
        "attend_back",
        kernel,
        (number,),
        [
            block((rows, LANES), first=begin),
            block((rows, LANES), first=first + begin),
            block((2, rows), first=begin),
        ]
        + [block((piece.shape[1], 2 * LANES), first=begin) for piece in pieces],
        [block((rows, LANES))]
        + [block((piece.shape[1], 2 * LANES)) for piece in pieces]
        + [block((1, LANES))],
        [shaped((number, rows, LANES), BF16)]
        + [
            shaped((number, piece.shape[1], 2 * LANES), kind)
            for piece, kind in zip(pieces, kinds)
        ]
        + [shaped((number, 1, LANES), F32)],
        scratch=[pltpu.VMEM((piece.shape[1], 2 * LANES), F32) for piece in pieces],
    )(queries, incoming, logs, *pieces)


def block_at(features, width):
    return block((features, width))


class Steps:
    def __init__(self, steps):
        self.steps, self.result = steps, None
        self.got = next(steps)

    def step(self):
        if self.result is None:
            try:
                self.got = self.steps.send(self.got)
            except StopIteration as end:
                self.got = self.result = end.value

    def hold(self):
        LAST.extend(jax.tree.leaves(self.got))

    def behind(self, *values):
        (*values, self.got) = lax.optimization_barrier((*values, self.got))
        return values

    def finish(self):
        while self.result is None:
            self.step()
        return self.result


class Plain:
    def __init__(self, sizes):
        self.latents, self.parts, self.width = sizes
        self.row = lax.axis_size("y") * lax.axis_size("core")
        self.col = lax.axis_size("lat") * lax.axis_size("sub")

    def scatter(self, values, held=None):
        rows, width = values.shape
        shaped_in = values.reshape(self.latents, 2, LENGTH // 2, width)
        halves = lax.all_to_all(shaped_in, "core", 1, 0, tiled=True)
        pieces = halves.reshape(self.col, -1, width)
        pieces = lax.all_to_all(pieces, COLS, 0, 0, tiled=True)
        return pieces.transpose(1, 0, 2).reshape(-1, self.col * width), held

    def collect_start(self, values):
        rows = values.shape[0]
        pieces = values.reshape(rows, self.col, -1).transpose(1, 0, 2)
        return [lax.all_to_all(pieces, COLS, 0, 0, tiled=True)]

    def collect(self, pieces):
        (pieces,) = pieces
        halves = pieces.reshape(2 * self.latents, 1, LENGTH // 2, -1)
        back = lax.all_to_all(halves, "core", 0, 1, tiled=True)
        return back.reshape(-1, self.width)

    def modulation(self, partial, bias, row_bias, col_bias):
        group = 2 * self.latents
        ours = lax.psum(partial, "core").reshape(-1, group, partial.shape[1])
        ours = lax.psum_scatter(ours, "y", scatter_dimension=0, tiled=True)[0] + bias
        sent = jnp.repeat(ours, self.col // group, axis=0)
        got = lax.all_to_all(sent, COLS, 0, 0, tiled=True)
        got = got.reshape(self.col, 6, -1).transpose(1, 0, 2).reshape(6, -1)
        cols = lax.all_gather(col_bias, COLS, axis=1, tiled=True)
        every = lax.all_gather(row_bias, ROWS, axis=0)
        return jnp.concatenate([got, cols], axis=0), [
            every.reshape(self.row * self.parts, 1, -1)
        ]

    def gather(self, parts, held):
        every = lax.all_gather(parts, COLS, axis=1, tiled=True)
        every = lax.all_gather(every, ROWS, axis=0, tiled=True)
        return [every[:, :, :LANES]], [every[:, :, LANES:]], held

    def gather_start(self, parts, held):
        return parts, held

    def gather_late(self, part):
        every = lax.all_gather(part, (*ROWS, *COLS), axis=0, tiled=True)
        return every.reshape(self.row, -1, part.shape[1])

    def expand_bias(self, row_bias, biases):
        every = lax.all_gather(row_bias, ROWS, axis=0)
        return every.reshape(self.row * self.parts, 1, -1)

    def with_units(self, row_sums, unit_sums):
        return [jnp.concatenate([row_sums[0], unit_sums[0]], axis=-1)]

    def tables(self):
        blocks = jnp.arange(self.row * self.parts, dtype=jnp.int32)
        return [jnp.stack([blocks // self.parts, blocks % self.parts])]


    def share(self, kv):
        return [[lax.all_gather(kv[0], ("core", "sub"), axis=1, tiled=True)]]

    def kinds(self):
        return [F32]

    PLACES = ((0, 0),)

    def give_back(self, backs):
        return [
            lax.psum_scatter(
                backs[0][0], ("core", "sub"), scatter_dimension=1, tiled=True
            ).astype(BF16)
        ]

    def sum_up(self, *args):
        return Steps(self.reduce(*args))

    def feed_back(self, low, turned, late, slopes, hidden, extras):
        table = jnp.stack([jnp.arange(self.row, dtype=jnp.int32)] * 2) * jnp.array(
            [[1], [0]], jnp.int32
        )
        shrink, grow, (sums, *ends) = feed_back(
            "feed_back", low, turned, late, slopes, hidden, table, self.parts, extras, None
        )

        def blocks(parts):
            return jnp.stack(parts, axis=1).reshape(-1, *parts[0].shape[1:])

        steps = [Steps(self.reduce_ready(blocks(one))) for one in (shrink, grow)]
        return steps, ends, [sums.reshape(self.row * self.parts, 1, -1)]

    def reduce(self, name, pairs):
        grads = gradients(name, pairs(0, 0, 0), self.row * self.parts)
        return (yield from self.reduce_ready(grads))

    def reduce_ready(self, grads):
        grads = grads.astype(F32)
        grads = yield grads
        grads = lax.psum_scatter(grads, ROWS, scatter_dimension=0, tiled=True)
        grads = lax.psum_scatter(grads, COLS, scatter_dimension=1, tiled=True)
        return lax.psum(grads, "dp")

    def small(self, vectors, row_sums, col_sums):
        every = ("dp", *ROWS, *COLS)
        group = 2 * self.latents
        total = yield lax.psum(vectors, ("core", "sub"))
        total = total.astype(BF16)
        mine = lax.all_gather(total[:, None], "lat", axis=1, tiled=True)
        mine = lax.all_gather(mine, "y", axis=1, tiled=True)
        mine = lax.all_gather(mine, "dp", axis=1, tiled=True)
        col = lax.axis_index("lat") * lax.axis_size("sub") + lax.axis_index("sub")
        cut = lax.dynamic_slice_in_dim(mine, col * self.width, self.width, axis=2)
        cut = cut.transpose(1, 0, 2).reshape(mine.shape[1], -1)
        rows = lax.psum(row_sums[0], every).reshape(self.row, self.parts, -1)
        row = lax.axis_index("y") * 2 + lax.axis_index("core")
        rows = lax.dynamic_index_in_dim(rows, row, 0, keepdims=False)
        cols = lax.psum(col_sums, every)
        cols = lax.dynamic_slice_in_dim(cols, col * self.width, self.width, axis=1)
        return cut, rows, cols

    def col_sum(self, values):
        return lax.psum(values, COLS)

    def both_groups(self, values):
        return lax.all_gather(values, "dp", axis=0, tiled=True)


class Cube(Plain):
    PLACES = ((0, 0), (0, 1), (1, 0), (1, 1))

    def __init__(self, sizes):
        super().__init__(sizes)
        self.x = lax.axis_index("dp")
        self.y = lax.axis_index("y")
        self.c = lax.axis_index("core")
        self.z = lax.axis_index("lat")

    def swap(self, values, axis):
        return lax.ppermute(values, axis, [(0, 1), (1, 0)])

    def along(self, values, bits):
        return lax.ppermute(values, "lat", [(i, i ^ bits) for i in range(4)])

    def scatter(self, values, held=None):
        rows, width = values.shape
        halves = values.reshape(self.latents, 2, LENGTH // 2, width)
        keep = lax.dynamic_index_in_dim(halves, self.c, 1, keepdims=False)
        send = lax.dynamic_index_in_dim(halves, 1 - self.c, 1, keepdims=False)
        every = jnp.concatenate([keep, self.swap(send, "core")], axis=0)
        if held is not None:
            every, held = lax.optimization_barrier((every, held))
        pieces = []
        for latent in range(4):
            index = ((latent // 2) ^ self.c) * 2 + latent % 2
            pieces.append(lax.dynamic_index_in_dim(every, index, 0, keepdims=False))
        pieces = lax.all_to_all(jnp.stack(pieces), "lat", 0, 0, tiled=True)
        return pieces.transpose(1, 0, 2).reshape(-1, 4 * width), held

    def placed(self, pieces):
        odd, high = self.z % 2 == 1, self.z >= 2
        one, two, three, four = pieces
        one, two = jnp.where(odd, two, one), jnp.where(odd, one, two)
        three, four = jnp.where(odd, four, three), jnp.where(odd, three, four)
        return [
            jnp.where(high, three, one),
            jnp.where(high, four, two),
            jnp.where(high, one, three),
            jnp.where(high, two, four),
        ]

    def collect_start(self, values):
        pieces = values.reshape(-1, 4, self.width).transpose(1, 0, 2)
        return [lax.all_to_all(pieces, "lat", 0, 0, tiled=True)]

    def collect(self, pieces):
        width = self.width
        every = pieces[0].reshape(2, 2, -1, width)

        def latents(core):
            return lax.dynamic_index_in_dim(every, core, 0, keepdims=False)

        keep = latents(self.c)
        got = self.swap(latents(1 - self.c), "core")
        first = jnp.where(self.c == 0, keep, got)
        second = jnp.where(self.c == 0, got, keep)
        return jnp.stack([first, second], axis=1).reshape(-1, width)

    def modulation(self, partial, bias, row_bias, col_bias):
        span = partial.shape[1]
        own = row_bias.reshape(1, -1)
        got = self.swap(jnp.concatenate([partial, own], axis=0), "core")
        ours, other = partial + got[:-1], got[-1:]
        halves = ours.reshape(2, 4, span)
        keep = lax.dynamic_index_in_dim(halves, self.y, 0, keepdims=False)
        send = lax.dynamic_index_in_dim(halves, 1 - self.y, 0, keepdims=False)
        got = self.swap(jnp.concatenate([send, own, other], axis=0), "y")
        ours = keep + got[:4] + bias
        rows = jnp.stack([own, got[4:5], other, got[5:6]]).reshape(2, 2, 2, -1)
        flip = jnp.stack([rows[:, :, 1], rows[:, :, 0]], axis=2)
        rows = jnp.where(self.x == 0, rows, flip).transpose(2, 0, 1, 3)[:, :, :, None]
        pieces = []
        for bits in range(4):
            piece = lax.dynamic_index_in_dim(ours, self.z ^ bits, 0, keepdims=False)
            piece = jnp.concatenate([piece.reshape(6, -1), col_bias], axis=0)
            pieces.append(piece if bits == 0 else self.along(piece, bits))
        vectors = jnp.concatenate(self.placed(pieces), axis=1)
        return vectors, [rows[x, core] for x, core in self.PLACES]

    def gather_start(self, parts, held):
        part = lax.dynamic_index_in_dim(parts, self.x, 0, keepdims=False)
        odd, high = self.z % 2 == 1, self.z >= 2
        got = self.along(part, 1)
        part = jnp.concatenate([jnp.where(odd, got, part), jnp.where(odd, part, got)], axis=0)
        part, held = lax.optimization_barrier((part, held))
        got = self.along(part, 2)
        part = jnp.concatenate(
            [jnp.where(high, got, part), jnp.where(high, part, got)], axis=0
        )

        return part, held

    def gather(self, part, held):
        one, two = part[:, :LANES], part[:, LANES:]
        one_pair = jnp.stack([one, self.swap(one, "dp")])
        near = jnp.stack([two, self.swap(two, "y")])
        near = after(near, one_pair)
        far = self.swap(near, "dp")
        kv = [near, self.swap(near, "core"), far, self.swap(far, "core")]
        one_pair, held = lax.optimization_barrier((one_pair, held))
        got = self.swap(one_pair, "y")
        near = jnp.stack([one_pair[0], got[0]])
        far = jnp.stack([one_pair[1], got[1]])
        queries = [near, self.swap(near, "core"), far, self.swap(far, "core")]
        return queries, kv, held

    def expand_bias(self, row_bias, biases):
        number = self.row * self.parts
        table = jnp.concatenate(self.tables(), axis=1)
        place = table[0] * self.parts + table[1]
        chosen = place[None, :] == lax.broadcasted_iota(jnp.int32, (number, number), 0)
        every = jnp.concatenate(biases, axis=0)[:, 0]
        found = jnp.dot(chosen.astype(F32), every, precision=lax.Precision.HIGHEST)
        return found[:, None]

    def with_units(self, row_sums, unit_sums):
        found = []
        for one, (x, core) in zip(row_sums, self.PLACES):
            units = unit_sums[1 - core][2 * x : 2 * x + 2]
            found.append(jnp.concatenate([one, units], axis=-1))
        return found

    def tables(self):
        side = jnp.arange(2, dtype=jnp.int32)
        return [
            jnp.stack(
                [(side ^ self.y) * 2 + (self.c ^ core), jnp.full((2,), self.x ^ x)]
            ).astype(jnp.int32)
            for x, core in self.PLACES
        ]

    def share(self, kv):
        return [
            [kv[2 * x + core], self.swap(kv[2 * x + 1 - core], "core")]
            for x, core in self.PLACES
        ]

    def kinds(self):
        return [F32, BF16]

    def give_back(self, backs):
        got = [self.swap(backs[1 - core][1], "core") for core in (0, 1)]
        return [(own[0] + one.astype(F32)).astype(BF16) for own, one in zip(backs, got)]

    def feed_back(self, low, turned, late, slopes, hidden, extras):
        tables = self.tables()
        found, sums, before = [], [], None
        for core in (1, 0):
            rows = tables[core][0]
            shrink, grow, (one, *ends) = feed_back(
                "feed_back",
                low,
                turned,
                late,
                slopes,
                hidden,
                jnp.stack([rows, jnp.full((2,), self.x, jnp.int32)]),
                self.parts,
                [] if core else extras,
                before,
            )
            if core:
                (before,) = ends
                found = [[self.swap(one, "core") for one in part] for part in (shrink, grow)]
            else:
                LAST.extend([one for part in found for one in part])
                steps = [
                    Steps(self.reduce_ready(name, near, far, order))
                    for name, near, far, order in (
                        ("d_shrink", shrink, found[0], "yx"),
                        ("d_expand", grow, found[1], "xy"),
                    )
                ]
            one = one.reshape(2, 1, self.parts, -1).transpose(2, 0, 1, 3)
            one = jnp.where(self.x == 0, one, jnp.stack([one[1], one[0]]))
            sums.append(one.reshape(4, 1, -1))
        return steps, ends, sums

    def reduce_ready(self, name, near, far, order):
        axes, one, two = (("dp", "y"), 2, 1) if order == "xy" else (("y", "dp"), 1, 2)
        near, far = (
            [(part[x], y) for x in (0, 1) for y in (0, 1)] for part in (near, far)
        )
        sent = add_up(name, [[near[one], far[one]], [near[3], far[3]]])
        second = yield self.swap(sent, axes[0])
        sent = add_up(name, [[near[two], far[two], (second, 1)]])
        third = yield self.swap(sent, axes[1])
        terms = [near[0], far[0], (second, 0), (third, 0)]
        return (yield from self.reduce_col(add_up(name, [terms])))

    def reduce_col(self, blocks):
        own = yield lax.psum_scatter(blocks[0], COLS, scatter_dimension=0, tiled=True)
        got = yield self.swap(gate(own), "dp")
        return jnp.stack(
            [jnp.where(self.x == 0, own, got), jnp.where(self.x == 0, got, own)]
        ).astype(F32)

    def reduce(self, name, pairs):
        def grads(place, count, adds=(), form="one"):
            return gradients(name, pairs(*place), count, adds, form)

        def far(place, count):
            sent = grads(place, count, form="apart")
            return [self.swap(one, "core") for one in sent]

        near = yield far((1, 0, 1), 2)
        second = yield self.swap(grads((1, 0, 0), 2, [[near[:2], near[2:]]]), "dp")
        near = yield far((0, 1, 1), 1)
        last = yield far((0, 0, 1), 1)
        third = yield self.swap(grads((0, 1, 0), 1, [[near], [(second, 1)]]), "y")
        adds = [[last], [(second, 0)], [(third, 0)]]
        return (yield from self.reduce_col(grads((0, 0, 0), 1, adds)))

    def small(self, vectors, row_sums, col_sums):
        span = row_sums[0].shape[-1]
        features = vectors.shape[1]

        def flat(*parts):
            return jnp.concatenate([part.reshape(-1, LANES) for part in parts], axis=0)

        def cut(message, *shapes):
            parts, start = [], 0
            for shape in shapes:
                size = math.prod(shape) // LANES
                parts.append(message[start : start + size].reshape(shape))
                start += size
            return parts

        every = jnp.stack(row_sums).reshape(2, 2, 2, span)
        rows0, rows1 = every[:, 0], every[:, 1]
        got = yield self.swap(gate(flat(rows1, col_sums, vectors)), "core")
        got = cut(got, rows1.shape, col_sums.shape, vectors.shape)
        rows, cols = rows0 + got[0], col_sums + got[1]
        mine = (vectors + got[2]).astype(BF16).astype(F32)
        got = yield self.swap(gate(flat(rows[:, 1], cols, mine)), "y")
        got = cut(got, (2, span), cols.shape, mine.shape)
        rows, cols = rows[:, 0] + got[0], cols + got[1]
        pair = jnp.stack([mine, got[2]])
        got = yield self.swap(gate(flat(rows, cols, pair)), "dp")
        got = cut(got, rows.shape, cols.shape, pair.shape)
        rows = rows + jnp.stack([got[0][1], got[0][0]])
        rows = jnp.where(self.x == 0, rows, jnp.stack([rows[1], rows[0]]))
        cols = cols + got[1]
        four = jnp.stack([pair, got[2]]).reshape(4, 6, features)
        width = self.width

        def cuts(values):
            return self.placed(
                [values[..., i * width : (i + 1) * width] for i in range(4)]
            )

        found = []
        for bits, piece in enumerate(zip(cuts(four), cuts(cols))):
            piece = [*piece, rows]
            if bits:
                got = self.along(flat(*piece), bits)
                piece = cut(got, *[part.shape for part in piece])
            found.append(piece)
        tree = [(found[0][i] + found[1][i]) + (found[2][i] + found[3][i]) for i in (1, 2)]
        every = jnp.stack([one[0] for one in found])
        every = every.reshape(16, -1)
        place = lax.broadcasted_iota(jnp.int32, (16, 16), 0)
        held = lax.broadcasted_iota(jnp.int32, (16, 16), 1)
        latent = (
            (((held // 2) % 2) ^ self.x) * 8 + ((held % 2) ^ self.y) * 4 + ((held // 4) ^ self.z)
        )
        chosen = (latent == place).astype(F32)
        every = jnp.dot(chosen, every, precision=lax.Precision.HIGHEST).astype(BF16)
        return every, tree[1], tree[0]

    def col_sum(self, values):
        got = [values] + [self.along(values, bits) for bits in (1, 2, 3)]
        return (got[0] + got[1]) + (got[2] + got[3])

    def both_groups(self, values):
        got = self.swap(values, "dp")
        return jnp.where(
            self.x == 0,
            jnp.concatenate([values, got], axis=0),
            jnp.concatenate([got, values], axis=0),
        )


def body(
    fast,
    tokens,
    condition,
    modulation_weight,
    modulation_bias,
    input_weight,
    input_bias,
    output_weight,
    output_bias,
    expand_weight,
    expand_bias,
    shrink_weight,
    shrink_bias,
    cotangent,
):
    LAST.clear()
    width = tokens.shape[1]
    inner = input_weight.shape[2]
    parts = inner // LANES
    units = expand_weight.shape[1] // parts
    sizes = (tokens.shape[0] // LENGTH, parts, width)
    net = (Cube if fast else Plain)(sizes)

    own_in = (
        input_weight.reshape(width, 3, parts, LANES)
        .transpose(2, 0, 1, 3)
        .reshape(parts, width, 3 * LANES)
    )
    own_late = with_layout_constraint(
        jnp.concatenate([expand_weight, shrink_weight.T, output_weight.T], axis=1),
        Layout((0, 1)),
    )
    out_start = 2 * parts * units // LANES

    condition_float = condition.astype(F32)
    silu_low = jax.nn.silu(condition_float).astype(BF16)
    modulator = modulation_weight.reshape(modulation_weight.shape[0], -1)
    row_bias = jnp.concatenate(
        [
            input_bias.reshape(2, parts, LANES).transpose(1, 0, 2).reshape(parts, -1),
            expand_bias.reshape(parts, units),
        ],
        axis=1,
    ).astype(F32)
    late = net.gather_late(own_late)
    vectors, row_biases = net.modulation(
        dot(silu_low, modulator),
        modulation_bias.astype(F32).reshape(1, -1),
        row_bias,
        jnp.stack([output_bias, shrink_bias]).astype(F32),
    )
    silu_all = net.both_groups(silu_low)
    own_in, (vectors, silu_all) = net.gather_start(own_in, (vectors, silu_all))
    mine, own_in = net.scatter(tokens, own_in)
    query_bufs, kv_bufs, mine = net.gather(own_in, mine)
    rows = mine.shape[0]
    features = mine.shape[1]
    expand_biases = net.expand_bias(
        row_bias[:, 2 * LANES :], [one[..., 2 * LANES :] for one in row_biases]
    )
    tables = net.tables()

    low_one, turned_one = enter(mine, vectors)
    queries, own_kv = [], []
    for one, two, bias in zip(query_bufs, kv_bufs, row_biases):
        one, two = project(low_one, one, two, bias)
        queries.append(one)
        own_kv.append(two)
    kv = net.share(own_kv)
    attended, logs = [], []
    for one, pieces in zip(queries, kv):
        out, log = attend(one, pieces)
        attended.append(out)
        logs.append(log)
    back, (late, attended[-1]) = net.scatter(cotangent, (late, attended[-1]))

    def out_place(number):
        def place(features, width):
            return tabled((features, width), (2 * number, 2 * number + 1), out_start)

        return place

    branch_one, middle, low_two, turned_two = contract(
        "out",
        [(one, late, out_place(i)) for i, one in enumerate(attended)],
        [mine, vectors],
        finish_middle,
        [
            shaped((rows, features), F32),
            shaped((rows, features), F32),
            shaped((rows, features), BF16),
            shaped((features, rows), BF16),
        ],
        table=jnp.concatenate(tables, axis=0),
    )
    slopes, hidden, branch_two, output = feed_forward(
        low_two, late, expand_biases.reshape(-1, 1, parts * units), [middle, vectors]
    )
    branch_two_back, turned_two_back, sums_back = enter_back(back, branch_two, vectors)
    shrink_sum, gate_two_back = sums_back[0:1], sums_back[1:2]

    steps, ends, expand_sums = net.feed_back(
        branch_two_back,
        (turned_two_back, turned_two),
        late,
        slopes,
        hidden,
        [middle, branch_one, back, vectors],
    )
    middle_back, branch_one_back, turned_one_back, sums_two = ends
    shrink_steps, expand_steps = steps
    incoming = attended_backward(
        branch_one_back, late, jnp.concatenate(tables, axis=1), out_start
    )
    output = net.collect_start(gate(output))
    number = len(kv)
    blocks = queries[0].shape[0]
    found = {}

    def attention_back(i, begin, count):
        got = attend_back(
            queries[i], kv[i], logs[i], incoming, i * blocks, net.kinds(), begin, count
        )
        found[i, begin] = [got[0], got[1:-1], got[-1]]

    def kv_final(keys):
        for key, one in zip(keys, net.give_back([found[key][1] for key in keys])):
            found[key][1] = one

    def pairs(x, y, core):
        i = 2 * x + core
        key, begin = ((i, 0), y) if (i, 1) not in found else ((i, y), 0)
        heads = [(found[key][0], begin), (found[key][1], begin)]
        return [(turned_one, heads), (turned_one_back, [(attended[i], y)])]

    def every_block(i, which):
        ones = [found[key][which] for key in sorted(found) if key[0] == i]
        return ones if len(ones) > 1 else ones[0]

    if number > 1:
        attention_back(3, 0, 2)
        attention_back(2, 0, 2)
        LAST.extend(output)
        shrink_steps.hold()
        expand_steps.hold()
        shrink_steps.step()
        expand_steps.step()
        kv_final([(2, 0), (3, 0)])
        in_steps = net.sum_up("d_in", pairs)
        attention_back(1, 1, 1)
        in_steps.step()
        attention_back(0, 1, 1)
        shrink_steps.step()
        kv_final([(0, 1), (1, 1)])
        in_steps.step()
        attention_back(1, 0, 1)
        attention_back(0, 0, 1)
        expand_steps.step()
        kv_final([(0, 0), (1, 0)])
        in_steps.step()
        in_steps.step()
    else:
        attention_back(0, 0, blocks)
        kv_final([(0, 0)])
        in_steps = net.sum_up("d_in", pairs)
    shrink_steps.hold()
    tokens_back, sums_one = contract(
        "tokens_back",
        [(every_block(i, 0), buf, block_at) for i, buf in enumerate(query_bufs)]
        + [(every_block(i, 1), buf, block_at) for i, buf in enumerate(kv_bufs)],
        [mine, middle_back, vectors],
        finish_tokens_back,
        [shaped((rows, features), BF16), shaped((2, features), F32)],
    )
    summed = jnp.concatenate([sums_one, sums_two[2:3], sums_two[0:2], gate_two_back], axis=0)

    def value_sum(one):
        return jnp.sum(one[:, :, LANES:].astype(F32), axis=1, keepdims=True)

    row_sums = []
    for i in range(number):
        ones = [found[key] for key in sorted(found) if key[0] == i]
        row_sums.append(
            jnp.concatenate(
                [
                    jnp.concatenate([one[2], value_sum(one[1])], axis=-1)
                    for one in ones
                ]
            )
        )
    row_sums = net.with_units(row_sums, expand_sums)
    col_sums = jnp.concatenate([sums_two[3:4], shrink_sum], axis=0)
    tokens_back = net.collect_start(gate(tokens_back))
    small_steps = Steps(net.small(summed, row_sums, col_sums))
    in_steps.step()
    small_steps.step()
    LAST.extend(tokens_back)
    small_steps.step()
    shrink_steps.step()
    expand_steps.step()
    in_steps.step()
    shrink_parts = shrink_steps.finish()
    expand_parts = expand_steps.finish()
    in_parts = in_steps.finish()

    every, row_found, col_found = small_steps.finish()
    modulation_weight_gradient = lax.dot_general(
        silu_all, every, (((0,), (0,)), ((), ())), preferred_element_type=F32
    ).reshape(modulation_weight.shape)
    modulation_bias_gradient = jnp.sum(every.astype(F32), axis=0).reshape(6, width)
    groups = condition.shape[0]
    ours = lax.dynamic_slice_in_dim(every, lax.axis_index("dp") * groups, groups, axis=0)
    silu_back = net.col_sum(dot_nt(ours, modulator))
    silu_pull = jax.vjp(jax.nn.silu, condition_float)[1]
    condition_gradient = silu_pull(silu_back)[0]

    return (
        net.collect(output),
        net.collect(tokens_back).astype(F32),
        condition_gradient,
        modulation_weight_gradient,
        modulation_bias_gradient,
        in_parts[:, :, : 3 * LANES]
        .reshape(parts, width, 3, LANES)
        .transpose(1, 2, 0, 3)
        .reshape(input_weight.shape),
        row_found[:, : 2 * LANES]
        .reshape(parts, 2, LANES)
        .transpose(1, 0, 2)
        .reshape(input_bias.shape),
        in_parts[:, :, 3 * LANES :].transpose(0, 2, 1).reshape(output_weight.shape),
        col_found[0],
        expand_parts.transpose(1, 0, 2).reshape(expand_weight.shape),
        row_found[:, 2 * LANES :].reshape(expand_bias.shape),
        shrink_parts.transpose(0, 2, 1).reshape(shrink_weight.shape),
        col_found[1],
    )


def solution(mesh):
    dp, row, col = (mesh.shape[name] for name in ("dp", "row", "col"))

    def run(*arrays):
        latents = arrays[0].shape[0] // (dp * row * LENGTH)
        group = 2 * latents
        refined = Mesh(
            mesh.devices.reshape(dp, row // 2, 2, group, col // group),
            ("dp", "y", "core", "lat", "sub"),
        )
        fast = (dp, row, col, latents) == (2, 4, 4, 2)
        token = P(("dp", *ROWS), COLS)
        weights = (
            P(ROWS, None, COLS),
            P(None, COLS),
            P(COLS, None, ROWS),
            P(None, ROWS),
            P(ROWS, COLS),
            P(COLS),
            P(COLS, ROWS),
            P(ROWS),
            P(ROWS, COLS),
            P(COLS),
        )
        given = P("dp", ROWS)
        return jax.shard_map(
            functools.partial(body, fast),
            mesh=refined,
            in_specs=(token, given, *weights, token),
            out_specs=(token, token, given, *weights),
            check_vma=False,
        )(*arrays)

    return run
```

```python
import functools
import math

import jax
import jax.numpy as jnp
from jax import lax
from jax.experimental import pallas as pl
from jax.experimental.layout import Layout, with_layout_constraint
from jax.experimental.pallas import tpu as pltpu
from jax.sharding import Mesh
from jax.sharding import PartitionSpec as P

HEAD_DIM = 64
LENGTH = 1024
EPS = 1e-06
LANES = 128
SCALE = HEAD_DIM ** (-0.5)
SCALE_LOG2 = SCALE * math.log2(math.e)
ROWS = ("y", "core")
COLS = ("lat", "sub")
NT = (((1,), (1,)), ((), ()))
F32 = jnp.float32
BF16 = jnp.bfloat16
VMEM_LIMIT = 56 * 1024 * 1024
LAST = []


def dot(left, right):
    return jnp.dot(left, right, preferred_element_type=F32)


def dot_nt(left, right):
    return lax.dot_general(left, right, NT, preferred_element_type=F32)


def gelu_and_slope(values):
    square = values * values
    half = 0.5 + 0.5 * jnp.tanh(0.7978845608028654 * values * (1.0 + 0.044715 * square))
    rate = (2 * 0.7978845608028654) * (1.0 + 3 * 0.044715 * square)
    return values * half, half + values * (half - half * half) * rate


def whole(shape):
    return pl.BlockSpec(shape, lambda *_: (0,) * len(shape))


def fixed(shape):
    return pl.BlockSpec(
        shape, lambda *_: (0,) * len(shape), pipeline_mode=pl.Buffered(1)
    )


def block(shape, column=0, first=0, step=1):
    return pl.BlockSpec((None, *shape), lambda b, *_: (first + step * b, 0, column))


def tabled(shape, place, start=0):
    row, column = place

    def index(b, table):
        return table[row, b], 0, start if column is None else start + table[column, b]

    return pl.BlockSpec((None, *shape), index)


def call(name, kernel, grid, in_specs, out_specs, out_shape, scratch=(), table=None):
    run = pl.pallas_call(
        kernel,
        grid_spec=pltpu.PrefetchScalarGridSpec(
            num_scalar_prefetch=0 if table is None else 1,
            grid=grid,
            in_specs=in_specs,
            out_specs=out_specs,
            scratch_shapes=list(scratch),
        ),
        out_shape=out_shape,
        compiler_params=pltpu.CompilerParams(vmem_limit_bytes=VMEM_LIMIT),
        cost_estimate=pl.CostEstimate(flops=0, bytes_accessed=0, transcendentals=0),
        name=name,
    )

    def ordered(first, *others):
        first = after(first, *LAST)
        found = run(first, *others) if table is None else run(table, first, *others)
        LAST[:] = jax.tree.leaves(found)[:1]
        return found

    return ordered


def after(value, *others):
    return lax.optimization_barrier((value, *others))[0]


def shaped(shape, dtype):
    return jax.ShapeDtypeStruct(shape, dtype)


def gate(values):
    def kernel(given, out):
        out[...] = given[...]

    return call(
        "gate", kernel, (1,), [whole(values.shape)], whole(values.shape), shaped(values.shape, values.dtype)
    )(values)


def project(left, query_blocks, kv_blocks, bias):
    number, features, _ = query_blocks.shape
    rows = left.shape[0]

    def kernel(a, g, h, c, query, kv):
        query[...] = (dot(a[...], g[...]) + c[:, :LANES]).astype(BF16)
        kv[:, :LANES] = dot(a[...], h[:, :LANES]).astype(BF16)
        kv[:, LANES:] = (dot(a[...], h[:, LANES:]) + c[:, LANES : 2 * LANES]).astype(BF16)

    return call(
        "project",
        kernel,
        (number,),
        [
            fixed(left.shape),
            block((features, LANES)),
            block((features, 2 * LANES)),
            block((1, bias.shape[-1])),
        ],
        [block((rows, LANES)), block((rows, 2 * LANES))],
        [shaped((number, rows, LANES), BF16), shaped((number, rows, 2 * LANES), BF16)],
    )(left, query_blocks, kv_blocks, bias)


def feed_forward(left, late, bias, extras):
    number, _, width = bias.shape
    rows, features = left.shape

    def kernel(a, g, h, c, middle, vectors, slopes, hidden, branch, output, total):
        low, slope = gelu_and_slope(dot(a[...], g[...]) + c[...])
        slopes[...] = slope
        low = low.astype(BF16)
        hidden[...] = low
        out = dot_nt(low, h[...])

        @pl.when(pl.program_id(0) == 0)
        def _():
            total[...] = out

        @pl.when(pl.program_id(0) > 0)
        def _():
            total[...] += out

        @pl.when(pl.program_id(0) == number - 1)
        def _():
            finish_output(total, (middle, vectors), (branch, output))

    return call(
        "feed_forward",
        kernel,
        (number,),
        [
            fixed(left.shape),
            block((features, width)),
            block((features, width), 1),
            block((1, width)),
        ]
        + [fixed(extra.shape) for extra in extras],
        [
            block((rows, width)),
            block((rows, width)),
            whole((rows, features)),
            whole((rows, features)),
        ],
        [
            shaped((number, rows, width), F32),
            shaped((number, rows, width), BF16),
            shaped((rows, features), F32),
            shaped((rows, features), BF16),
        ],
        scratch=[pltpu.VMEM((rows, features), F32)],
    )(left, late, late, bias, *extras)


def feed_back(name, low, turned, late, slopes, hidden, table, parts, extras, before):
    _, rows, width = slopes.shape
    features = low.shape[1]
    number = table.shape[1]
    part = width // parts
    more = [] if before is None else [before]

    def kernel(table_ref, *refs):
        low, turned_low, turned_in, shrink, grow, slope, after_act = refs[:7]
        refs = list(refs[7:])
        start = [refs.pop(0) for _ in more]
        given = [refs.pop(0) for _ in extras]
        shrink_outs = [refs.pop(0) for _ in range(parts)]
        expand_outs = [refs.pop(0) for _ in range(parts)]
        sums = refs.pop(0)
        results, total = (refs[:-1], refs[-1]) if extras else (None, refs[0])
        step = pl.program_id(0)
        back = (dot(low[...], shrink[...]) * slope[...]).astype(BF16)
        sums[...] = jnp.sum(back.astype(F32), axis=0, keepdims=True)
        side = table_ref[1, 0]
        for place in range(parts):
            here = slice(place * part, (place + 1) * part)
            found = dot(turned_low[...], after_act[:, here]).astype(BF16)
            grown = dot(turned_in[...], back[:, here]).astype(BF16)
            for index in range(parts):

                @pl.when(side == (place ^ index))
                def _():
                    shrink_outs[index][...] = found
                    expand_outs[index][...] = grown

        out = dot_nt(back, grow[...])

        @pl.when(step == 0)
        def _():
            total[...] = out + start[0][...] if start else out

        @pl.when(step > 0)
        def _():
            total[...] += out

        if extras:

            @pl.when(step == number - 1)
            def _():
                finish_middle_back(total, given, results)

    ends = [shaped((number, 1, width), F32)]
    if extras:
        ends += [
            shaped((rows, features), F32),
            shaped((rows, features), BF16),
            shaped((features, rows), BF16),
            shaped((4, features), F32),
        ]
    else:
        ends += [shaped((rows, features), F32)]
    outs = [shaped((number, features, part), BF16)] * (2 * parts)
    got = call(
        name,
        kernel,
        (number,),
        [
            fixed(low.shape),
            *[fixed(one.shape) for one in turned],
            tabled((features, width), (0, None), 1),
            tabled((features, width), (0, None), 0),
            tabled((rows, width), (0, None)),
            tabled((rows, width), (0, None)),
        ]
        + [fixed(one.shape) for one in (*more, *extras)],
        [block((features, part))] * (2 * parts)
        + [block((1, width))]
        + [whole(one.shape) for one in ends[1:]],
        outs + ends,
        scratch=[pltpu.VMEM((rows, features), F32)] if extras else (),
        table=table,
    )(low, *turned, late, late, slopes, hidden, *more, *extras)
    return got[:parts], got[parts : 2 * parts], got[2 * parts :]


def add_up(name, blocks, upper=None):
    _, features, width = blocks[0][0][0].shape
    tile = min(features if upper is None else features // 2, 512)
    terms = [one for block_terms in blocks for one in block_terms]
    count = len(blocks)

    def kernel(*refs):
        if upper is not None:
            refs = refs[1:]
        given = list(refs[: len(terms)]) if upper is None else list(refs[: 2 * len(terms)])
        outs = refs[len(given) :]

        def total(number):
            return sum(given.pop(0)[...].astype(F32) for _ in range(number)).astype(BF16)

        if upper is None:
            for index, one in enumerate(blocks):
                outs[0][index] = total(len(one))
        else:
            for out in outs:
                out[...] = total(len(terms))

    def spec(index, side=None):
        if side is None:
            return pl.BlockSpec((None, tile, width), lambda i: (index, i, 0))
        half = features // 2 // tile
        if side == 0:
            return pl.BlockSpec((None, tile, width), lambda i, t: (index, t[0] * half + i, 0))
        return pl.BlockSpec((None, tile, width), lambda i, t: (index, (1 - t[0]) * half + i, 0))

    arrays = [array for array, _ in terms]
    if upper is None:
        return call(
            name,
            kernel,
            (features // tile,),
            [spec(index) for _, index in terms],
            pl.BlockSpec((count, tile, width), lambda i: (0, i, 0)),
            shaped((count, features, width), BF16),
        )(*arrays)
    return call(
        name,
        kernel,
        (features // 2 // tile,),
        [spec(index, 0) for _, index in terms] + [spec(index, 1) for _, index in terms],
        [pl.BlockSpec((tile, width), lambda i, _: (i, 0))] * 2,
        [shaped((features // 2, width), BF16)] * 2,
        table=jnp.full((1,), upper, jnp.int32),
    )(*arrays, *arrays)


def attended_backward(left, late, table, start):
    number = table.shape[1]
    rows, features = left.shape

    def kernel(_, a, g, out):
        out[...] = dot(a[...], g[...]).astype(BF16)

    return call(
        "attended_back",
        kernel,
        (number,),
        [fixed(left.shape), tabled((features, LANES), (0, 1), start)],
        block((rows, LANES)),
        shaped((number, rows, LANES), BF16),
        table=table,
    )(left, late)


def contract(name, terms, extras, finish, outs, table=None):
    terms = [(left if isinstance(left, list) else [left], *more) for left, *more in terms]
    number = max(len(left) * left[0].shape[0] for left, _, _ in terms)
    rows = terms[0][0][0].shape[1]
    features = terms[0][1].shape[1]
    count, more = len(terms), len(extras)
    given_lefts = [one for left, _, _ in terms for one in left]

    def kernel(*refs):
        refs = list(refs if table is None else refs[1:])
        lefts = [chosen([refs.pop(0) for _ in left]) for left, _, _ in terms]
        rights = refs[:count]
        given = refs[count : count + more]
        results, total = refs[count + more : -1], refs[-1]
        out = dot_nt(lefts[0], rights[0][...])
        for left, right in zip(lefts[1:], rights[1:]):
            out = out + dot_nt(left, right[...])
        step = pl.program_id(0)

        @pl.when(step == 0)
        def _():
            total[...] = out

        @pl.when(step > 0)
        def _():
            total[...] += out

        @pl.when(step == number - 1)
        def _():
            finish(total, given, results)

    return call(
        name,
        kernel,
        (number,),
        [
            block(one.shape[1:], step=0 if len(left) > 1 else 1)
            for left, _, _ in terms
            for one in left
        ]
        + [where(features, left[0].shape[2]) for left, _, where in terms]
        + [fixed(extra.shape) for extra in extras],
        [whole(out.shape) for out in outs],
        outs,
        scratch=[pltpu.VMEM((rows, features), F32)],
        table=table,
    )(*given_lefts, *[right for _, right, _ in terms], *extras)


def by_rows(rows, sums, features, work, tile=64):
    tile = min(rows, tile)

    def step(i, totals):
        found = work(pl.ds(pl.multiple_of(i * tile, tile), tile))
        return tuple(
            total + jnp.sum(one.reshape(-1, 8, features), axis=0)
            for total, one in zip(totals, found)
        )

    zero = jnp.zeros((8, features), F32)
    totals = lax.fori_loop(0, rows // tile, step, (zero,) * sums)
    return [jnp.sum(total, axis=0, keepdims=True) for total in totals]


def normalize(values):
    average = jnp.mean(values, axis=1, keepdims=True)
    inverse = lax.rsqrt(
        jnp.mean(values * values, axis=1, keepdims=True) - average * average + EPS
    )
    return (values - average) * inverse, inverse


def norm_back(incoming, normed, inverse):
    return inverse * (
        incoming
        - jnp.mean(incoming, axis=1, keepdims=True)
        - normed * jnp.mean(incoming * normed, axis=1, keepdims=True)
    )


def enter(tokens, vectors):
    rows, features = tokens.shape

    def kernel(tokens, vectors, low, turned):
        shift, scale = vectors[0:1], 1.0 + vectors[1:2]

        def work(here):
            values = normalize(tokens[here, :].astype(F32))[0] * scale + shift
            values = values.astype(BF16)
            low[here, :] = values
            turned[:, here] = values.T
            return ()

        by_rows(rows, 0, features, work, LANES)

    return call(
        "enter",
        kernel,
        (1,),
        [whole(tokens.shape), whole(vectors.shape)],
        [whole((rows, features)), whole((features, rows))],
        [shaped((rows, features), BF16), shaped((features, rows), BF16)],
    )(tokens, vectors)


def enter_back(cotangent, branch, vectors):
    rows, features = cotangent.shape

    def kernel(cotangent, branch, vectors, low, turned, sums):
        gate = vectors[5:6]

        def work(here):
            upstream = cotangent[here, :].astype(F32)
            values = (gate * upstream).astype(BF16)
            low[here, :] = values
            turned[:, here] = values.T
            return values.astype(F32), branch[here, :] * upstream

        sums[...] = jnp.concatenate(by_rows(rows, 2, features, work, LANES), axis=0)

    return call(
        "enter_back",
        kernel,
        (1,),
        [whole(cotangent.shape), whole(branch.shape), whole(vectors.shape)],
        [whole((rows, features)), whole((features, rows)), whole((2, features))],
        [
            shaped((rows, features), BF16),
            shaped((features, rows), BF16),
            shaped((2, features), F32),
        ],
    )(cotangent, branch, vectors)


def finish_middle(total, given, results):
    tokens, vectors = given
    branch, middle, low, turned = results
    rows, features = total.shape
    shift, scale, gate = vectors[3:4], 1.0 + vectors[4:5], vectors[2:3]
    bias = vectors[6:7]

    def work(here):
        one = total[here, :] + bias
        branch[here, :] = one
        values = tokens[here, :].astype(F32) + gate * one
        middle[here, :] = values
        values = (normalize(values)[0] * scale + shift).astype(BF16)
        low[here, :] = values
        turned[:, here] = values.T
        return ()

    by_rows(rows, 0, features, work, LANES)


def finish_output(total, given, results):
    middle, vectors = given
    branch, output = results
    rows, features = total.shape
    gate, bias = vectors[5:6], vectors[7:8]

    def work(here):
        two = total[here, :] + bias
        branch[here, :] = two
        output[here, :] = (middle[here, :] + gate * two).astype(BF16)
        return ()

    by_rows(rows, 0, features, work)


def finish_middle_back(total, given, results):
    middle, branch, cotangent, vectors = given
    middle_back, low, turned, sums = results
    rows, features = total.shape
    gate, scale = vectors[2:3], 1.0 + vectors[4:5]

    def work(here):
        back = total[here, :]
        normed, inverse = normalize(middle[here, :])
        out = cotangent[here, :].astype(F32) + norm_back(back * scale, normed, inverse)
        middle_back[here, :] = out
        rounded = (gate * out).astype(BF16)
        low[here, :] = rounded
        turned[:, here] = rounded.T
        return back, back * normed, branch[here, :] * out, rounded.astype(F32)

    sums[...] = jnp.concatenate(by_rows(rows, 4, features, work, LANES), axis=0)


def finish_tokens_back(total, given, results):
    tokens, middle_back, vectors = given
    tokens_back, sums = results
    rows, features = total.shape
    scale = 1.0 + vectors[1:2]

    def work(here):
        back = total[here, :]
        normed, inverse = normalize(tokens[here, :].astype(F32))
        out = middle_back[here, :] + norm_back(back * scale, normed, inverse)
        tokens_back[here, :] = out.astype(BF16)
        return back, back * normed

    sums[...] = jnp.concatenate(by_rows(rows, 2, features, work), axis=0)


def chosen(parts):
    found = parts[0][...]
    for index, part in enumerate(parts[1:], 1):
        found = jnp.where(pl.program_id(0) == index, part[...], found)
    return found


def gradients(name, pairs, count, adds=(), form="one"):
    features, rows = pairs[0][0].shape
    parts = [one for _, parts in pairs for one in parts]
    width = sum(one.shape[2] for one, _ in parts)
    lefts, rights = len(pairs), len(parts)
    half = features // 2
    split = [isinstance(add[0], list) for add in adds]
    given = []
    for add, two in zip(adds, split):
        given += [(one[side][None], 0) for side in (0, 1) for one in add] if two else add

    def kernel(*refs):
        left_refs = refs[:lefts]
        right_refs = list(refs[lefts : lefts + rights])
        add_refs = list(refs[lefts + rights : lefts + rights + len(given)])
        outs = refs[lefts + rights + len(given) :]
        found = []
        for left, (_, own) in zip(left_refs, pairs):
            for _ in own:
                found.append(dot(left[...], right_refs.pop(0)[...]))
        out = found[0] if len(found) == 1 else jnp.concatenate(found, axis=1)
        for add, two in zip(adds, split):
            sides = [
                chosen([add_refs.pop(0) for _ in add]).astype(F32)
                for _ in range(2 if two else 1)
            ]
            out = out + (jnp.concatenate(sides, axis=0) if two else sides[0])
        out = out.astype(BF16)
        if form == "one":
            outs[0][...] = out
        else:
            for index in range(count):

                @pl.when(pl.program_id(0) == index)
                def _():
                    outs[2 * index][...] = out[:half]
                    outs[2 * index + 1][...] = out[half:]

    def addend(one):
        array, index = one
        return pl.BlockSpec((None, *array.shape[1:]), lambda *_: (index, 0, 0))

    if form == "one":
        out_specs, shape = [block((features, width))], (count, features, width)
    else:
        shape = (half, width)
        out_specs = [whole(shape)] * (2 * count)
    got = call(
        name,
        kernel,
        (count,),
        [fixed(left.shape) for left, _ in pairs]
        + [block(one.shape[1:], 0, first) for one, first in parts]
        + [addend(one) for one in given],
        out_specs,
        [shaped(shape, BF16)] * len(out_specs),
    )(
        *[left for left, _ in pairs],
        *[one for one, _ in parts],
        *[array for array, _ in given],
    )
    return got[0] if form == "one" else got


def attend(queries, pieces):
    number, rows, _ = queries.shape
    count = len(pieces)
    keys = sum(piece.shape[1] for piece in pieces)
    tile = min(rows, 256)

    def kernel(*refs):
        query, kv = refs[0], refs[1 : 1 + count]
        out_ref, log_ref = refs[1 + count :]
        head = lax.broadcasted_iota(jnp.int32, (1, LANES), 1) < HEAD_DIM

        def step(i, _):
            here = pl.ds(pl.multiple_of(i * tile, tile), tile)
            both = query[here, :]
            outs, logs = [], []
            for keep in (head, ~head):
                one = jnp.where(keep, both, jnp.zeros_like(both))
                scores = [dot_nt(one, piece[:, :LANES]) for piece in kv]
                top = functools.reduce(
                    jnp.maximum, [jnp.max(s, axis=1, keepdims=True) for s in scores]
                )
                weights = [jnp.exp2((s - top) * SCALE_LOG2) for s in scores]
                total = sum(jnp.sum(w, axis=1, keepdims=True) for w in weights)
                inverse = 1.0 / total
                out = sum(
                    dot((w * inverse).astype(BF16), piece[:, LANES:])
                    for w, piece in zip(weights, kv)
                )
                outs.append(out)
                logs.append(top * SCALE_LOG2 + jnp.log(total) * math.log2(math.e))
            out_ref[here, :] = jnp.where(head, outs[0], outs[1]).astype(BF16)
            table = jnp.where(head, logs[0], logs[1]).T
            log_ref[0:1, here] = table[0:1]
            log_ref[1:2, here] = table[HEAD_DIM : HEAD_DIM + 1]
            return 0

        lax.fori_loop(0, rows // tile, step, 0)

    return call(
        "attend",
        kernel,
        (number,),
        [block((rows, LANES))] + [block((piece.shape[1], 2 * LANES)) for piece in pieces],
        [block((rows, LANES)), block((2, rows))],
        [shaped((number, rows, LANES), BF16), shaped((number, 2, rows), F32)],
    )(queries, *pieces)


def attend_back(queries, pieces, logs, incoming, first, kinds, begin, number):
    rows = queries.shape[1]
    count = len(pieces)
    keys = sum(piece.shape[1] for piece in pieces)
    tile = min(rows, 256)

    def kernel(*refs):
        query, back_ref, log_ref = refs[:3]
        kv = refs[3 : 3 + count]
        query_back = refs[3 + count]
        kv_back = refs[4 + count : 4 + 2 * count]
        sums, scratch = refs[4 + 2 * count], refs[5 + 2 * count :]
        head = lax.broadcasted_iota(jnp.int32, (1, LANES), 1) < HEAD_DIM
        turned = [piece[:, :LANES].T for piece in kv]
        top = lax.broadcasted_iota(jnp.int32, (LANES, 1), 0) < HEAD_DIM
        for held in scratch:
            held[...] = jnp.zeros_like(held)

        def step(j, query_sum):
            here = pl.ds(pl.multiple_of(j * tile, tile), tile)
            backs = []
            for index, keep in enumerate((head, ~head)):
                zero = jnp.zeros((tile, LANES), BF16)
                one = jnp.where(keep, query[here, :], zero)
                back = jnp.where(keep, back_ref[here, :], zero)
                log = log_ref[index : index + 1, here]
                chances, mixes = [], []
                for piece in kv:
                    scores = dot_nt(piece[:, :LANES], one)
                    chances.append(jnp.exp2(scores * SCALE_LOG2 - log))
                    mixes.append(dot_nt(piece[:, LANES:], back))
                centre = sum(
                    jnp.sum(p * m, axis=0, keepdims=True) for p, m in zip(chances, mixes)
                )
                total = None
                for i in range(count):
                    score_back = (chances[i] * (mixes[i] - centre)).astype(BF16)
                    scratch[i][:, :LANES] += dot(score_back, one) * SCALE
                    scratch[i][:, LANES:] += dot(chances[i].astype(BF16), back)
                    term = dot(turned[i], score_back)
                    total = term if total is None else total + term
                backs.append(total)
            both = (jnp.where(top, backs[0], backs[1]).T * SCALE).astype(BF16)
            query_back[here, :] = both
            return query_sum + jnp.sum(both.astype(F32), axis=0, keepdims=True)

        sums[...] = lax.fori_loop(0, rows // tile, step, jnp.zeros((1, LANES), F32))
        for out, held in zip(kv_back, scratch):
            out[...] = held[...].astype(out.dtype)

    return call(
        "attend_back",
        kernel,
        (number,),
        [
            block((rows, LANES), first=begin),
            block((rows, LANES), first=first + begin),
            block((2, rows), first=begin),
        ]
        + [block((piece.shape[1], 2 * LANES), first=begin) for piece in pieces],
        [block((rows, LANES))]
        + [block((piece.shape[1], 2 * LANES)) for piece in pieces]
        + [block((1, LANES))],
        [shaped((number, rows, LANES), BF16)]
        + [
            shaped((number, piece.shape[1], 2 * LANES), kind)
            for piece, kind in zip(pieces, kinds)
        ]
        + [shaped((number, 1, LANES), F32)],
        scratch=[pltpu.VMEM((piece.shape[1], 2 * LANES), F32) for piece in pieces],
    )(queries, incoming, logs, *pieces)


def block_at(features, width):
    return block((features, width))


class Steps:
    def __init__(self, steps):
        self.steps, self.result = steps, None
        self.got = next(steps)

    def step(self):
        if self.result is None:
            try:
                self.got = self.steps.send(self.got)
            except StopIteration as end:
                self.got = self.result = end.value

    def hold(self):
        LAST.extend(jax.tree.leaves(self.got))

    def behind(self, *values):
        (*values, self.got) = lax.optimization_barrier((*values, self.got))
        return values

    def finish(self):
        while self.result is None:
            self.step()
        return self.result


class Plain:
    def __init__(self, sizes):
        self.latents, self.parts, self.width = sizes
        self.row = lax.axis_size("y") * lax.axis_size("core")
        self.col = lax.axis_size("lat") * lax.axis_size("sub")

    def scatter(self, values, held=None):
        rows, width = values.shape
        shaped_in = values.reshape(self.latents, 2, LENGTH // 2, width)
        halves = lax.all_to_all(shaped_in, "core", 1, 0, tiled=True)
        pieces = halves.reshape(self.col, -1, width)
        pieces = lax.all_to_all(pieces, COLS, 0, 0, tiled=True)
        return pieces.transpose(1, 0, 2).reshape(-1, self.col * width), held

    def collect_start(self, values):
        rows = values.shape[0]
        pieces = values.reshape(rows, self.col, -1).transpose(1, 0, 2)
        return [lax.all_to_all(pieces, COLS, 0, 0, tiled=True)]

    def collect(self, pieces):
        (pieces,) = pieces
        halves = pieces.reshape(2 * self.latents, 1, LENGTH // 2, -1)
        back = lax.all_to_all(halves, "core", 0, 1, tiled=True)
        return back.reshape(-1, self.width)

    def modulation(self, partial, bias, row_bias, col_bias):
        group = 2 * self.latents
        ours = lax.psum(partial, "core").reshape(-1, group, partial.shape[1])
        ours = lax.psum_scatter(ours, "y", scatter_dimension=0, tiled=True)[0] + bias
        sent = jnp.repeat(ours, self.col // group, axis=0)
        got = lax.all_to_all(sent, COLS, 0, 0, tiled=True)
        got = got.reshape(self.col, 6, -1).transpose(1, 0, 2).reshape(6, -1)
        cols = lax.all_gather(col_bias, COLS, axis=1, tiled=True)
        every = lax.all_gather(row_bias, ROWS, axis=0)
        return jnp.concatenate([got, cols], axis=0), [
            every.reshape(self.row * self.parts, 1, -1)
        ]

    def gather(self, parts, held):
        every = lax.all_gather(parts, COLS, axis=1, tiled=True)
        every = lax.all_gather(every, ROWS, axis=0, tiled=True)
        return [every[:, :, :LANES]], [every[:, :, LANES:]], held

    def gather_start(self, parts, held):
        return parts, held

    def gather_late(self, part):
        every = lax.all_gather(part, (*ROWS, *COLS), axis=0, tiled=True)
        return every.reshape(self.row, -1, part.shape[1])

    def expand_bias(self, row_bias, biases):
        every = lax.all_gather(row_bias, ROWS, axis=0)
        return every.reshape(self.row * self.parts, 1, -1)

    def with_units(self, row_sums, unit_sums):
        return [jnp.concatenate([row_sums[0], unit_sums[0]], axis=-1)]

    def tables(self):
        blocks = jnp.arange(self.row * self.parts, dtype=jnp.int32)
        return [jnp.stack([blocks // self.parts, blocks % self.parts])]


    def share(self, kv):
        return [[lax.all_gather(kv[0], ("core", "sub"), axis=1, tiled=True)]]

    def kinds(self):
        return [F32]

    PLACES = ((0, 0),)

    def give_back(self, backs):
        return [
            lax.psum_scatter(
                backs[0][0], ("core", "sub"), scatter_dimension=1, tiled=True
            ).astype(BF16)
        ]

    def sum_up(self, *args):
        return Steps(self.reduce(*args))

    def feed_back(self, low, turned, late, slopes, hidden, extras):
        table = jnp.stack([jnp.arange(self.row, dtype=jnp.int32)] * 2) * jnp.array(
            [[1], [0]], jnp.int32
        )
        shrink, grow, (sums, *ends) = feed_back(
            "feed_back", low, turned, late, slopes, hidden, table, self.parts, extras, None
        )

        def blocks(parts):
            return jnp.stack(parts, axis=1).reshape(-1, *parts[0].shape[1:])

        steps = [Steps(self.reduce_ready(blocks(one))) for one in (shrink, grow)]
        return steps, ends, [sums.reshape(self.row * self.parts, 1, -1)]

    def reduce(self, name, pairs):
        grads = gradients(name, pairs(0, 0, 0), self.row * self.parts)
        return (yield from self.reduce_ready(grads))

    def reduce_ready(self, grads):
        grads = grads.astype(F32)
        grads = yield grads
        grads = lax.psum_scatter(grads, ROWS, scatter_dimension=0, tiled=True)
        grads = lax.psum_scatter(grads, COLS, scatter_dimension=1, tiled=True)
        return lax.psum(grads, "dp")

    def small(self, vectors, row_sums, col_sums):
        every = ("dp", *ROWS, *COLS)
        group = 2 * self.latents
        total = yield lax.psum(vectors, ("core", "sub"))
        total = total.astype(BF16)
        mine = lax.all_gather(total[:, None], "lat", axis=1, tiled=True)
        mine = lax.all_gather(mine, "y", axis=1, tiled=True)
        mine = lax.all_gather(mine, "dp", axis=1, tiled=True)
        col = lax.axis_index("lat") * lax.axis_size("sub") + lax.axis_index("sub")
        cut = lax.dynamic_slice_in_dim(mine, col * self.width, self.width, axis=2)
        cut = cut.transpose(1, 0, 2).reshape(mine.shape[1], -1)
        rows = lax.psum(row_sums[0], every).reshape(self.row, self.parts, -1)
        row = lax.axis_index("y") * 2 + lax.axis_index("core")
        rows = lax.dynamic_index_in_dim(rows, row, 0, keepdims=False)
        cols = lax.psum(col_sums, every)
        cols = lax.dynamic_slice_in_dim(cols, col * self.width, self.width, axis=1)
        return cut, rows, cols

    def col_sum(self, values):
        return lax.psum(values, COLS)

    def both_groups(self, values):
        return lax.all_gather(values, "dp", axis=0, tiled=True)


class Cube(Plain):
    PLACES = ((0, 0), (0, 1), (1, 0), (1, 1))

    def __init__(self, sizes):
        super().__init__(sizes)
        self.x = lax.axis_index("dp")
        self.y = lax.axis_index("y")
        self.c = lax.axis_index("core")
        self.z = lax.axis_index("lat")

    def swap(self, values, axis):
        return lax.ppermute(values, axis, [(0, 1), (1, 0)])

    def along(self, values, bits):
        return lax.ppermute(values, "lat", [(i, i ^ bits) for i in range(4)])

    def scatter(self, values, held=None):
        rows, width = values.shape
        halves = values.reshape(self.latents, 2, LENGTH // 2, width)
        keep = lax.dynamic_index_in_dim(halves, self.c, 1, keepdims=False)
        send = lax.dynamic_index_in_dim(halves, 1 - self.c, 1, keepdims=False)
        every = jnp.concatenate([keep, self.swap(send, "core")], axis=0)
        if held is not None:
            every, held = lax.optimization_barrier((every, held))
        pieces = []
        for latent in range(4):
            index = ((latent // 2) ^ self.c) * 2 + latent % 2
            pieces.append(lax.dynamic_index_in_dim(every, index, 0, keepdims=False))
        pieces = lax.all_to_all(jnp.stack(pieces), "lat", 0, 0, tiled=True)
        return pieces.transpose(1, 0, 2).reshape(-1, 4 * width), held

    def placed(self, pieces):
        odd, high = self.z % 2 == 1, self.z >= 2
        one, two, three, four = pieces
        one, two = jnp.where(odd, two, one), jnp.where(odd, one, two)
        three, four = jnp.where(odd, four, three), jnp.where(odd, three, four)
        return [
            jnp.where(high, three, one),
            jnp.where(high, four, two),
            jnp.where(high, one, three),
            jnp.where(high, two, four),
        ]

    def collect_start(self, values):
        pieces = values.reshape(-1, 4, self.width).transpose(1, 0, 2)
        return [lax.all_to_all(pieces, "lat", 0, 0, tiled=True)]

    def collect(self, pieces):
        width = self.width
        every = pieces[0].reshape(2, 2, -1, width)

        def latents(core):
            return lax.dynamic_index_in_dim(every, core, 0, keepdims=False)

        keep = latents(self.c)
        got = self.swap(latents(1 - self.c), "core")
        first = jnp.where(self.c == 0, keep, got)
        second = jnp.where(self.c == 0, got, keep)
        return jnp.stack([first, second], axis=1).reshape(-1, width)

    def modulation(self, partial, bias, row_bias, col_bias):
        span = partial.shape[1]
        own = row_bias.reshape(1, -1)
        got = self.swap(jnp.concatenate([partial, own], axis=0), "core")
        ours, other = partial + got[:-1], got[-1:]
        halves = ours.reshape(2, 4, span)
        keep = lax.dynamic_index_in_dim(halves, self.y, 0, keepdims=False)
        send = lax.dynamic_index_in_dim(halves, 1 - self.y, 0, keepdims=False)
        got = self.swap(jnp.concatenate([send, own, other], axis=0), "y")
        ours = keep + got[:4] + bias
        rows = jnp.stack([own, got[4:5], other, got[5:6]]).reshape(2, 2, 2, -1)
        flip = jnp.stack([rows[:, :, 1], rows[:, :, 0]], axis=2)
        rows = jnp.where(self.x == 0, rows, flip).transpose(2, 0, 1, 3)[:, :, :, None]
        pieces = []
        for bits in range(4):
            piece = lax.dynamic_index_in_dim(ours, self.z ^ bits, 0, keepdims=False)
            piece = jnp.concatenate([piece.reshape(6, -1), col_bias], axis=0)
            pieces.append(piece if bits == 0 else self.along(piece, bits))
        vectors = jnp.concatenate(self.placed(pieces), axis=1)
        return vectors, [rows[x, core] for x, core in self.PLACES]

    def gather_start(self, parts, held):
        part = lax.dynamic_index_in_dim(parts, self.x, 0, keepdims=False)
        odd, high = self.z % 2 == 1, self.z >= 2
        got = self.along(part, 1)
        part = jnp.concatenate([jnp.where(odd, got, part), jnp.where(odd, part, got)], axis=0)
        part, held = lax.optimization_barrier((part, held))
        got = self.along(part, 2)
        part = jnp.concatenate(
            [jnp.where(high, got, part), jnp.where(high, part, got)], axis=0
        )

        return part, held

    def gather(self, part, held):
        one, two = part[:, :LANES], part[:, LANES:]
        one_pair = jnp.stack([one, self.swap(one, "dp")])
        near = jnp.stack([two, self.swap(two, "y")])
        near = after(near, one_pair)
        far = self.swap(near, "dp")
        kv = [near, self.swap(near, "core"), far, self.swap(far, "core")]
        got = self.swap(one_pair, "y")
        near = jnp.stack([one_pair[0], got[0]])
        far = jnp.stack([one_pair[1], got[1]])
        near, held = lax.optimization_barrier((near, held))
        queries = [near, self.swap(near, "core"), far, self.swap(far, "core")]
        return queries, kv, held

    def expand_bias(self, row_bias, biases):
        number = self.row * self.parts
        table = jnp.concatenate(self.tables(), axis=1)
        place = table[0] * self.parts + table[1]
        chosen = place[None, :] == lax.broadcasted_iota(jnp.int32, (number, number), 0)
        every = jnp.concatenate(biases, axis=0)[:, 0]
        found = jnp.dot(chosen.astype(F32), every, precision=lax.Precision.HIGHEST)
        return found[:, None]

    def with_units(self, row_sums, unit_sums):
        found = []
        for one, (x, core) in zip(row_sums, self.PLACES):
            units = unit_sums[1 - core][2 * x : 2 * x + 2]
            found.append(jnp.concatenate([one, units], axis=-1))
        return found

    def tables(self):
        side = jnp.arange(2, dtype=jnp.int32)
        return [
            jnp.stack(
                [(side ^ self.y) * 2 + (self.c ^ core), jnp.full((2,), self.x ^ x)]
            ).astype(jnp.int32)
            for x, core in self.PLACES
        ]

    def share(self, kv):
        return [
            [kv[2 * x + core], self.swap(kv[2 * x + 1 - core], "core")]
            for x, core in self.PLACES
        ]

    def kinds(self):
        return [F32, BF16]

    def give_back(self, backs):
        got = [self.swap(backs[1 - core][1], "core") for core in (0, 1)]
        return [(own[0] + one.astype(F32)).astype(BF16) for own, one in zip(backs, got)]

    def feed_back(self, low, turned, late, slopes, hidden, extras):
        tables = self.tables()
        found, sums, before = [], [], None
        for core in (1, 0):
            rows = tables[core][0]
            shrink, grow, (one, *ends) = feed_back(
                "feed_back",
                low,
                turned,
                late,
                slopes,
                hidden,
                jnp.stack([rows, jnp.full((2,), self.x, jnp.int32)]),
                self.parts,
                [] if core else extras,
                before,
            )
            if core:
                (before,) = ends
                found = [[self.swap(one, "core") for one in part] for part in (shrink, grow)]
            else:
                LAST.extend([one for part in found for one in part])
                steps = [
                    Steps(self.reduce_ready(name, near, far, order))
                    for name, near, far, order in (
                        ("d_shrink", shrink, found[0], "yx"),
                        ("d_expand", grow, found[1], "xy"),
                    )
                ]
            one = one.reshape(2, 1, self.parts, -1).transpose(2, 0, 1, 3)
            one = jnp.where(self.x == 0, one, jnp.stack([one[1], one[0]]))
            sums.append(one.reshape(4, 1, -1))
        return steps, ends, sums

    def reduce_ready(self, name, near, far, order):
        axes, one, two = (("dp", "y"), 2, 1) if order == "xy" else (("y", "dp"), 1, 2)
        near, far = (
            [(part[x], y) for x in (0, 1) for y in (0, 1)] for part in (near, far)
        )
        sent = add_up(name, [[near[one], far[one]], [near[3], far[3]]])
        second = yield self.swap(sent, axes[0])
        sent = add_up(name, [[near[two], far[two], (second, 1)]])
        third = yield self.swap(sent, axes[1])
        terms = [near[0], far[0], (second, 0), (third, 0)]
        return (yield from self.reduce_col(add_up(name, [terms])))

    def reduce_col(self, blocks):
        own = yield lax.psum_scatter(blocks[0], COLS, scatter_dimension=0, tiled=True)
        got = yield self.swap(gate(own), "dp")
        return jnp.stack(
            [jnp.where(self.x == 0, own, got), jnp.where(self.x == 0, got, own)]
        ).astype(F32)

    def reduce(self, name, pairs):
        def grads(place, count, adds=(), form="one"):
            return gradients(name, pairs(*place), count, adds, form)

        def far(place, count):
            sent = grads(place, count, form="apart")
            return [self.swap(one, "core") for one in sent]

        near = yield far((1, 0, 1), 2)
        second = yield self.swap(grads((1, 0, 0), 2, [[near[:2], near[2:]]]), "dp")
        near = yield far((0, 1, 1), 1)
        last = yield far((0, 0, 1), 1)
        third = yield self.swap(grads((0, 1, 0), 1, [[near], [(second, 1)]]), "y")
        adds = [[last], [(second, 0)], [(third, 0)]]
        return (yield from self.reduce_col(grads((0, 0, 0), 1, adds)))

    def small(self, vectors, row_sums, col_sums):
        span = row_sums[0].shape[-1]
        features = vectors.shape[1]

        def flat(*parts):
            return jnp.concatenate([part.reshape(-1, LANES) for part in parts], axis=0)

        def cut(message, *shapes):
            parts, start = [], 0
            for shape in shapes:
                size = math.prod(shape) // LANES
                parts.append(message[start : start + size].reshape(shape))
                start += size
            return parts

        every = jnp.stack(row_sums).reshape(2, 2, 2, span)
        rows0, rows1 = every[:, 0], every[:, 1]
        got = yield self.swap(gate(flat(rows1, col_sums, vectors)), "core")
        got = cut(got, rows1.shape, col_sums.shape, vectors.shape)
        rows, cols = rows0 + got[0], col_sums + got[1]
        mine = (vectors + got[2]).astype(BF16).astype(F32)
        got = yield self.swap(gate(flat(rows[:, 1], cols, mine)), "y")
        got = cut(got, (2, span), cols.shape, mine.shape)
        rows, cols = rows[:, 0] + got[0], cols + got[1]
        pair = jnp.stack([mine, got[2]])
        got = yield self.swap(gate(flat(rows, cols, pair)), "dp")
        got = cut(got, rows.shape, cols.shape, pair.shape)
        rows = rows + jnp.stack([got[0][1], got[0][0]])
        rows = jnp.where(self.x == 0, rows, jnp.stack([rows[1], rows[0]]))
        cols = cols + got[1]
        four = jnp.stack([pair, got[2]]).reshape(4, 6, features)
        width = self.width

        def cuts(values):
            return self.placed(
                [values[..., i * width : (i + 1) * width] for i in range(4)]
            )

        found = []
        for bits, piece in enumerate(zip(cuts(four), cuts(cols))):
            piece = [*piece, rows]
            if bits:
                got = self.along(flat(*piece), bits)
                piece = cut(got, *[part.shape for part in piece])
            found.append(piece)
        tree = [(found[0][i] + found[1][i]) + (found[2][i] + found[3][i]) for i in (1, 2)]
        every = jnp.stack([one[0] for one in found])
        every = every.reshape(16, -1)
        place = lax.broadcasted_iota(jnp.int32, (16, 16), 0)
        held = lax.broadcasted_iota(jnp.int32, (16, 16), 1)
        latent = (
            (((held // 2) % 2) ^ self.x) * 8 + ((held % 2) ^ self.y) * 4 + ((held // 4) ^ self.z)
        )
        chosen = (latent == place).astype(F32)
        every = jnp.dot(chosen, every, precision=lax.Precision.HIGHEST).astype(BF16)
        return every, tree[1], tree[0]

    def col_sum(self, values):
        got = [values] + [self.along(values, bits) for bits in (1, 2, 3)]
        return (got[0] + got[1]) + (got[2] + got[3])

    def both_groups(self, values):
        got = self.swap(values, "dp")
        return jnp.where(
            self.x == 0,
            jnp.concatenate([values, got], axis=0),
            jnp.concatenate([got, values], axis=0),
        )


def body(
    fast,
    tokens,
    condition,
    modulation_weight,
    modulation_bias,
    input_weight,
    input_bias,
    output_weight,
    output_bias,
    expand_weight,
    expand_bias,
    shrink_weight,
    shrink_bias,
    cotangent,
):
    LAST.clear()
    width = tokens.shape[1]
    inner = input_weight.shape[2]
    parts = inner // LANES
    units = expand_weight.shape[1] // parts
    sizes = (tokens.shape[0] // LENGTH, parts, width)
    net = (Cube if fast else Plain)(sizes)

    own_in = (
        input_weight.reshape(width, 3, parts, LANES)
        .transpose(2, 0, 1, 3)
        .reshape(parts, width, 3 * LANES)
    )
    own_late = with_layout_constraint(
        jnp.concatenate([expand_weight, shrink_weight.T, output_weight.T], axis=1),
        Layout((0, 1)),
    )
    out_start = 2 * parts * units // LANES

    condition_float = condition.astype(F32)
    silu_low = jax.nn.silu(condition_float).astype(BF16)
    modulator = modulation_weight.reshape(modulation_weight.shape[0], -1)
    row_bias = jnp.concatenate(
        [
            input_bias.reshape(2, parts, LANES).transpose(1, 0, 2).reshape(parts, -1),
            expand_bias.reshape(parts, units),
        ],
        axis=1,
    ).astype(F32)
    late = net.gather_late(own_late)
    vectors, row_biases = net.modulation(
        dot(silu_low, modulator),
        modulation_bias.astype(F32).reshape(1, -1),
        row_bias,
        jnp.stack([output_bias, shrink_bias]).astype(F32),
    )
    silu_all = net.both_groups(silu_low)
    own_in, (vectors, silu_all) = net.gather_start(own_in, (vectors, silu_all))
    mine, own_in = net.scatter(tokens, own_in)
    query_bufs, kv_bufs, mine = net.gather(own_in, mine)
    rows = mine.shape[0]
    features = mine.shape[1]
    expand_biases = net.expand_bias(
        row_bias[:, 2 * LANES :], [one[..., 2 * LANES :] for one in row_biases]
    )
    tables = net.tables()

    low_one, turned_one = enter(mine, vectors)
    queries, own_kv = [], []
    for one, two, bias in zip(query_bufs, kv_bufs, row_biases):
        one, two = project(low_one, one, two, bias)
        queries.append(one)
        own_kv.append(two)
    kv = net.share(own_kv)
    attended, logs = [], []
    for one, pieces in zip(queries, kv):
        out, log = attend(one, pieces)
        attended.append(out)
        logs.append(log)
    back, (late, attended[-1]) = net.scatter(cotangent, (late, attended[-1]))

    def out_place(number):
        def place(features, width):
            return tabled((features, width), (2 * number, 2 * number + 1), out_start)

        return place

    branch_one, middle, low_two, turned_two = contract(
        "out",
        [(one, late, out_place(i)) for i, one in enumerate(attended)],
        [mine, vectors],
        finish_middle,
        [
            shaped((rows, features), F32),
            shaped((rows, features), F32),
            shaped((rows, features), BF16),
            shaped((features, rows), BF16),
        ],
        table=jnp.concatenate(tables, axis=0),
    )
    slopes, hidden, branch_two, output = feed_forward(
        low_two, late, expand_biases.reshape(-1, 1, parts * units), [middle, vectors]
    )
    branch_two_back, turned_two_back, sums_back = enter_back(back, branch_two, vectors)
    shrink_sum, gate_two_back = sums_back[0:1], sums_back[1:2]

    steps, ends, expand_sums = net.feed_back(
        branch_two_back,
        (turned_two_back, turned_two),
        late,
        slopes,
        hidden,
        [middle, branch_one, back, vectors],
    )
    middle_back, branch_one_back, turned_one_back, sums_two = ends
    shrink_steps, expand_steps = steps
    incoming = attended_backward(
        branch_one_back, late, jnp.concatenate(tables, axis=1), out_start
    )
    output = net.collect_start(gate(output))
    number = len(kv)
    blocks = queries[0].shape[0]
    found = {}

    def attention_back(i, begin, count):
        got = attend_back(
            queries[i], kv[i], logs[i], incoming, i * blocks, net.kinds(), begin, count
        )
        found[i, begin] = [got[0], got[1:-1], got[-1]]

    def kv_final(keys):
        for key, one in zip(keys, net.give_back([found[key][1] for key in keys])):
            found[key][1] = one

    def pairs(x, y, core):
        i = 2 * x + core
        key, begin = ((i, 0), y) if (i, 1) not in found else ((i, y), 0)
        heads = [(found[key][0], begin), (found[key][1], begin)]
        return [(turned_one, heads), (turned_one_back, [(attended[i], y)])]

    def every_block(i, which):
        ones = [found[key][which] for key in sorted(found) if key[0] == i]
        return ones if len(ones) > 1 else ones[0]

    if number > 1:
        attention_back(3, 0, 2)
        attention_back(2, 0, 2)
        LAST.extend(output)
        shrink_steps.hold()
        expand_steps.hold()
        shrink_steps.step()
        expand_steps.step()
        kv_final([(2, 0), (3, 0)])
        in_steps = net.sum_up("d_in", pairs)
        attention_back(1, 1, 1)
        in_steps.step()
        attention_back(0, 1, 1)
        shrink_steps.step()
        kv_final([(0, 1), (1, 1)])
        in_steps.step()
        attention_back(1, 0, 1)
        attention_back(0, 0, 1)
        expand_steps.step()
        kv_final([(0, 0), (1, 0)])
        in_steps.step()
        in_steps.step()
    else:
        attention_back(0, 0, blocks)
        kv_final([(0, 0)])
        in_steps = net.sum_up("d_in", pairs)
    shrink_steps.hold()
    tokens_back, sums_one = contract(
        "tokens_back",
        [(every_block(i, 0), buf, block_at) for i, buf in enumerate(query_bufs)]
        + [(every_block(i, 1), buf, block_at) for i, buf in enumerate(kv_bufs)],
        [mine, middle_back, vectors],
        finish_tokens_back,
        [shaped((rows, features), BF16), shaped((2, features), F32)],
    )
    summed = jnp.concatenate([sums_one, sums_two[2:3], sums_two[0:2], gate_two_back], axis=0)

    def value_sum(one):
        return jnp.sum(one[:, :, LANES:].astype(F32), axis=1, keepdims=True)

    row_sums = []
    for i in range(number):
        ones = [found[key] for key in sorted(found) if key[0] == i]
        row_sums.append(
            jnp.concatenate(
                [
                    jnp.concatenate([one[2], value_sum(one[1])], axis=-1)
                    for one in ones
                ]
            )
        )
    row_sums = net.with_units(row_sums, expand_sums)
    col_sums = jnp.concatenate([sums_two[3:4], shrink_sum], axis=0)
    tokens_back = net.collect_start(gate(tokens_back))
    small_steps = Steps(net.small(summed, row_sums, col_sums))
    in_steps.step()
    small_steps.step()
    LAST.extend(tokens_back)
    small_steps.step()
    shrink_steps.step()
    expand_steps.step()
    in_steps.step()
    shrink_parts = shrink_steps.finish()
    expand_parts = expand_steps.finish()
    in_parts = in_steps.finish()

    every, row_found, col_found = small_steps.finish()
    modulation_weight_gradient = lax.dot_general(
        silu_all, every, (((0,), (0,)), ((), ())), preferred_element_type=F32
    ).reshape(modulation_weight.shape)
    modulation_bias_gradient = jnp.sum(every.astype(F32), axis=0).reshape(6, width)
    groups = condition.shape[0]
    ours = lax.dynamic_slice_in_dim(every, lax.axis_index("dp") * groups, groups, axis=0)
    silu_back = net.col_sum(dot_nt(ours, modulator))
    silu_pull = jax.vjp(jax.nn.silu, condition_float)[1]
    condition_gradient = silu_pull(silu_back)[0]

    return (
        net.collect(output),
        net.collect(tokens_back).astype(F32),
        condition_gradient,
        modulation_weight_gradient,
        modulation_bias_gradient,
        in_parts[:, :, : 3 * LANES]
        .reshape(parts, width, 3, LANES)
        .transpose(1, 2, 0, 3)
        .reshape(input_weight.shape),
        row_found[:, : 2 * LANES]
        .reshape(parts, 2, LANES)
        .transpose(1, 0, 2)
        .reshape(input_bias.shape),
        in_parts[:, :, 3 * LANES :].transpose(0, 2, 1).reshape(output_weight.shape),
        col_found[0],
        expand_parts.transpose(1, 0, 2).reshape(expand_weight.shape),
        row_found[:, 2 * LANES :].reshape(expand_bias.shape),
        shrink_parts.transpose(0, 2, 1).reshape(shrink_weight.shape),
        col_found[1],
    )


def solution(mesh):
    dp, row, col = (mesh.shape[name] for name in ("dp", "row", "col"))

    def run(*arrays):
        latents = arrays[0].shape[0] // (dp * row * LENGTH)
        group = 2 * latents
        refined = Mesh(
            mesh.devices.reshape(dp, row // 2, 2, group, col // group),
            ("dp", "y", "core", "lat", "sub"),
        )
        fast = (dp, row, col, latents) == (2, 4, 4, 2)
        token = P(("dp", *ROWS), COLS)
        weights = (
            P(ROWS, None, COLS),
            P(None, COLS),
            P(COLS, None, ROWS),
            P(None, ROWS),
            P(ROWS, COLS),
            P(COLS),
            P(COLS, ROWS),
            P(ROWS),
            P(ROWS, COLS),
            P(COLS),
        )
        given = P("dp", ROWS)
        return jax.shard_map(
            functools.partial(body, fast),
            mesh=refined,
            in_specs=(token, given, *weights, token),
            out_specs=(token, token, given, *weights),
            check_vma=False,
        )(*arrays)

    return run
```

```python
import functools
import math

import jax
import jax.numpy as jnp
from jax import lax
from jax.experimental import pallas as pl
from jax.experimental.layout import Layout, with_layout_constraint
from jax.experimental.pallas import tpu as pltpu
from jax.sharding import Mesh
from jax.sharding import PartitionSpec as P

HEAD_DIM = 64
LENGTH = 1024
EPS = 1e-06
LANES = 128
SCALE = HEAD_DIM ** (-0.5)
SCALE_LOG2 = SCALE * math.log2(math.e)
ROWS = ("y", "core")
COLS = ("lat", "sub")
NT = (((1,), (1,)), ((), ()))
F32 = jnp.float32
BF16 = jnp.bfloat16
VMEM_LIMIT = 56 * 1024 * 1024
LAST = []


def dot(left, right):
    return jnp.dot(left, right, preferred_element_type=F32)


def dot_nt(left, right):
    return lax.dot_general(left, right, NT, preferred_element_type=F32)


def gelu_and_slope(values):
    square = values * values
    half = 0.5 + 0.5 * jnp.tanh(0.7978845608028654 * values * (1.0 + 0.044715 * square))
    rate = (2 * 0.7978845608028654) * (1.0 + 3 * 0.044715 * square)
    return values * half, half + values * (half - half * half) * rate


def whole(shape):
    return pl.BlockSpec(shape, lambda *_: (0,) * len(shape))


def fixed(shape):
    return pl.BlockSpec(
        shape, lambda *_: (0,) * len(shape), pipeline_mode=pl.Buffered(1)
    )


def block(shape, column=0, first=0, step=1):
    return pl.BlockSpec((None, *shape), lambda b, *_: (first + step * b, 0, column))


def tabled(shape, place, start=0):
    row, column = place

    def index(b, table):
        return table[row, b], 0, start if column is None else start + table[column, b]

    return pl.BlockSpec((None, *shape), index)


def call(name, kernel, grid, in_specs, out_specs, out_shape, scratch=(), table=None):
    run = pl.pallas_call(
        kernel,
        grid_spec=pltpu.PrefetchScalarGridSpec(
            num_scalar_prefetch=0 if table is None else 1,
            grid=grid,
            in_specs=in_specs,
            out_specs=out_specs,
            scratch_shapes=list(scratch),
        ),
        out_shape=out_shape,
        compiler_params=pltpu.CompilerParams(vmem_limit_bytes=VMEM_LIMIT),
        cost_estimate=pl.CostEstimate(flops=0, bytes_accessed=0, transcendentals=0),
        name=name,
    )

    def ordered(first, *others):
        first = after(first, *LAST)
        found = run(first, *others) if table is None else run(table, first, *others)
        LAST[:] = jax.tree.leaves(found)[:1]
        return found

    return ordered


def after(value, *others):
    return lax.optimization_barrier((value, *others))[0]


def shaped(shape, dtype):
    return jax.ShapeDtypeStruct(shape, dtype)


def gate(values):
    def kernel(given, out):
        out[...] = given[...]

    return call(
        "gate", kernel, (1,), [whole(values.shape)], whole(values.shape), shaped(values.shape, values.dtype)
    )(values)


def project(left, query_blocks, kv_blocks, bias):
    number, features, _ = query_blocks.shape
    rows = left.shape[0]

    def kernel(a, g, h, c, query, kv):
        query[...] = (dot(a[...], g[...]) + c[:, :LANES]).astype(BF16)
        kv[:, :LANES] = dot(a[...], h[:, :LANES]).astype(BF16)
        kv[:, LANES:] = (dot(a[...], h[:, LANES:]) + c[:, LANES : 2 * LANES]).astype(BF16)

    return call(
        "project",
        kernel,
        (number,),
        [
            fixed(left.shape),
            block((features, LANES)),
            block((features, 2 * LANES)),
            block((1, bias.shape[-1])),
        ],
        [block((rows, LANES)), block((rows, 2 * LANES))],
        [shaped((number, rows, LANES), BF16), shaped((number, rows, 2 * LANES), BF16)],
    )(left, query_blocks, kv_blocks, bias)


def feed_forward(left, late, bias, extras):
    number, _, width = bias.shape
    rows, features = left.shape

    def kernel(a, g, h, c, middle, vectors, slopes, hidden, branch, output, total):
        low, slope = gelu_and_slope(dot(a[...], g[...]) + c[...])
        slopes[...] = slope
        low = low.astype(BF16)
        hidden[...] = low
        out = dot_nt(low, h[...])

        @pl.when(pl.program_id(0) == 0)
        def _():
            total[...] = out

        @pl.when(pl.program_id(0) > 0)
        def _():
            total[...] += out

        @pl.when(pl.program_id(0) == number - 1)
        def _():
            finish_output(total, (middle, vectors), (branch, output))

    return call(
        "feed_forward",
        kernel,
        (number,),
        [
            fixed(left.shape),
            block((features, width)),
            block((features, width), 1),
            block((1, width)),
        ]
        + [fixed(extra.shape) for extra in extras],
        [
            block((rows, width)),
            block((rows, width)),
            whole((rows, features)),
            whole((rows, features)),
        ],
        [
            shaped((number, rows, width), F32),
            shaped((number, rows, width), BF16),
            shaped((rows, features), F32),
            shaped((rows, features), BF16),
        ],
        scratch=[pltpu.VMEM((rows, features), F32)],
    )(left, late, late, bias, *extras)


def feed_back(name, low, turned, late, slopes, hidden, table, parts, extras, before):
    _, rows, width = slopes.shape
    features = low.shape[1]
    number = table.shape[1]
    part = width // parts
    more = [] if before is None else [before]

    def kernel(table_ref, *refs):
        low, turned_low, turned_in, shrink, grow, slope, after_act = refs[:7]
        refs = list(refs[7:])
        start = [refs.pop(0) for _ in more]
        given = [refs.pop(0) for _ in extras]
        shrink_outs = [refs.pop(0) for _ in range(parts)]
        expand_outs = [refs.pop(0) for _ in range(parts)]
        sums = refs.pop(0)
        results, total = (refs[:-1], refs[-1]) if extras else (None, refs[0])
        step = pl.program_id(0)
        back = (dot(low[...], shrink[...]) * slope[...]).astype(BF16)
        sums[...] = jnp.sum(back.astype(F32), axis=0, keepdims=True)
        side = table_ref[1, 0]
        for place in range(parts):
            here = slice(place * part, (place + 1) * part)
            found = dot(turned_low[...], after_act[:, here]).astype(BF16)
            grown = dot(turned_in[...], back[:, here]).astype(BF16)
            for index in range(parts):

                @pl.when(side == (place ^ index))
                def _():
                    shrink_outs[index][...] = found
                    expand_outs[index][...] = grown

        out = dot_nt(back, grow[...])

        @pl.when(step == 0)
        def _():
            total[...] = out + start[0][...] if start else out

        @pl.when(step > 0)
        def _():
            total[...] += out

        if extras:

            @pl.when(step == number - 1)
            def _():
                finish_middle_back(total, given, results)

    ends = [shaped((number, 1, width), F32)]
    if extras:
        ends += [
            shaped((rows, features), F32),
            shaped((rows, features), BF16),
            shaped((features, rows), BF16),
            shaped((4, features), F32),
        ]
    else:
        ends += [shaped((rows, features), F32)]
    outs = [shaped((number, features, part), BF16)] * (2 * parts)
    got = call(
        name,
        kernel,
        (number,),
        [
            fixed(low.shape),
            *[fixed(one.shape) for one in turned],
            tabled((features, width), (0, None), 1),
            tabled((features, width), (0, None), 0),
            tabled((rows, width), (0, None)),
            tabled((rows, width), (0, None)),
        ]
        + [fixed(one.shape) for one in (*more, *extras)],
        [block((features, part))] * (2 * parts)
        + [block((1, width))]
        + [whole(one.shape) for one in ends[1:]],
        outs + ends,
        scratch=[pltpu.VMEM((rows, features), F32)] if extras else (),
        table=table,
    )(low, *turned, late, late, slopes, hidden, *more, *extras)
    return got[:parts], got[parts : 2 * parts], got[2 * parts :]


def add_up(name, blocks, upper=None):
    _, features, width = blocks[0][0][0].shape
    tile = min(features if upper is None else features // 2, 512)
    terms = [one for block_terms in blocks for one in block_terms]
    count = len(blocks)

    def kernel(*refs):
        if upper is not None:
            refs = refs[1:]
        given = list(refs[: len(terms)]) if upper is None else list(refs[: 2 * len(terms)])
        outs = refs[len(given) :]

        def total(number):
            return sum(given.pop(0)[...].astype(F32) for _ in range(number)).astype(BF16)

        if upper is None:
            for index, one in enumerate(blocks):
                outs[0][index] = total(len(one))
        else:
            for out in outs:
                out[...] = total(len(terms))

    def spec(index, side=None):
        if side is None:
            return pl.BlockSpec((None, tile, width), lambda i: (index, i, 0))
        half = features // 2 // tile
        if side == 0:
            return pl.BlockSpec((None, tile, width), lambda i, t: (index, t[0] * half + i, 0))
        return pl.BlockSpec((None, tile, width), lambda i, t: (index, (1 - t[0]) * half + i, 0))

    arrays = [array for array, _ in terms]
    if upper is None:
        return call(
            name,
            kernel,
            (features // tile,),
            [spec(index) for _, index in terms],
            pl.BlockSpec((count, tile, width), lambda i: (0, i, 0)),
            shaped((count, features, width), BF16),
        )(*arrays)
    return call(
        name,
        kernel,
        (features // 2 // tile,),
        [spec(index, 0) for _, index in terms] + [spec(index, 1) for _, index in terms],
        [pl.BlockSpec((tile, width), lambda i, _: (i, 0))] * 2,
        [shaped((features // 2, width), BF16)] * 2,
        table=jnp.full((1,), upper, jnp.int32),
    )(*arrays, *arrays)


def attended_backward(left, late, table, start):
    number = table.shape[1]
    rows, features = left.shape

    def kernel(_, a, g, out):
        out[...] = dot(a[...], g[...]).astype(BF16)

    return call(
        "attended_back",
        kernel,
        (number,),
        [fixed(left.shape), tabled((features, LANES), (0, 1), start)],
        block((rows, LANES)),
        shaped((number, rows, LANES), BF16),
        table=table,
    )(left, late)


def contract(name, terms, extras, finish, outs, table=None):
    terms = [(left if isinstance(left, list) else [left], *more) for left, *more in terms]
    number = max(len(left) * left[0].shape[0] for left, _, _ in terms)
    rows = terms[0][0][0].shape[1]
    features = terms[0][1].shape[1]
    count, more = len(terms), len(extras)
    given_lefts = [one for left, _, _ in terms for one in left]

    def kernel(*refs):
        refs = list(refs if table is None else refs[1:])
        lefts = [chosen([refs.pop(0) for _ in left]) for left, _, _ in terms]
        rights = refs[:count]
        given = refs[count : count + more]
        results, total = refs[count + more : -1], refs[-1]
        out = dot_nt(lefts[0], rights[0][...])
        for left, right in zip(lefts[1:], rights[1:]):
            out = out + dot_nt(left, right[...])
        step = pl.program_id(0)

        @pl.when(step == 0)
        def _():
            total[...] = out

        @pl.when(step > 0)
        def _():
            total[...] += out

        @pl.when(step == number - 1)
        def _():
            finish(total, given, results)

    return call(
        name,
        kernel,
        (number,),
        [
            block(one.shape[1:], step=0 if len(left) > 1 else 1)
            for left, _, _ in terms
            for one in left
        ]
        + [where(features, left[0].shape[2]) for left, _, where in terms]
        + [fixed(extra.shape) for extra in extras],
        [whole(out.shape) for out in outs],
        outs,
        scratch=[pltpu.VMEM((rows, features), F32)],
        table=table,
    )(*given_lefts, *[right for _, right, _ in terms], *extras)


def by_rows(rows, sums, features, work, tile=64):
    tile = min(rows, tile)

    def step(i, totals):
        found = work(pl.ds(pl.multiple_of(i * tile, tile), tile))
        return tuple(
            total + jnp.sum(one.reshape(-1, 8, features), axis=0)
            for total, one in zip(totals, found)
        )

    zero = jnp.zeros((8, features), F32)
    totals = lax.fori_loop(0, rows // tile, step, (zero,) * sums)
    return [jnp.sum(total, axis=0, keepdims=True) for total in totals]


def normalize(values):
    average = jnp.mean(values, axis=1, keepdims=True)
    inverse = lax.rsqrt(
        jnp.mean(values * values, axis=1, keepdims=True) - average * average + EPS
    )
    return (values - average) * inverse, inverse


def norm_back(incoming, normed, inverse):
    return inverse * (
        incoming
        - jnp.mean(incoming, axis=1, keepdims=True)
        - normed * jnp.mean(incoming * normed, axis=1, keepdims=True)
    )


def enter(tokens, vectors):
    rows, features = tokens.shape

    def kernel(tokens, vectors, low, turned):
        shift, scale = vectors[0:1], 1.0 + vectors[1:2]

        def work(here):
            values = normalize(tokens[here, :].astype(F32))[0] * scale + shift
            values = values.astype(BF16)
            low[here, :] = values
            turned[:, here] = values.T
            return ()

        by_rows(rows, 0, features, work, LANES)

    return call(
        "enter",
        kernel,
        (1,),
        [whole(tokens.shape), whole(vectors.shape)],
        [whole((rows, features)), whole((features, rows))],
        [shaped((rows, features), BF16), shaped((features, rows), BF16)],
    )(tokens, vectors)


def enter_back(cotangent, branch, vectors):
    rows, features = cotangent.shape

    def kernel(cotangent, branch, vectors, low, turned, sums):
        gate = vectors[5:6]

        def work(here):
            upstream = cotangent[here, :].astype(F32)
            values = (gate * upstream).astype(BF16)
            low[here, :] = values
            turned[:, here] = values.T
            return values.astype(F32), branch[here, :] * upstream

        sums[...] = jnp.concatenate(by_rows(rows, 2, features, work, LANES), axis=0)

    return call(
        "enter_back",
        kernel,
        (1,),
        [whole(cotangent.shape), whole(branch.shape), whole(vectors.shape)],
        [whole((rows, features)), whole((features, rows)), whole((2, features))],
        [
            shaped((rows, features), BF16),
            shaped((features, rows), BF16),
            shaped((2, features), F32),
        ],
    )(cotangent, branch, vectors)


def finish_middle(total, given, results):
    tokens, vectors = given
    branch, middle, low, turned = results
    rows, features = total.shape
    shift, scale, gate = vectors[3:4], 1.0 + vectors[4:5], vectors[2:3]
    bias = vectors[6:7]

    def work(here):
        one = total[here, :] + bias
        branch[here, :] = one
        values = tokens[here, :].astype(F32) + gate * one
        middle[here, :] = values
        values = (normalize(values)[0] * scale + shift).astype(BF16)
        low[here, :] = values
        turned[:, here] = values.T
        return ()

    by_rows(rows, 0, features, work, LANES)


def finish_output(total, given, results):
    middle, vectors = given
    branch, output = results
    rows, features = total.shape
    gate, bias = vectors[5:6], vectors[7:8]

    def work(here):
        two = total[here, :] + bias
        branch[here, :] = two
        output[here, :] = (middle[here, :] + gate * two).astype(BF16)
        return ()

    by_rows(rows, 0, features, work)


def finish_middle_back(total, given, results):
    middle, branch, cotangent, vectors = given
    middle_back, low, turned, sums = results
    rows, features = total.shape
    gate, scale = vectors[2:3], 1.0 + vectors[4:5]

    def work(here):
        back = total[here, :]
        normed, inverse = normalize(middle[here, :])
        out = cotangent[here, :].astype(F32) + norm_back(back * scale, normed, inverse)
        middle_back[here, :] = out
        rounded = (gate * out).astype(BF16)
        low[here, :] = rounded
        turned[:, here] = rounded.T
        return back, back * normed, branch[here, :] * out, rounded.astype(F32)

    sums[...] = jnp.concatenate(by_rows(rows, 4, features, work, LANES), axis=0)


def finish_tokens_back(total, given, results):
    tokens, middle_back, vectors = given
    tokens_back, sums = results
    rows, features = total.shape
    scale = 1.0 + vectors[1:2]

    def work(here):
        back = total[here, :]
        normed, inverse = normalize(tokens[here, :].astype(F32))
        out = middle_back[here, :] + norm_back(back * scale, normed, inverse)
        tokens_back[here, :] = out.astype(BF16)
        return back, back * normed

    sums[...] = jnp.concatenate(by_rows(rows, 2, features, work), axis=0)


def chosen(parts):
    found = parts[0][...]
    for index, part in enumerate(parts[1:], 1):
        found = jnp.where(pl.program_id(0) == index, part[...], found)
    return found


def gradients(name, pairs, count, adds=(), form="one"):
    features, rows = pairs[0][0].shape
    parts = [one for _, parts in pairs for one in parts]
    width = sum(one.shape[2] for one, _ in parts)
    lefts, rights = len(pairs), len(parts)
    half = features // 2
    split = [isinstance(add[0], list) for add in adds]
    given = []
    for add, two in zip(adds, split):
        given += [(one[side][None], 0) for side in (0, 1) for one in add] if two else add

    def kernel(*refs):
        left_refs = refs[:lefts]
        right_refs = list(refs[lefts : lefts + rights])
        add_refs = list(refs[lefts + rights : lefts + rights + len(given)])
        outs = refs[lefts + rights + len(given) :]
        found = []
        for left, (_, own) in zip(left_refs, pairs):
            for _ in own:
                found.append(dot(left[...], right_refs.pop(0)[...]))
        out = found[0] if len(found) == 1 else jnp.concatenate(found, axis=1)
        for add, two in zip(adds, split):
            sides = [
                chosen([add_refs.pop(0) for _ in add]).astype(F32)
                for _ in range(2 if two else 1)
            ]
            out = out + (jnp.concatenate(sides, axis=0) if two else sides[0])
        out = out.astype(BF16)
        if form == "one":
            outs[0][...] = out
        else:
            for index in range(count):

                @pl.when(pl.program_id(0) == index)
                def _():
                    outs[2 * index][...] = out[:half]
                    outs[2 * index + 1][...] = out[half:]

    def addend(one):
        array, index = one
        return pl.BlockSpec((None, *array.shape[1:]), lambda *_: (index, 0, 0))

    if form == "one":
        out_specs, shape = [block((features, width))], (count, features, width)
    else:
        shape = (half, width)
        out_specs = [whole(shape)] * (2 * count)
    got = call(
        name,
        kernel,
        (count,),
        [fixed(left.shape) for left, _ in pairs]
        + [block(one.shape[1:], 0, first) for one, first in parts]
        + [addend(one) for one in given],
        out_specs,
        [shaped(shape, BF16)] * len(out_specs),
    )(
        *[left for left, _ in pairs],
        *[one for one, _ in parts],
        *[array for array, _ in given],
    )
    return got[0] if form == "one" else got


def attend(queries, pieces):
    number, rows, _ = queries.shape
    count = len(pieces)
    keys = sum(piece.shape[1] for piece in pieces)
    tile = min(rows, 256)

    def kernel(*refs):
        query, kv = refs[0], refs[1 : 1 + count]
        out_ref, log_ref = refs[1 + count :]
        head = lax.broadcasted_iota(jnp.int32, (1, LANES), 1) < HEAD_DIM

        def step(i, _):
            here = pl.ds(pl.multiple_of(i * tile, tile), tile)
            both = query[here, :]
            outs, logs = [], []
            for keep in (head, ~head):
                one = jnp.where(keep, both, jnp.zeros_like(both))
                scores = [dot_nt(one, piece[:, :LANES]) for piece in kv]
                top = functools.reduce(
                    jnp.maximum, [jnp.max(s, axis=1, keepdims=True) for s in scores]
                )
                weights = [jnp.exp2((s - top) * SCALE_LOG2) for s in scores]
                total = sum(jnp.sum(w, axis=1, keepdims=True) for w in weights)
                inverse = 1.0 / total
                out = sum(
                    dot((w * inverse).astype(BF16), piece[:, LANES:])
                    for w, piece in zip(weights, kv)
                )
                outs.append(out)
                logs.append(top * SCALE_LOG2 + jnp.log(total) * math.log2(math.e))
            out_ref[here, :] = jnp.where(head, outs[0], outs[1]).astype(BF16)
            table = jnp.where(head, logs[0], logs[1]).T
            log_ref[0:1, here] = table[0:1]
            log_ref[1:2, here] = table[HEAD_DIM : HEAD_DIM + 1]
            return 0

        lax.fori_loop(0, rows // tile, step, 0)

    return call(
        "attend",
        kernel,
        (number,),
        [block((rows, LANES))] + [block((piece.shape[1], 2 * LANES)) for piece in pieces],
        [block((rows, LANES)), block((2, rows))],
        [shaped((number, rows, LANES), BF16), shaped((number, 2, rows), F32)],
    )(queries, *pieces)


def attend_back(queries, pieces, logs, incoming, first, kinds, begin, number):
    rows = queries.shape[1]
    count = len(pieces)
    keys = sum(piece.shape[1] for piece in pieces)
    tile = min(rows, 256)

    def kernel(*refs):
        query, back_ref, log_ref = refs[:3]
        kv = refs[3 : 3 + count]
        query_back = refs[3 + count]
        kv_back = refs[4 + count : 4 + 2 * count]
        sums, scratch = refs[4 + 2 * count], refs[5 + 2 * count :]
        head = lax.broadcasted_iota(jnp.int32, (1, LANES), 1) < HEAD_DIM
        turned = [piece[:, :LANES].T for piece in kv]
        top = lax.broadcasted_iota(jnp.int32, (LANES, 1), 0) < HEAD_DIM
        for held in scratch:
            held[...] = jnp.zeros_like(held)

        def step(j, query_sum):
            here = pl.ds(pl.multiple_of(j * tile, tile), tile)
            backs = []
            for index, keep in enumerate((head, ~head)):
                zero = jnp.zeros((tile, LANES), BF16)
                one = jnp.where(keep, query[here, :], zero)
                back = jnp.where(keep, back_ref[here, :], zero)
                log = log_ref[index : index + 1, here]
                chances, mixes = [], []
                for piece in kv:
                    scores = dot_nt(piece[:, :LANES], one)
                    chances.append(jnp.exp2(scores * SCALE_LOG2 - log))
                    mixes.append(dot_nt(piece[:, LANES:], back))
                centre = sum(
                    jnp.sum(p * m, axis=0, keepdims=True) for p, m in zip(chances, mixes)
                )
                total = None
                for i in range(count):
                    score_back = (chances[i] * (mixes[i] - centre)).astype(BF16)
                    scratch[i][:, :LANES] += dot(score_back, one) * SCALE
                    scratch[i][:, LANES:] += dot(chances[i].astype(BF16), back)
                    term = dot(turned[i], score_back)
                    total = term if total is None else total + term
                backs.append(total)
            both = (jnp.where(top, backs[0], backs[1]).T * SCALE).astype(BF16)
            query_back[here, :] = both
            return query_sum + jnp.sum(both.astype(F32), axis=0, keepdims=True)

        sums[...] = lax.fori_loop(0, rows // tile, step, jnp.zeros((1, LANES), F32))
        for out, held in zip(kv_back, scratch):
            out[...] = held[...].astype(out.dtype)

    return call(
        "attend_back",
        kernel,
        (number,),
        [
            block((rows, LANES), first=begin),
            block((rows, LANES), first=first + begin),
            block((2, rows), first=begin),
        ]
        + [block((piece.shape[1], 2 * LANES), first=begin) for piece in pieces],
        [block((rows, LANES))]
        + [block((piece.shape[1], 2 * LANES)) for piece in pieces]
        + [block((1, LANES))],
        [shaped((number, rows, LANES), BF16)]
        + [
            shaped((number, piece.shape[1], 2 * LANES), kind)
            for piece, kind in zip(pieces, kinds)
        ]
        + [shaped((number, 1, LANES), F32)],
        scratch=[pltpu.VMEM((piece.shape[1], 2 * LANES), F32) for piece in pieces],
    )(queries, incoming, logs, *pieces)


def block_at(features, width):
    return block((features, width))


class Steps:
    def __init__(self, steps):
        self.steps, self.result = steps, None
        self.got = next(steps)

    def step(self):
        if self.result is None:
            try:
                self.got = self.steps.send(self.got)
            except StopIteration as end:
                self.got = self.result = end.value

    def hold(self):
        LAST.extend(jax.tree.leaves(self.got))

    def behind(self, *values):
        (*values, self.got) = lax.optimization_barrier((*values, self.got))
        return values

    def finish(self):
        while self.result is None:
            self.step()
        return self.result


class Plain:
    def __init__(self, sizes):
        self.latents, self.parts, self.width = sizes
        self.row = lax.axis_size("y") * lax.axis_size("core")
        self.col = lax.axis_size("lat") * lax.axis_size("sub")

    def scatter(self, values, held=None):
        rows, width = values.shape
        shaped_in = values.reshape(self.latents, 2, LENGTH // 2, width)
        halves = lax.all_to_all(shaped_in, "core", 1, 0, tiled=True)
        pieces = halves.reshape(self.col, -1, width)
        pieces = lax.all_to_all(pieces, COLS, 0, 0, tiled=True)
        return pieces.transpose(1, 0, 2).reshape(-1, self.col * width), held

    def collect_start(self, values):
        rows = values.shape[0]
        pieces = values.reshape(rows, self.col, -1).transpose(1, 0, 2)
        return [lax.all_to_all(pieces, COLS, 0, 0, tiled=True)]

    def collect(self, pieces):
        (pieces,) = pieces
        halves = pieces.reshape(2 * self.latents, 1, LENGTH // 2, -1)
        back = lax.all_to_all(halves, "core", 0, 1, tiled=True)
        return back.reshape(-1, self.width)

    def modulation(self, partial, bias, row_bias, col_bias):
        group = 2 * self.latents
        ours = lax.psum(partial, "core").reshape(-1, group, partial.shape[1])
        ours = lax.psum_scatter(ours, "y", scatter_dimension=0, tiled=True)[0] + bias
        sent = jnp.repeat(ours, self.col // group, axis=0)
        got = lax.all_to_all(sent, COLS, 0, 0, tiled=True)
        got = got.reshape(self.col, 6, -1).transpose(1, 0, 2).reshape(6, -1)
        cols = lax.all_gather(col_bias, COLS, axis=1, tiled=True)
        every = lax.all_gather(row_bias, ROWS, axis=0)
        return jnp.concatenate([got, cols], axis=0), [
            every.reshape(self.row * self.parts, 1, -1)
        ]

    def gather(self, parts, held):
        every = lax.all_gather(parts, COLS, axis=1, tiled=True)
        every = lax.all_gather(every, ROWS, axis=0, tiled=True)
        return [every[:, :, :LANES]], [every[:, :, LANES:]], held

    def gather_start(self, parts, held):
        return parts, held

    def gather_late(self, part):
        every = lax.all_gather(part, (*ROWS, *COLS), axis=0, tiled=True)
        return every.reshape(self.row, -1, part.shape[1])

    def expand_bias(self, row_bias, biases):
        every = lax.all_gather(row_bias, ROWS, axis=0)
        return every.reshape(self.row * self.parts, 1, -1)

    def with_units(self, row_sums, unit_sums):
        return [jnp.concatenate([row_sums[0], unit_sums[0]], axis=-1)]

    def tables(self):
        blocks = jnp.arange(self.row * self.parts, dtype=jnp.int32)
        return [jnp.stack([blocks // self.parts, blocks % self.parts])]


    def share(self, kv):
        return [[lax.all_gather(kv[0], ("core", "sub"), axis=1, tiled=True)]]

    def kinds(self):
        return [F32]

    PLACES = ((0, 0),)

    def give_back(self, backs):
        return [
            lax.psum_scatter(
                backs[0][0], ("core", "sub"), scatter_dimension=1, tiled=True
            ).astype(BF16)
        ]

    def sum_up(self, *args):
        return Steps(self.reduce(*args))

    def feed_back(self, low, turned, late, slopes, hidden, extras):
        table = jnp.stack([jnp.arange(self.row, dtype=jnp.int32)] * 2) * jnp.array(
            [[1], [0]], jnp.int32
        )
        shrink, grow, (sums, *ends) = feed_back(
            "feed_back", low, turned, late, slopes, hidden, table, self.parts, extras, None
        )

        def blocks(parts):
            return jnp.stack(parts, axis=1).reshape(-1, *parts[0].shape[1:])

        steps = [Steps(self.reduce_ready(blocks(one))) for one in (shrink, grow)]
        return steps, ends, [sums.reshape(self.row * self.parts, 1, -1)]

    def reduce(self, name, pairs):
        grads = gradients(name, pairs(0, 0, 0), self.row * self.parts)
        return (yield from self.reduce_ready(grads))

    def reduce_ready(self, grads):
        grads = grads.astype(F32)
        grads = yield grads
        grads = lax.psum_scatter(grads, ROWS, scatter_dimension=0, tiled=True)
        grads = lax.psum_scatter(grads, COLS, scatter_dimension=1, tiled=True)
        return lax.psum(grads, "dp")

    def small(self, vectors, row_sums, col_sums):
        every = ("dp", *ROWS, *COLS)
        group = 2 * self.latents
        total = yield lax.psum(vectors, ("core", "sub"))
        total = total.astype(BF16)
        mine = lax.all_gather(total[:, None], "lat", axis=1, tiled=True)
        mine = lax.all_gather(mine, "y", axis=1, tiled=True)
        mine = lax.all_gather(mine, "dp", axis=1, tiled=True)
        col = lax.axis_index("lat") * lax.axis_size("sub") + lax.axis_index("sub")
        cut = lax.dynamic_slice_in_dim(mine, col * self.width, self.width, axis=2)
        cut = cut.transpose(1, 0, 2).reshape(mine.shape[1], -1)
        rows = lax.psum(row_sums[0], every).reshape(self.row, self.parts, -1)
        row = lax.axis_index("y") * 2 + lax.axis_index("core")
        rows = lax.dynamic_index_in_dim(rows, row, 0, keepdims=False)
        cols = lax.psum(col_sums, every)
        cols = lax.dynamic_slice_in_dim(cols, col * self.width, self.width, axis=1)
        return cut, rows, cols

    def col_sum(self, values):
        return lax.psum(values, COLS)

    def both_groups(self, values):
        return lax.all_gather(values, "dp", axis=0, tiled=True)


class Cube(Plain):
    PLACES = ((0, 0), (0, 1), (1, 0), (1, 1))

    def __init__(self, sizes):
        super().__init__(sizes)
        self.x = lax.axis_index("dp")
        self.y = lax.axis_index("y")
        self.c = lax.axis_index("core")
        self.z = lax.axis_index("lat")

    def swap(self, values, axis):
        return lax.ppermute(values, axis, [(0, 1), (1, 0)])

    def along(self, values, bits):
        return lax.ppermute(values, "lat", [(i, i ^ bits) for i in range(4)])

    def scatter(self, values, held=None):
        rows, width = values.shape
        halves = values.reshape(self.latents, 2, LENGTH // 2, width)
        keep = lax.dynamic_index_in_dim(halves, self.c, 1, keepdims=False)
        send = lax.dynamic_index_in_dim(halves, 1 - self.c, 1, keepdims=False)
        every = jnp.concatenate([keep, self.swap(send, "core")], axis=0)
        if held is not None:
            every, held = lax.optimization_barrier((every, held))
        pieces = []
        for latent in range(4):
            index = ((latent // 2) ^ self.c) * 2 + latent % 2
            pieces.append(lax.dynamic_index_in_dim(every, index, 0, keepdims=False))
        pieces = lax.all_to_all(jnp.stack(pieces), "lat", 0, 0, tiled=True)
        return pieces.transpose(1, 0, 2).reshape(-1, 4 * width), held

    def placed(self, pieces):
        odd, high = self.z % 2 == 1, self.z >= 2
        one, two, three, four = pieces
        one, two = jnp.where(odd, two, one), jnp.where(odd, one, two)
        three, four = jnp.where(odd, four, three), jnp.where(odd, three, four)
        return [
            jnp.where(high, three, one),
            jnp.where(high, four, two),
            jnp.where(high, one, three),
            jnp.where(high, two, four),
        ]

    def collect_start(self, values):
        pieces = values.reshape(-1, 4, self.width).transpose(1, 0, 2)
        return [lax.all_to_all(pieces, "lat", 0, 0, tiled=True)]

    def collect(self, pieces):
        width = self.width
        every = pieces[0].reshape(2, 2, -1, width)

        def latents(core):
            return lax.dynamic_index_in_dim(every, core, 0, keepdims=False)

        keep = latents(self.c)
        got = self.swap(latents(1 - self.c), "core")
        first = jnp.where(self.c == 0, keep, got)
        second = jnp.where(self.c == 0, got, keep)
        return jnp.stack([first, second], axis=1).reshape(-1, width)

    def modulation(self, partial, bias, row_bias, col_bias):
        span = partial.shape[1]
        own = row_bias.reshape(1, -1)
        got = self.swap(jnp.concatenate([partial, own], axis=0), "core")
        ours, other = partial + got[:-1], got[-1:]
        halves = ours.reshape(2, 4, span)
        keep = lax.dynamic_index_in_dim(halves, self.y, 0, keepdims=False)
        send = lax.dynamic_index_in_dim(halves, 1 - self.y, 0, keepdims=False)
        got = self.swap(jnp.concatenate([send, own, other], axis=0), "y")
        ours = keep + got[:4] + bias
        rows = jnp.stack([own, got[4:5], other, got[5:6]]).reshape(2, 2, 2, -1)
        flip = jnp.stack([rows[:, :, 1], rows[:, :, 0]], axis=2)
        rows = jnp.where(self.x == 0, rows, flip).transpose(2, 0, 1, 3)[:, :, :, None]
        pieces = []
        for bits in range(4):
            piece = lax.dynamic_index_in_dim(ours, self.z ^ bits, 0, keepdims=False)
            piece = jnp.concatenate([piece.reshape(6, -1), col_bias], axis=0)
            pieces.append(piece if bits == 0 else self.along(piece, bits))
        vectors = jnp.concatenate(self.placed(pieces), axis=1)
        return vectors, [rows[x, core] for x, core in self.PLACES]

    def gather_start(self, parts, held):
        part = lax.dynamic_index_in_dim(parts, self.x, 0, keepdims=False)
        odd, high = self.z % 2 == 1, self.z >= 2
        got = self.along(part, 1)
        part = jnp.concatenate([jnp.where(odd, got, part), jnp.where(odd, part, got)], axis=0)
        got = self.along(part, 2)
        part = jnp.concatenate(
            [jnp.where(high, got, part), jnp.where(high, part, got)], axis=0
        )
        return lax.optimization_barrier((part, held))

    def gather(self, part, held):
        one, two = part[:, :LANES], part[:, LANES:]
        one_pair = jnp.stack([one, self.swap(one, "dp")])
        near = jnp.stack([two, self.swap(two, "y")])
        near = after(near, one_pair)
        far = self.swap(near, "dp")
        kv = [near, self.swap(near, "core"), far, self.swap(far, "core")]
        got = self.swap(one_pair, "y")
        near = jnp.stack([one_pair[0], got[0]])
        far = jnp.stack([one_pair[1], got[1]])
        near, held = lax.optimization_barrier((near, held))
        queries = [near, self.swap(near, "core"), far, self.swap(far, "core")]
        return queries, kv, held

    def expand_bias(self, row_bias, biases):
        number = self.row * self.parts
        table = jnp.concatenate(self.tables(), axis=1)
        place = table[0] * self.parts + table[1]
        chosen = place[None, :] == lax.broadcasted_iota(jnp.int32, (number, number), 0)
        every = jnp.concatenate(biases, axis=0)[:, 0]
        found = jnp.dot(chosen.astype(F32), every, precision=lax.Precision.HIGHEST)
        return found[:, None]

    def with_units(self, row_sums, unit_sums):
        found = []
        for one, (x, core) in zip(row_sums, self.PLACES):
            units = unit_sums[1 - core][2 * x : 2 * x + 2]
            found.append(jnp.concatenate([one, units], axis=-1))
        return found

    def tables(self):
        side = jnp.arange(2, dtype=jnp.int32)
        return [
            jnp.stack(
                [(side ^ self.y) * 2 + (self.c ^ core), jnp.full((2,), self.x ^ x)]
            ).astype(jnp.int32)
            for x, core in self.PLACES
        ]

    def share(self, kv):
        return [
            [kv[2 * x + core], self.swap(kv[2 * x + 1 - core], "core")]
            for x, core in self.PLACES
        ]

    def kinds(self):
        return [F32, BF16]

    def give_back(self, backs):
        got = [self.swap(backs[1 - core][1], "core") for core in (0, 1)]
        return [(own[0] + one.astype(F32)).astype(BF16) for own, one in zip(backs, got)]

    def feed_back(self, low, turned, late, slopes, hidden, extras):
        tables = self.tables()
        found, sums, before = [], [], None
        for core in (1, 0):
            rows = tables[core][0]
            shrink, grow, (one, *ends) = feed_back(
                "feed_back",
                low,
                turned,
                late,
                slopes,
                hidden,
                jnp.stack([rows, jnp.full((2,), self.x, jnp.int32)]),
                self.parts,
                [] if core else extras,
                before,
            )
            if core:
                (before,) = ends
                found = [[self.swap(one, "core") for one in part] for part in (shrink, grow)]
            else:
                LAST.extend([one for part in found for one in part])
                steps = [
                    Steps(self.reduce_ready(name, near, far, order))
                    for name, near, far, order in (
                        ("d_shrink", shrink, found[0], "yx"),
                        ("d_expand", grow, found[1], "xy"),
                    )
                ]
            one = one.reshape(2, 1, self.parts, -1).transpose(2, 0, 1, 3)
            one = jnp.where(self.x == 0, one, jnp.stack([one[1], one[0]]))
            sums.append(one.reshape(4, 1, -1))
        return steps, ends, sums

    def reduce_ready(self, name, near, far, order):
        axes, one, two = (("dp", "y"), 2, 1) if order == "xy" else (("y", "dp"), 1, 2)
        near, far = (
            [(part[x], y) for x in (0, 1) for y in (0, 1)] for part in (near, far)
        )
        sent = add_up(name, [[near[one], far[one]], [near[3], far[3]]])
        second = yield self.swap(sent, axes[0])
        sent = add_up(name, [[near[two], far[two], (second, 1)]])
        third = yield self.swap(sent, axes[1])
        terms = [near[0], far[0], (second, 0), (third, 0)]
        return (yield from self.reduce_col(add_up(name, [terms])))

    def reduce_col(self, blocks):
        own = yield lax.psum_scatter(blocks[0], COLS, scatter_dimension=0, tiled=True)
        got = yield self.swap(gate(own), "dp")
        return jnp.stack(
            [jnp.where(self.x == 0, own, got), jnp.where(self.x == 0, got, own)]
        ).astype(F32)

    def reduce(self, name, pairs):
        def grads(place, count, adds=(), form="one"):
            return gradients(name, pairs(*place), count, adds, form)

        def far(place, count):
            sent = grads(place, count, form="apart")
            return [self.swap(one, "core") for one in sent]

        near = yield far((1, 0, 1), 2)
        second = yield self.swap(grads((1, 0, 0), 2, [[near[:2], near[2:]]]), "dp")
        near = yield far((0, 1, 1), 1)
        last = yield far((0, 0, 1), 1)
        third = yield self.swap(grads((0, 1, 0), 1, [[near], [(second, 1)]]), "y")
        adds = [[last], [(second, 0)], [(third, 0)]]
        return (yield from self.reduce_col(grads((0, 0, 0), 1, adds)))

    def small(self, vectors, row_sums, col_sums):
        span = row_sums[0].shape[-1]
        features = vectors.shape[1]

        def flat(*parts):
            return jnp.concatenate([part.reshape(-1, LANES) for part in parts], axis=0)

        def cut(message, *shapes):
            parts, start = [], 0
            for shape in shapes:
                size = math.prod(shape) // LANES
                parts.append(message[start : start + size].reshape(shape))
                start += size
            return parts

        every = jnp.stack(row_sums).reshape(2, 2, 2, span)
        rows0, rows1 = every[:, 0], every[:, 1]
        got = yield self.swap(gate(flat(rows1, col_sums, vectors)), "core")
        got = cut(got, rows1.shape, col_sums.shape, vectors.shape)
        rows, cols = rows0 + got[0], col_sums + got[1]
        mine = (vectors + got[2]).astype(BF16).astype(F32)
        got = yield self.swap(gate(flat(rows[:, 1], cols, mine)), "y")
        got = cut(got, (2, span), cols.shape, mine.shape)
        rows, cols = rows[:, 0] + got[0], cols + got[1]
        pair = jnp.stack([mine, got[2]])
        got = yield self.swap(gate(flat(rows, cols, pair)), "dp")
        got = cut(got, rows.shape, cols.shape, pair.shape)
        rows = rows + jnp.stack([got[0][1], got[0][0]])
        rows = jnp.where(self.x == 0, rows, jnp.stack([rows[1], rows[0]]))
        cols = cols + got[1]
        four = jnp.stack([pair, got[2]]).reshape(4, 6, features)
        width = self.width

        def cuts(values):
            return self.placed(
                [values[..., i * width : (i + 1) * width] for i in range(4)]
            )

        found = []
        for bits, piece in enumerate(zip(cuts(four), cuts(cols))):
            piece = [*piece, rows]
            if bits:
                got = self.along(flat(*piece), bits)
                piece = cut(got, *[part.shape for part in piece])
            found.append(piece)
        tree = [(found[0][i] + found[1][i]) + (found[2][i] + found[3][i]) for i in (1, 2)]
        every = jnp.stack([one[0] for one in found])
        every = every.reshape(16, -1)
        place = lax.broadcasted_iota(jnp.int32, (16, 16), 0)
        held = lax.broadcasted_iota(jnp.int32, (16, 16), 1)
        latent = (
            (((held // 2) % 2) ^ self.x) * 8 + ((held % 2) ^ self.y) * 4 + ((held // 4) ^ self.z)
        )
        chosen = (latent == place).astype(F32)
        every = jnp.dot(chosen, every, precision=lax.Precision.HIGHEST).astype(BF16)
        return every, tree[1], tree[0]

    def col_sum(self, values):
        got = [values] + [self.along(values, bits) for bits in (1, 2, 3)]
        return (got[0] + got[1]) + (got[2] + got[3])

    def both_groups(self, values):
        got = self.swap(values, "dp")
        return jnp.where(
            self.x == 0,
            jnp.concatenate([values, got], axis=0),
            jnp.concatenate([got, values], axis=0),
        )


def body(
    fast,
    tokens,
    condition,
    modulation_weight,
    modulation_bias,
    input_weight,
    input_bias,
    output_weight,
    output_bias,
    expand_weight,
    expand_bias,
    shrink_weight,
    shrink_bias,
    cotangent,
):
    LAST.clear()
    width = tokens.shape[1]
    inner = input_weight.shape[2]
    parts = inner // LANES
    units = expand_weight.shape[1] // parts
    sizes = (tokens.shape[0] // LENGTH, parts, width)
    net = (Cube if fast else Plain)(sizes)

    own_in = (
        input_weight.reshape(width, 3, parts, LANES)
        .transpose(2, 0, 1, 3)
        .reshape(parts, width, 3 * LANES)
    )
    own_late = with_layout_constraint(
        jnp.concatenate([expand_weight, shrink_weight.T, output_weight.T], axis=1),
        Layout((0, 1)),
    )
    out_start = 2 * parts * units // LANES

    condition_float = condition.astype(F32)
    silu_low = jax.nn.silu(condition_float).astype(BF16)
    modulator = modulation_weight.reshape(modulation_weight.shape[0], -1)
    row_bias = jnp.concatenate(
        [
            input_bias.reshape(2, parts, LANES).transpose(1, 0, 2).reshape(parts, -1),
            expand_bias.reshape(parts, units),
        ],
        axis=1,
    ).astype(F32)
    late = net.gather_late(own_late)
    vectors, row_biases = net.modulation(
        dot(silu_low, modulator),
        modulation_bias.astype(F32).reshape(1, -1),
        row_bias,
        jnp.stack([output_bias, shrink_bias]).astype(F32),
    )
    silu_all = net.both_groups(silu_low)
    own_in, (vectors, silu_all) = net.gather_start(own_in, (vectors, silu_all))
    mine, own_in = net.scatter(tokens, own_in)
    query_bufs, kv_bufs, mine = net.gather(own_in, mine)
    rows = mine.shape[0]
    features = mine.shape[1]
    expand_biases = net.expand_bias(
        row_bias[:, 2 * LANES :], [one[..., 2 * LANES :] for one in row_biases]
    )
    tables = net.tables()

    low_one, turned_one = enter(mine, vectors)
    queries, own_kv = [], []
    for one, two, bias in zip(query_bufs, kv_bufs, row_biases):
        one, two = project(low_one, one, two, bias)
        queries.append(one)
        own_kv.append(two)
    kv = net.share(own_kv)
    attended, logs = [], []
    for one, pieces in zip(queries, kv):
        out, log = attend(one, pieces)
        attended.append(out)
        logs.append(log)
    back, (late, attended[-1]) = net.scatter(cotangent, (late, attended[-1]))

    def out_place(number):
        def place(features, width):
            return tabled((features, width), (2 * number, 2 * number + 1), out_start)

        return place

    branch_one, middle, low_two, turned_two = contract(
        "out",
        [(one, late, out_place(i)) for i, one in enumerate(attended)],
        [mine, vectors],
        finish_middle,
        [
            shaped((rows, features), F32),
            shaped((rows, features), F32),
            shaped((rows, features), BF16),
            shaped((features, rows), BF16),
        ],
        table=jnp.concatenate(tables, axis=0),
    )
    slopes, hidden, branch_two, output = feed_forward(
        low_two, late, expand_biases.reshape(-1, 1, parts * units), [middle, vectors]
    )
    branch_two_back, turned_two_back, sums_back = enter_back(back, branch_two, vectors)
    shrink_sum, gate_two_back = sums_back[0:1], sums_back[1:2]

    steps, ends, expand_sums = net.feed_back(
        branch_two_back,
        (turned_two_back, turned_two),
        late,
        slopes,
        hidden,
        [middle, branch_one, back, vectors],
    )
    middle_back, branch_one_back, turned_one_back, sums_two = ends
    shrink_steps, expand_steps = steps
    incoming = attended_backward(
        branch_one_back, late, jnp.concatenate(tables, axis=1), out_start
    )
    output = net.collect_start(gate(output))
    number = len(kv)
    blocks = queries[0].shape[0]
    found = {}

    def attention_back(i, begin, count):
        got = attend_back(
            queries[i], kv[i], logs[i], incoming, i * blocks, net.kinds(), begin, count
        )
        found[i, begin] = [got[0], got[1:-1], got[-1]]

    def kv_final(keys):
        for key, one in zip(keys, net.give_back([found[key][1] for key in keys])):
            found[key][1] = one

    def pairs(x, y, core):
        i = 2 * x + core
        key, begin = ((i, 0), y) if (i, 1) not in found else ((i, y), 0)
        heads = [(found[key][0], begin), (found[key][1], begin)]
        return [(turned_one, heads), (turned_one_back, [(attended[i], y)])]

    def every_block(i, which):
        ones = [found[key][which] for key in sorted(found) if key[0] == i]
        return ones if len(ones) > 1 else ones[0]

    if number > 1:
        attention_back(3, 0, 2)
        attention_back(2, 0, 2)
        LAST.extend(output)
        shrink_steps.hold()
        expand_steps.hold()
        shrink_steps.step()
        expand_steps.step()
        kv_final([(2, 0), (3, 0)])
        in_steps = net.sum_up("d_in", pairs)
        attention_back(1, 1, 1)
        in_steps.step()
        attention_back(0, 1, 1)
        shrink_steps.step()
        kv_final([(0, 1), (1, 1)])
        in_steps.step()
        attention_back(1, 0, 1)
        attention_back(0, 0, 1)
        expand_steps.step()
        kv_final([(0, 0), (1, 0)])
        in_steps.step()
        in_steps.step()
    else:
        attention_back(0, 0, blocks)
        kv_final([(0, 0)])
        in_steps = net.sum_up("d_in", pairs)
    shrink_steps.hold()
    tokens_back, sums_one = contract(
        "tokens_back",
        [(every_block(i, 0), buf, block_at) for i, buf in enumerate(query_bufs)]
        + [(every_block(i, 1), buf, block_at) for i, buf in enumerate(kv_bufs)],
        [mine, middle_back, vectors],
        finish_tokens_back,
        [shaped((rows, features), BF16), shaped((2, features), F32)],
    )
    summed = jnp.concatenate([sums_one, sums_two[2:3], sums_two[0:2], gate_two_back], axis=0)

    def value_sum(one):
        return jnp.sum(one[:, :, LANES:].astype(F32), axis=1, keepdims=True)

    row_sums = []
    for i in range(number):
        ones = [found[key] for key in sorted(found) if key[0] == i]
        row_sums.append(
            jnp.concatenate(
                [
                    jnp.concatenate([one[2], value_sum(one[1])], axis=-1)
                    for one in ones
                ]
            )
        )
    row_sums = net.with_units(row_sums, expand_sums)
    col_sums = jnp.concatenate([sums_two[3:4], shrink_sum], axis=0)
    tokens_back = net.collect_start(tokens_back)
    small_steps = Steps(net.small(summed, row_sums, col_sums))
    in_steps.step()
    small_steps.step()
    LAST.extend(tokens_back)
    small_steps.step()
    shrink_steps.step()
    expand_steps.step()
    in_steps.step()
    shrink_parts = shrink_steps.finish()
    expand_parts = expand_steps.finish()
    in_parts = in_steps.finish()

    every, row_found, col_found = small_steps.finish()
    modulation_weight_gradient = lax.dot_general(
        silu_all, every, (((0,), (0,)), ((), ())), preferred_element_type=F32
    ).reshape(modulation_weight.shape)
    modulation_bias_gradient = jnp.sum(every.astype(F32), axis=0).reshape(6, width)
    groups = condition.shape[0]
    ours = lax.dynamic_slice_in_dim(every, lax.axis_index("dp") * groups, groups, axis=0)
    silu_back = net.col_sum(dot_nt(ours, modulator))
    silu_pull = jax.vjp(jax.nn.silu, condition_float)[1]
    condition_gradient = silu_pull(silu_back)[0]

    return (
        net.collect(output),
        net.collect(tokens_back).astype(F32),
        condition_gradient,
        modulation_weight_gradient,
        modulation_bias_gradient,
        in_parts[:, :, : 3 * LANES]
        .reshape(parts, width, 3, LANES)
        .transpose(1, 2, 0, 3)
        .reshape(input_weight.shape),
        row_found[:, : 2 * LANES]
        .reshape(parts, 2, LANES)
        .transpose(1, 0, 2)
        .reshape(input_bias.shape),
        in_parts[:, :, 3 * LANES :].transpose(0, 2, 1).reshape(output_weight.shape),
        col_found[0],
        expand_parts.transpose(1, 0, 2).reshape(expand_weight.shape),
        row_found[:, 2 * LANES :].reshape(expand_bias.shape),
        shrink_parts.transpose(0, 2, 1).reshape(shrink_weight.shape),
        col_found[1],
    )


def solution(mesh):
    dp, row, col = (mesh.shape[name] for name in ("dp", "row", "col"))

    def run(*arrays):
        latents = arrays[0].shape[0] // (dp * row * LENGTH)
        group = 2 * latents
        refined = Mesh(
            mesh.devices.reshape(dp, row // 2, 2, group, col // group),
            ("dp", "y", "core", "lat", "sub"),
        )
        fast = (dp, row, col, latents) == (2, 4, 4, 2)
        token = P(("dp", *ROWS), COLS)
        weights = (
            P(ROWS, None, COLS),
            P(None, COLS),
            P(COLS, None, ROWS),
            P(None, ROWS),
            P(ROWS, COLS),
            P(COLS),
            P(COLS, ROWS),
            P(ROWS),
            P(ROWS, COLS),
            P(COLS),
        )
        given = P("dp", ROWS)
        return jax.shard_map(
            functools.partial(body, fast),
            mesh=refined,
            in_specs=(token, given, *weights, token),
            out_specs=(token, token, given, *weights),
            check_vma=False,
        )(*arrays)

    return run
```
